32 devices in a mesh: grp: 2 (over core), tp: 4 (over y, x), src: 4 (over z).
Axes of the slice: x: 2, y: 2, z: 4, core: 2. Of those that a mesh axis runs over, the one named last changes fastest.
Arguments:
- hidden_in: bfloat16 [512, 5120], P(('grp', 'src')), may hold values from -6 to 6
- attn_gain: float32 [5120], replicated, may hold values from 0.5 to 1.5
- w_qkv: int32 [1280, 5120], P(None, 'tp'), may hold values from -2147483648 to 2147483646
- qkv_scale: float32 [5120], P('tp'), may hold values from 0.0001118034 to 0.00041926274
- q_gain: float32 [128], replicated, may hold values from 0.25 to 1.75
- k_gain: float32 [128], replicated, may hold values from 0.1 to 1.9
- key_cache: bfloat16 [8, 64, 128, 512], P(('grp', 'src'), 'tp'), may hold values from -400 to 400
- value_cache: bfloat16 [8, 64, 128, 512], P(('grp', 'src'), 'tp'), may hold values from -9 to 9
- lengths: int32 [8, 64], P(('grp', 'src'), 'tp'), may hold values from 1 to 128, as said below
- w_out: int32 [1024, 5120], P('tp'), may hold values from -2147483648 to 2147483646
- out_scale: float32 [5120], replicated, may hold values from 0.0003125 to 0.00125
- mlp_gain: float32 [5120], replicated, may hold values from 0.5 to 1.5
- w_gate: int32 [1280, 12800], P(('grp', 'src'), 'tp'), may hold values from -2147483648 to 2147483646
- w_up: int32 [1280, 12800], P(('grp', 'src'), 'tp'), may hold values from -2147483648 to 2147483646
- gate_scale: float32 [12800], P('tp'), may hold values from 0.0001118034 to 0.00041926274
- up_scale: float32 [12800], P('tp'), may hold values from 0.0001118034 to 0.00041926274
- w_down: int32 [3200, 5120], P('tp', ('grp', 'src')), may hold values from -2147483648 to 2147483646
- down_scale: float32 [5120], replicated, may hold values from 0.00013258251 to 0.00053033006
Outputs:
- layer_out: bfloat16 [512, 5120], P(('grp', 'src'), 'tp')
The draws below stay inside these ranges and needn't reach their ends.
Inputs may be any that keep to these rules, and one draw needn't show every extreme that they name: `lengths`: some sequence has exactly 128 cached positions.
All inputs are finite; a program needn't handle non-finite values.
Results may differ from the reference program's by a relative error of at most 0.028.
Values may be sent and summed in bfloat16 or wider, within the bound.
A program may use at most 128 MiB of HBM per device.

```python
import math
import jax
import jax.numpy as jnp
from jax import lax

D = 5120
QUERY_HEADS = 32
KEY_VALUE_HEADS = 4
HEAD_SIZE = 128
FFW = 12800
B_DEV = 64
CACHE_POSITIONS = 128
NGROUPS = 8
B = 512
QUERY_COLUMNS = 4096
KEY_COLUMNS = 512
QKV = 5120


def draw_key_cache(key, part):
    first_key = jax.random.fold_in(jax.random.fold_in(key, 11), 0)
    normal_part = jax.random.normal(first_key, (NGROUPS, B_DEV, CACHE_POSITIONS, KEY_COLUMNS), jnp.float32)
    return jnp.clip(normal_part, -6.0, 6.0).astype(jnp.bfloat16)


def draw_lengths(key, part):
    first_key, second_key = jax.random.split(jax.random.fold_in(key, 23))
    base_lengths = jax.random.randint(first_key, (NGROUPS * B_DEV,), 1, CACHE_POSITIONS + 1)
    longest_slot = jax.random.randint(second_key, (), 0, NGROUPS * B_DEV)
    flat_lengths = jnp.where(jnp.arange(NGROUPS * B_DEV) == longest_slot, CACHE_POSITIONS, base_lengths)
    return flat_lengths.reshape(NGROUPS, B_DEV).astype(jnp.int32)


def set_ends(array, stream_key, least, largest):
    longest = array.shape.index(max(array.shape))
    spots = []
    for shift in (0, 1):
        where = [jax.random.randint(jax.random.fold_in(stream_key, axis), (), 0, length) for axis, length in enumerate(array.shape)]
        where[longest] = (where[longest] + shift) % array.shape[longest]
        spots.append(tuple(where))
    return array.at[spots[0]].set(least).at[spots[1]].set(largest)


def steps_of(own_key, extent, pieces, least, top_value):
    level, own = 1.0, jax.random.fold_in(own_key, 6)
    for axis_at, blocks in pieces:
        draws = jnp.exp(jax.random.uniform(jax.random.fold_in(own, axis_at), (blocks,), jnp.float32, least / len(pieces), top_value / len(pieces)))
        level = level * jnp.repeat(draws, extent[axis_at] // blocks).reshape([-1 if axis == axis_at else 1 for axis in range(len(extent))])
    return level


def scatter_about(rng, dims, width, bound, cuts=(), kind=jnp.bfloat16):
    loudness = steps_of(rng, dims, cuts, -0.22, 0.18) if cuts else 1.0
    result = jax.random.normal(rng, dims, jnp.float32) * width * loudness
    return jnp.minimum(jnp.maximum(result, -bound), bound).astype(kind)


def setup_inputs(seed: int = 0) -> dict:
    arg_keys = jax.random.split(jax.random.key(seed), 19)
    hidden_in = scatter_about(arg_keys[0], (B, D), 1.0, 6.0, ((0, 8),))
    attn_gain = jnp.clip(1.0 + 0.1 * jax.random.normal(arg_keys[1], (D,), jnp.float32), 0.5, 1.5)
    w_qkv = set_ends(jax.random.randint(arg_keys[2], (D // 4, QKV), -2147483648, 2147483647), jax.random.fold_in(arg_keys[2], 1), -2147483648, 2147483646).astype(jnp.int32)
    qkv_scale = jnp.clip(jnp.exp(math.log(0.00041926274) - 1.32175583 * jax.random.uniform(arg_keys[3], (QKV,), jnp.float32) ** steps_of(arg_keys[3], (QKV,), ((0, 4),), -0.2, 0.2)), 0.0001118034, 0.00041926274)
    q_gain = jnp.clip(1.0 + 0.15 * jax.random.normal(arg_keys[4], (HEAD_SIZE,), jnp.float32), 0.25, 1.75)
    k_gain = jnp.clip(1.0 + 0.18 * jax.random.normal(arg_keys[5], (HEAD_SIZE,), jnp.float32), 0.1, 1.9)
    key_cache = draw_key_cache(jax.random.fold_in(arg_keys[18], 71), 0)
    value_cache = scatter_about(arg_keys[7], (NGROUPS, B_DEV, CACHE_POSITIONS, KEY_COLUMNS), 1.5, 9.0, ((0, 8), (1, 4)))
    lengths = draw_lengths(jax.random.fold_in(arg_keys[18], 71), 0)
    w_out = set_ends(jax.random.randint(arg_keys[9], (QUERY_COLUMNS // 4, D), -2147483648, 2147483647), jax.random.fold_in(arg_keys[9], 1), -2147483648, 2147483646).astype(jnp.int32)
    out_scale = jnp.clip(jnp.exp(jax.random.uniform(arg_keys[10], (D,), jnp.float32, math.log(0.0003125), math.log(0.00125))), 0.0003125, 0.00125)
    mlp_gain = jnp.clip(1.0 + 0.1 * jax.random.normal(arg_keys[11], (D,), jnp.float32), 0.5, 1.5)
    w_gate = set_ends(jax.random.randint(arg_keys[12], (D // 4, FFW), -2147483648, 2147483647), jax.random.fold_in(arg_keys[12], 1), -2147483648, 2147483646).astype(jnp.int32)
    w_up = set_ends(jax.random.randint(arg_keys[13], (D // 4, FFW), -2147483648, 2147483647), jax.random.fold_in(arg_keys[13], 1), -2147483648, 2147483646).astype(jnp.int32)
    gate_scale = jnp.clip(jnp.exp(math.log(0.00041926274) - 1.32175583 * jax.random.uniform(arg_keys[14], (FFW,), jnp.float32) ** steps_of(arg_keys[14], (FFW,), ((0, 4),), -0.2, 0.2)), 0.0001118034, 0.00041926274)
    up_scale = jnp.clip(jnp.exp(math.log(0.00041926274) - 1.32175583 * jax.random.uniform(arg_keys[15], (FFW,), jnp.float32) ** steps_of(arg_keys[15], (FFW,), ((0, 4),), -0.2, 0.2)), 0.0001118034, 0.00041926274)
    w_down = set_ends(jax.random.randint(arg_keys[16], (FFW // 4, D), -2147483648, 2147483647), jax.random.fold_in(arg_keys[16], 1), -2147483648, 2147483646).astype(jnp.int32)
    down_scale = jnp.clip(jnp.exp(jax.random.uniform(arg_keys[17], (D,), jnp.float32, math.log(0.00013258251), math.log(0.00053033006))), 0.00013258251, 0.00053033006)
    return dict(hidden_in=hidden_in, attn_gain=attn_gain, w_qkv=w_qkv, qkv_scale=qkv_scale, q_gain=q_gain, k_gain=k_gain, key_cache=key_cache, value_cache=value_cache, lengths=lengths, w_out=w_out, out_scale=out_scale, mlp_gain=mlp_gain, w_gate=w_gate, w_up=w_up, gate_scale=gate_scale, up_scale=up_scale, w_down=w_down, down_scale=down_scale)


norm_epsilon = 1e-06
rope_base = 1000000.0

def unpack_bytes(packed, byte_index):
    return jnp.right_shift(jnp.left_shift(packed, 24 - 8 * byte_index), 24)

def byte_product(activations, packed):
    products = [jnp.dot(activations[:, byte_index::4], unpack_bytes(packed, byte_index).astype(jnp.bfloat16), preferred_element_type=jnp.float32) for byte_index in range(4)]
    return products[0] + products[1] + products[2] + products[3]

def normalize_rows(values, gain_row):
    return values * lax.rsqrt(lax.optimization_barrier(jnp.mean(values * values, axis=-1, keepdims=True)) + norm_epsilon) * gain_row

def rotary_embed(values, positions):
    half_dim = values.shape[-1] // 2
    freq_index = jnp.arange(half_dim, dtype=jnp.float32)
    inverse = jnp.exp(freq_index * (-math.log(rope_base) / half_dim))
    angles = positions.astype(jnp.float32)[:, None] * inverse[None, :]
    cosine = jnp.cos(angles)[:, None, :]
    sine_part = jnp.sin(angles)[:, None, :]
    lower_half = values[..., :half_dim]
    upper_half = values[..., half_dim:]
    return jnp.concatenate([lower_half * cosine - upper_half * sine_part, upper_half * cosine + lower_half * sine_part], axis=-1)

def attention_rows(query_key_value, q_gain, k_gain, stored_keys, stored_values, seq_lengths):
    count_of_rows = query_key_value.shape[0]
    query_matrix = query_key_value[:, :QUERY_COLUMNS].astype(jnp.float32).reshape(count_of_rows, QUERY_HEADS, HEAD_SIZE)
    incoming_keys = query_key_value[:, QUERY_COLUMNS:QUERY_COLUMNS + KEY_COLUMNS].astype(jnp.float32).reshape(count_of_rows, KEY_VALUE_HEADS, HEAD_SIZE)
    incoming_values = query_key_value[:, QUERY_COLUMNS + KEY_COLUMNS:].reshape(count_of_rows, KEY_VALUE_HEADS, HEAD_SIZE)
    query_matrix = rotary_embed(normalize_rows(query_matrix, q_gain), seq_lengths).astype(jnp.bfloat16)
    incoming_keys = rotary_embed(normalize_rows(incoming_keys, k_gain), seq_lengths).astype(jnp.bfloat16)
    query_groups = query_matrix.astype(jnp.float32).reshape(count_of_rows, KEY_VALUE_HEADS, QUERY_HEADS // KEY_VALUE_HEADS, HEAD_SIZE)
    key_slices = stored_keys.astype(jnp.float32).reshape(count_of_rows, CACHE_POSITIONS, KEY_VALUE_HEADS, HEAD_SIZE)
    value_slices = stored_values.astype(jnp.float32).reshape(count_of_rows, CACHE_POSITIONS, KEY_VALUE_HEADS, HEAD_SIZE)
    logit_scale = 1.0 / math.sqrt(HEAD_SIZE)
    scores = jnp.einsum('bkgd,bpkd->bkgp', query_groups, key_slices) * logit_scale
    live_mask = jnp.arange(CACHE_POSITIONS, dtype=jnp.int32)[None, :] < seq_lengths[:, None]
    scores = jnp.where(live_mask[:, None, None, :], scores, -jnp.inf)
    self_score = jnp.einsum('nufi,nui->nuf', query_groups, incoming_keys.astype(jnp.float32)) * logit_scale
    row_max = jnp.maximum(lax.optimization_barrier(jnp.max(scores, axis=-1)), self_score)
    soft_weights = jnp.exp(scores - row_max[..., None])
    own_weight = jnp.exp(self_score - row_max)
    denominator = lax.optimization_barrier(jnp.sum(soft_weights, axis=-1)) + own_weight
    soft_low = lax.optimization_barrier(soft_weights.astype(jnp.bfloat16)).astype(jnp.float32)
    own_low = lax.optimization_barrier(own_weight.astype(jnp.bfloat16)).astype(jnp.float32)
    numerator = jnp.einsum('bkgp,bpkd->bkgd', soft_low, value_slices) + own_low[..., None] * incoming_values.astype(jnp.float32)[:, :, None, :]
    return (numerator / denominator[..., None]).reshape(count_of_rows, QUERY_COLUMNS).astype(jnp.bfloat16)

def reference(hidden_in, attn_gain, w_qkv, qkv_scale, q_gain, k_gain, key_cache, value_cache, lengths, w_out, out_scale, mlp_gain, w_gate, w_up, gate_scale, up_scale, w_down, down_scale):
    total_rows = hidden_in.shape[0]
    residual = hidden_in.astype(jnp.float32)
    normed = normalize_rows(residual, attn_gain).astype(jnp.bfloat16)
    query_key_value = (byte_product(normed, w_qkv) * qkv_scale).astype(jnp.bfloat16)
    flat_lengths = lengths.reshape(total_rows)
    heads_out = attention_rows(query_key_value, q_gain, k_gain, key_cache.reshape(total_rows, CACHE_POSITIONS, KEY_COLUMNS), value_cache.reshape(total_rows, CACHE_POSITIONS, KEY_COLUMNS), flat_lengths)
    middle = (residual + byte_product(heads_out, w_out) * out_scale).astype(jnp.bfloat16)
    normed_mlp = normalize_rows(middle.astype(jnp.float32), mlp_gain).astype(jnp.bfloat16)
    gate_value = byte_product(normed_mlp, w_gate) * gate_scale
    up_value = byte_product(normed_mlp, w_up) * up_scale
    activated = (jax.nn.silu(gate_value) * up_value).astype(jnp.bfloat16)
    down_value = byte_product(activated, w_down) * down_scale
    return (middle.astype(jnp.float32) + down_value).astype(jnp.bfloat16)
```

```python
import functools
import math

import jax
import jax.numpy as jnp
from jax import lax
from jax.experimental import pallas as pl
from jax.experimental.pallas import tpu as pltpu
from jax.sharding import PartitionSpec as P

D = 5120
QUERY_HEADS = 32
KEY_VALUE_HEADS = 4
HEAD_SIZE = 128
QUERY_COLUMNS = 4096
KEY_COLUMNS = 512


norm_epsilon = 1e-06
rope_base = 1000000.0


def unpack_bytes(packed, byte_index):
    return jnp.right_shift(jnp.left_shift(packed, 24 - 8 * byte_index), 24)


def byte_order(block):
    source = lax.broadcasted_iota(jnp.int32, (block, block), 0)
    target = lax.broadcasted_iota(jnp.int32, (block, block), 1)
    return (target == (source % 4) * (block // 4) + source // 4).astype(jnp.bfloat16)


def split_kernel(block, x_ref, order_ref, out_ref):
    lanes = block // 4
    for c in range(x_ref.shape[1] // block):
        moved = jnp.dot(
            x_ref[:, c * block : (c + 1) * block],
            order_ref[...],
            preferred_element_type=jnp.float32,
        ).astype(jnp.bfloat16)
        for j in range(4):
            out_ref[j, :, c * lanes : (c + 1) * lanes] = moved[:, j * lanes : (j + 1) * lanes]


def split_bytes(activations):
    rows, width = activations.shape
    if width % 512:
        return [activations[:, byte_index::4] for byte_index in range(4)]
    split = pl.pallas_call(
        functools.partial(split_kernel, 512),
        out_shape=jax.ShapeDtypeStruct((4, rows, width // 4), jnp.bfloat16),
        cost_estimate=pl.CostEstimate(
            flops=2 * rows * width * 512, bytes_accessed=4 * rows * width, transcendentals=0
        ),
        name="split_bytes",
    )(activations, byte_order(512))
    return [split[byte_index] for byte_index in range(4)]


def byte_product(activations, packed):
    pieces = split_bytes(activations)
    products = [
        jnp.dot(
            pieces[byte_index],
            unpack_bytes(packed, byte_index).astype(jnp.bfloat16),
            preferred_element_type=jnp.float32,
        )
        for byte_index in range(4)
    ]
    return products[0] + products[1] + products[2] + products[3]


def block_of(width):
    return math.gcd(640, width)


def order_kernel(block, x_ref, order_ref, out_ref):
    for c in range(x_ref.shape[1] // block):
        out_ref[:, c * block : (c + 1) * block] = jnp.dot(
            x_ref[:, c * block : (c + 1) * block],
            order_ref[...],
            preferred_element_type=jnp.float32,
        ).astype(jnp.bfloat16)


def order_bytes(activations):
    rows, width = activations.shape
    block = block_of(width)
    if block == width:
        return jnp.dot(activations, byte_order(block), preferred_element_type=jnp.float32).astype(
            jnp.bfloat16
        )
    return pl.pallas_call(
        functools.partial(order_kernel, block),
        out_shape=jax.ShapeDtypeStruct((rows, width), jnp.bfloat16),
        cost_estimate=pl.CostEstimate(
            flops=2 * rows * width * block, bytes_accessed=4 * rows * width, transcendentals=0
        ),
        name="order_bytes",
    )(activations, byte_order(block))


def unpack_ordered(packed):
    rows, columns = packed.shape
    block = block_of(4 * rows) // 4
    blocks = packed.reshape(rows // block, block, columns)
    parts = [unpack_bytes(blocks, j).astype(jnp.bfloat16) for j in range(4)]
    return jnp.stack(parts, axis=1).reshape(4 * rows, columns)


def normalize_rows(values, gain_row):
    return (
        values
        * lax.rsqrt(jnp.mean(values * values, axis=-1, keepdims=True) + norm_epsilon)
        * gain_row
    )


def rotary_embed(values, positions):
    half_dim = values.shape[-1] // 2
    freq_index = jnp.arange(half_dim, dtype=jnp.float32)
    inverse = jnp.exp(freq_index * (-math.log(rope_base) / half_dim))
    angles = positions.astype(jnp.float32)[:, None] * inverse[None, :]
    cosine = jnp.cos(angles)[:, None, :]
    sine_part = jnp.sin(angles)[:, None, :]
    lower_half = values[..., :half_dim]
    upper_half = values[..., half_dim:]
    return jnp.concatenate(
        [
            lower_half * cosine - upper_half * sine_part,
            upper_half * cosine + lower_half * sine_part,
        ],
        axis=-1,
    )


def local_attention(query_key_value_rows, q_gain, k_gain, stored_keys, stored_values, seq_lengths):
    count_of_rows = query_key_value_rows.shape[0]
    cache_length = stored_keys.shape[1]
    query_matrix = (
        query_key_value_rows[:, :QUERY_COLUMNS]
        .astype(jnp.float32)
        .reshape(count_of_rows, QUERY_HEADS, HEAD_SIZE)
    )
    incoming_keys = (
        query_key_value_rows[:, QUERY_COLUMNS : QUERY_COLUMNS + KEY_COLUMNS]
        .astype(jnp.float32)
        .reshape(count_of_rows, KEY_VALUE_HEADS, HEAD_SIZE)
    )
    incoming_values = query_key_value_rows[:, QUERY_COLUMNS + KEY_COLUMNS :].reshape(
        count_of_rows, KEY_VALUE_HEADS, HEAD_SIZE
    )
    query_matrix = rotary_embed(normalize_rows(query_matrix, q_gain), seq_lengths).astype(
        jnp.bfloat16
    )
    incoming_keys = rotary_embed(normalize_rows(incoming_keys, k_gain), seq_lengths).astype(
        jnp.bfloat16
    )
    query_groups = query_matrix.reshape(
        count_of_rows, KEY_VALUE_HEADS, QUERY_HEADS // KEY_VALUE_HEADS, HEAD_SIZE
    )
    key_slices = stored_keys.reshape(count_of_rows, cache_length, KEY_VALUE_HEADS, HEAD_SIZE)
    value_slices = stored_values.reshape(count_of_rows, cache_length, KEY_VALUE_HEADS, HEAD_SIZE)
    logit_scale = 1.0 / math.sqrt(HEAD_SIZE)
    scores = (
        jnp.einsum("bkgd,bpkd->bkgp", query_groups, key_slices, preferred_element_type=jnp.float32)
        * logit_scale
    )
    live_mask = jnp.arange(cache_length, dtype=jnp.int32)[None, :] < seq_lengths[:, None]
    scores = jnp.where(live_mask[:, None, None, :], scores, -jnp.inf)
    self_score = (
        jnp.einsum("nufi,nui->nuf", query_groups, incoming_keys, preferred_element_type=jnp.float32)
        * logit_scale
    )
    row_max = jnp.maximum(jnp.max(scores, axis=-1), self_score)
    soft_weights = jnp.exp(scores - row_max[..., None])
    own_weight = jnp.exp(self_score - row_max)
    denominator = jnp.sum(soft_weights, axis=-1) + own_weight
    own_low = lax.optimization_barrier(own_weight.astype(jnp.bfloat16)).astype(jnp.float32)
    numerator = jnp.einsum(
        "bkgp,bpkd->bkgd",
        soft_weights.astype(jnp.bfloat16),
        value_slices,
        preferred_element_type=jnp.float32,
    )
    numerator = numerator + own_low[..., None] * incoming_values.astype(jnp.float32)[:, :, None, :]
    return (
        (numerator / denominator[..., None])
        .reshape(count_of_rows, QUERY_COLUMNS)
        .astype(jnp.bfloat16)
    )


def summed_share(terms, tp_count):
    rows, columns = terms.shape
    pieces = lax.all_to_all(terms, "tp", split_axis=1, concat_axis=0, tiled=True)
    return jnp.sum(
        pieces.reshape(tp_count, rows, columns // tp_count).astype(jnp.float32), axis=0
    )


def gathered_rows(rows, axis):
    count = lax.axis_size(axis)
    copies = jnp.broadcast_to(rows[None], (count, *rows.shape))
    pieces = lax.all_to_all(copies, axis, split_axis=0, concat_axis=0)
    return pieces.reshape(count * rows.shape[0], rows.shape[1])


def summed_rows(terms, axis):
    count = lax.axis_size(axis)
    rows, columns = terms.shape
    pieces = lax.all_to_all(
        terms.reshape(count, rows // count, columns), axis, split_axis=0, concat_axis=0
    )
    return jnp.sum(pieces.astype(jnp.float32), axis=0)


LANES = 128
MESH = pl.DeviceIdType.MESH


def lane_order(block):
    source = lax.broadcasted_iota(jnp.int32, (block, block), 0)
    target = lax.broadcasted_iota(jnp.int32, (block, block), 1)
    return (target == (source % 4) * (block // 4) + source // 4).astype(jnp.bfloat16)


def unpack_slab(packed):
    rows, columns = packed.shape
    slab = LANES // 4
    parts = []
    for k in range(rows // slab):
        words = packed[k * slab : (k + 1) * slab]
        for j in range(4):
            parts.append(unpack_bytes(words, j).astype(jnp.float32).astype(jnp.bfloat16))
    return jnp.concatenate(parts, axis=0)


def mlp_kernel(
    lag,
    x_ref,
    gate_own,
    gate_other,
    up_own,
    up_other,
    down_own,
    down_other,
    gate_scale,
    up_scale,
    down_scale,
    mid_ref,
    order_ref,
    out_ref,
    gate_v,
    up_v,
    down_v,
    x_v,
    partial,
    sum_send,
    sum_recv,
    act,
    total,
    part_send,
    part_recv,
    load_sem,
    sum_send_sem,
    sum_recv_sem,
    act_send_sem,
    act_recv_sem,
    part_send_sem,
    part_recv_sem,
):
    g, t, s = lax.axis_index("grp"), lax.axis_index("tp"), lax.axis_index("src")
    count_g, count_t, count_s = lax.axis_size("grp"), lax.axis_size("tp"), lax.axis_size("src")
    rows = x_ref.shape[0]
    half = rows // 2
    packed_rows, hidden = gate_own.shape
    block = down_own.shape[1]
    chunks = hidden // LANES
    groups = load_sem.shape[1]
    width = hidden // groups
    per_group = chunks // groups
    group_rows = rows // count_s

    def load(array, index):
        source = (gate_own, gate_other, up_own, up_other)[array]
        target = (gate_v, gate_v, up_v, up_v)[array]
        columns = pl.ds(pl.multiple_of(index * width, LANES), width)
        return pltpu.make_async_copy(
            source.at[:, columns], target.at[array % 2, :, columns], load_sem.at[array, index]
        )

    def load_down(index):
        source = (down_own, down_other)[index]
        return pltpu.make_async_copy(source, down_v.at[index], load_sem.at[4 + index, 0])

    for index in range(groups):
        for array in range(4):
            load(array, index).start()
    for index in range(2):
        load_down(index).start()

    barrier = pltpu.get_barrier_semaphore()
    for tt in range(count_t):
        for ss in range(count_s):

            @pl.when((tt != t) | (ss != s))
            def _():
                pl.semaphore_signal(
                    barrier, inc=1, device_id={"tp": tt, "src": ss}, device_id_type=MESH
                )

    total[...] = jnp.zeros_like(total)
    blocks = x_ref.shape[1] // LANES
    stacked = jnp.concatenate(
        [x_ref[:, k * LANES : (k + 1) * LANES] for k in range(blocks)], axis=0
    )
    moved = jnp.dot(stacked, order_ref[...], preferred_element_type=jnp.float32).astype(
        jnp.bfloat16
    )
    for k in range(blocks):
        x_v[:, k * LANES : (k + 1) * LANES] = moved[k * rows : (k + 1) * rows]
    pl.semaphore_wait(barrier, count_t * count_s - 1)

    last = count_s - 1
    far = last * lag
    toward = (s - 1, s + 1)

    def sum_copy(side, j):
        return pltpu.make_async_remote_copy(
            src_ref=sum_send.at[side, j],
            dst_ref=sum_recv.at[side, j],
            send_sem=sum_send_sem.at[side, j],
            recv_sem=sum_recv_sem.at[side, j],
            device_id={"src": toward[side]},
            device_id_type=MESH,
        )

    def act_copy(side, j):
        return pltpu.make_async_remote_copy(
            src_ref=act.at[j, side],
            dst_ref=act.at[j, side],
            send_sem=act_send_sem.at[side, j],
            recv_sem=act_recv_sem.at[side, j],
            device_id={"src": toward[1 - side]},
            device_id_type=MESH,
        )

    def depth_of(side):
        return last - s if side == 0 else s

    def sum_step(side, j):
        depth = depth_of(side)
        at_end = depth == last

        @pl.when(depth > 0)
        def _():
            sum_copy(side, j).wait_recv()

        @pl.when(depth == 0)
        def _():
            sum_send[side, j] = partial[j, side].astype(jnp.bfloat16)
            sum_copy(side, j).start()

        @pl.when((depth > 0) & jnp.logical_not(at_end))
        def _():
            sum_send[side, j] = (
                partial[j, side] + sum_recv[side, j].astype(jnp.float32)
            ).astype(jnp.bfloat16)
            sum_copy(side, j).start()

        @pl.when(at_end)
        def _():
            value = partial[j, side] + sum_recv[side, j].astype(jnp.float32)
            columns = pl.ds(pl.multiple_of(j * LANES, LANES), LANES)
            gate_value = value[:, :LANES] * gate_scale[:, columns]
            up_value = value[:, LANES:] * up_scale[:, columns]
            activated = (gate_value / (1.0 + jnp.exp(-gate_value)) * up_value).astype(jnp.bfloat16)
            act[j, side] = jnp.dot(
                activated, order_ref[...], preferred_element_type=jnp.float32
            ).astype(jnp.bfloat16)
            act_copy(side, j).start()

    def act_step(side, j):
        depth = last - depth_of(side)
        act_copy(side, j).wait_recv()

        @pl.when(depth < last)
        def _():
            act_copy(side, j).start()

    def step(i, carry):
        @pl.when(i < chunks)
        def _():
            @pl.when(lax.rem(i, per_group) == 0)
            def _():
                for array in range(4):
                    load(array, i // per_group).wait()

            columns = pl.ds(pl.multiple_of(i * LANES, LANES), LANES)
            gate_w = [unpack_slab(gate_v[index, :, columns]) for index in range(2)]
            up_w = [unpack_slab(up_v[index, :, columns]) for index in range(2)]
            weights = jnp.concatenate(
                [jnp.concatenate(gate_w, axis=0), jnp.concatenate(up_w, axis=0)], axis=1
            )
            product = jnp.dot(x_v[...], weights, preferred_element_type=jnp.float32)
            partial[i, 0] = product[:half]
            partial[i, 1] = product[half:]

        for side in range(2):
            j = i - depth_of(side) * lag

            @pl.when((j >= 0) & (j < chunks))
            def _():
                sum_step(side, j)

        for side in range(2):
            depth = last - depth_of(side)
            j = i - far - depth * lag

            @pl.when((depth > 0) & (j >= 0) & (j < chunks))
            def _():
                act_step(side, j)

        j = i - far - jnp.maximum(s, last - s) * lag

        @pl.when((j >= 0) & (j < chunks))
        def _():
            @pl.when(j == 0)
            def _():
                for index in range(2):
                    load_down(index).wait()

            slab = LANES // 4
            words = pl.ds(pl.multiple_of(j * slab, slab), slab)
            weights = jnp.concatenate(
                [unpack_slab(down_v[index, words, :]) for index in range(2)], axis=1
            )
            for side in range(2):
                total[side * half : (side + 1) * half] += jnp.dot(
                    act[j, side], weights, preferred_element_type=jnp.float32
                )

        return carry

    lax.fori_loop(0, chunks + 2 * far, step, 0)

    per_share = count_g * count_s // count_t

    def part_copy(index, ss):
        number = jnp.where(index == 0, g, count_g - 1 - g) * count_s + s
        owner = number // per_share
        slot = t * per_share + lax.rem(number, per_share)
        return owner, slot, pltpu.make_async_remote_copy(
            src_ref=part_send.at[index, ss],
            dst_ref=part_recv.at[slot],
            send_sem=part_send_sem.at[index, ss],
            recv_sem=part_recv_sem.at[slot],
            device_id={"tp": owner, "src": ss},
            device_id_type=MESH,
        )

    for shift in range(count_s):
        ss = lax.rem(s + 1 + shift, count_s)
        row = pl.ds(pl.multiple_of(ss * group_rows, group_rows), group_rows)
        for index in range(2):
            owner, slot, copy = part_copy(index, ss)
            piece = total[row, index * block : (index + 1) * block].astype(jnp.bfloat16)
            mine = (owner == t) & (ss == s)

            @pl.when(mine)
            def _():
                part_recv[slot] = piece

            @pl.when(jnp.logical_not(mine))
            def _():
                part_send[index, ss] = piece
                copy.start()

    for slot in range(count_t * per_share):
        number = t * per_share + slot % per_share
        from_me = (slot // per_share == t) & (lax.rem(number, count_s) == s)

        @pl.when(jnp.logical_not(from_me))
        def _():
            pltpu.make_async_remote_copy(
                src_ref=part_send.at[0, 0],
                dst_ref=part_recv.at[slot],
                send_sem=part_send_sem.at[0, 0],
                recv_sem=part_recv_sem.at[slot],
                device_id={"tp": t, "src": s},
                device_id_type=MESH,
            ).wait_recv()

    for place in range(per_share):
        value = part_recv[place].astype(jnp.float32)
        for tt in range(1, count_t):
            value += part_recv[tt * per_share + place].astype(jnp.float32)
        columns = slice(place * block, (place + 1) * block)
        out_ref[:, columns] = (
            mid_ref[:, columns].astype(jnp.float32) + value * down_scale[:, columns]
        ).astype(jnp.bfloat16)

    for ss in range(count_s):
        for index in range(2):
            owner, slot, copy = part_copy(index, ss)

            @pl.when((owner != t) | (ss != s))
            def _():
                copy.wait_send()

    def drain(j, carry):
        for side in range(2):
            depth = depth_of(side)

            @pl.when(depth < last)
            def _():
                sum_copy(side, j).wait_send()

            @pl.when(depth > 0)
            def _():
                act_copy(side, j).wait_send()

        return carry

    lax.fori_loop(0, chunks, drain, 0)


def mlp_block(x, gate, up, down, gate_scale, up_scale, down_scale, mid, lag):
    count_t, count_s = lax.axis_size("tp"), lax.axis_size("src")
    rows, depth = x.shape
    packed_rows, hidden = gate[0].shape
    packed_hidden, block = down[0].shape
    chunks = hidden // LANES
    groups = 5 if chunks % 5 == 0 else 1
    half = rows // 2
    group_rows = rows // count_s
    slots = count_t * (mid.shape[1] // block)
    bf16, f32 = jnp.bfloat16, jnp.float32
    vmem = pl.BlockSpec(memory_space=pltpu.VMEM)
    hbm = pl.BlockSpec(memory_space=pl.ANY)
    return pl.pallas_call(
        functools.partial(mlp_kernel, lag),
        out_shape=jax.ShapeDtypeStruct(mid.shape, bf16),
        in_specs=[vmem] + [hbm] * 6 + [vmem] * 5,
        out_specs=vmem,
        scratch_shapes=[
            pltpu.VMEM((2, packed_rows, hidden), jnp.int32),
            pltpu.VMEM((2, packed_rows, hidden), jnp.int32),
            pltpu.VMEM((2, packed_hidden, block), jnp.int32),
            pltpu.VMEM((rows, depth), bf16),
            pltpu.VMEM((chunks, 2, half, 2 * LANES), f32),
            pltpu.VMEM((2, chunks, half, 2 * LANES), bf16),
            pltpu.VMEM((2, chunks, half, 2 * LANES), bf16),
            pltpu.VMEM((chunks, 2, half, LANES), bf16),
            pltpu.VMEM((rows, depth), f32),
            pltpu.VMEM((2, count_s, group_rows, block), bf16),
            pltpu.VMEM((slots, group_rows, block), bf16),
            pltpu.SemaphoreType.DMA((6, groups)),
            pltpu.SemaphoreType.DMA((2, chunks)),
            pltpu.SemaphoreType.DMA((2, chunks)),
            pltpu.SemaphoreType.DMA((2, chunks)),
            pltpu.SemaphoreType.DMA((2, chunks)),
            pltpu.SemaphoreType.DMA((2, count_s)),
            pltpu.SemaphoreType.DMA((slots,)),
        ],
        compiler_params=pltpu.CompilerParams(
            collective_id=1, has_side_effects=True, vmem_limit_bytes=56 * 1024 * 1024
        ),
        cost_estimate=pl.CostEstimate(
            flops=2 * rows * depth * hidden * 3,
            bytes_accessed=4 * 3 * 2 * packed_rows * hidden,
            transcendentals=rows * hidden,
        ),
        name="mlp_block",
    )(x, *gate, *up, *down, gate_scale, up_scale, down_scale, mid, lane_order(LANES))


def fast_mlp(grp, tp, src, args):
    w_gate, w_down, hidden_in = args
    rows = hidden_in.shape[0]
    return (
        grp == 2
        and src > 1
        and (grp * src) % tp == 0
        and w_gate.shape[0] % 32 == 0
        and w_gate.shape[1] % LANES == 0
        and w_down.shape[1] % LANES == 0
        and rows % 16 == 0
        and (rows * src) % 32 == 0
    )


def local(
    hidden_in,
    attn_gain,
    w_qkv,
    qkv_scale,
    q_gain,
    k_gain,
    key_cache,
    value_cache,
    lengths,
    w_out,
    out_scale,
    mlp_gain,
    w_gate,
    w_up,
    gate_scale,
    up_scale,
    w_down,
    down_scale,
):
    tp_count = lax.axis_size("tp")
    tp_index = lax.axis_index("tp")
    share_cols = D // tp_count
    residual = hidden_in.astype(jnp.float32)
    normed = normalize_rows(residual, attn_gain).astype(jnp.bfloat16)
    qkv_part = (byte_product(normed, w_qkv) * qkv_scale).astype(jnp.bfloat16)
    query_key_value_rows = lax.all_to_all(qkv_part, "tp", split_axis=0, concat_axis=1, tiled=True)
    heads_out = local_attention(
        query_key_value_rows, q_gain, k_gain, key_cache[0], value_cache[0], lengths[0]
    )
    head_rows = lax.all_to_all(heads_out, "tp", split_axis=1, concat_axis=0, tiled=True)
    partial_value = (byte_product(head_rows, w_out) * out_scale).astype(jnp.bfloat16)
    residual_share = lax.dynamic_slice_in_dim(hidden_in, tp_index * share_cols, share_cols, 1)
    mid_share = (
        residual_share.astype(jnp.float32) + summed_share(partial_value, tp_count)
    ).astype(jnp.bfloat16)
    mid_full = lax.all_gather(mid_share, "tp", axis=1, tiled=True)
    normed_mlp = normalize_rows(mid_full.astype(jnp.float32), mlp_gain).astype(jnp.bfloat16)
    if fast_mlp(lax.axis_size("grp"), tp_count, lax.axis_size("src"), (w_gate, w_down, hidden_in)):
        g = lax.axis_index("grp")
        count_s = lax.axis_size("src")
        rows = hidden_in.shape[0]
        swap = [(0, 1), (1, 0)]
        gate = (w_gate, lax.ppermute(w_gate, "grp", swap))
        up = (w_up, lax.ppermute(w_up, "grp", swap))
        down = (w_down, lax.ppermute(w_down, "grp", swap))
        width = D // 2
        own = lax.dynamic_slice_in_dim(normed_mlp, g * width, width, 1)
        other = lax.dynamic_slice_in_dim(normed_mlp, (1 - g) * width, width, 1)
        both = jnp.concatenate(
            [own.reshape(rows, count_s, -1), other.reshape(rows, count_s, -1)], axis=2
        )
        x = lax.all_to_all(both, "src", split_axis=1, concat_axis=0, tiled=True)
        x = x.reshape(rows * count_s, -1)
        down_share = lax.dynamic_slice_in_dim(down_scale, tp_index * share_cols, share_cols, 0)
        return mlp_block(
            x,
            gate,
            up,
            down,
            gate_scale[None],
            up_scale[None],
            down_share[None],
            mid_share,
            2,
        )
    mlp_columns = order_bytes(
        lax.all_to_all(normed_mlp, ("grp", "src"), split_axis=1, concat_axis=0, tiled=True)
    )
    gate_terms = jnp.dot(mlp_columns, unpack_ordered(w_gate), preferred_element_type=jnp.float32)
    up_terms = jnp.dot(mlp_columns, unpack_ordered(w_up), preferred_element_type=jnp.float32)
    both_terms = jnp.concatenate(
        [gate_terms.astype(jnp.bfloat16), up_terms.astype(jnp.bfloat16)], axis=1
    )
    both = summed_rows(summed_rows(both_terms, "grp").astype(jnp.bfloat16), "src")
    hidden = gate_scale.shape[0]
    gate_value = both[:, :hidden] * gate_scale
    up_value = both[:, hidden:] * up_scale
    activated = order_bytes((jax.nn.silu(gate_value) * up_value).astype(jnp.bfloat16))
    all_activated = gathered_rows(gathered_rows(activated, "src"), "grp")
    down_columns = jnp.dot(
        all_activated, unpack_ordered(w_down), preferred_element_type=jnp.float32
    ).astype(jnp.bfloat16)
    down_rows = lax.all_to_all(
        down_columns, ("grp", "src"), split_axis=0, concat_axis=1, tiled=True
    )
    down_share = lax.dynamic_slice_in_dim(down_scale, tp_index * share_cols, share_cols, 0)
    mlp_share = summed_share(down_rows, tp_count) * down_share
    return (mid_share.astype(jnp.float32) + mlp_share).astype(jnp.bfloat16)


def solution(mesh):
    return jax.shard_map(
        local,
        mesh=mesh,
        in_specs=(
            P(("grp", "src"), None),
            P(),
            P(None, "tp"),
            P("tp"),
            P(),
            P(),
            P(("grp", "src"), "tp", None, None),
            P(("grp", "src"), "tp", None, None),
            P(("grp", "src"), "tp"),
            P("tp", None),
            P(),
            P(),
            P(("grp", "src"), "tp"),
            P(("grp", "src"), "tp"),
            P("tp"),
            P("tp"),
            P("tp", ("grp", "src")),
            P(),
        ),
        out_specs=P(("grp", "src"), "tp"),
        check_vma=False,
    )
```

```python
import functools
import math

import jax
import jax.numpy as jnp
from jax import lax
from jax.experimental import pallas as pl
from jax.experimental.pallas import tpu as pltpu
from jax.sharding import PartitionSpec as P

D = 5120
QUERY_HEADS = 32
KEY_VALUE_HEADS = 4
HEAD_SIZE = 128
QUERY_COLUMNS = 4096
KEY_COLUMNS = 512


norm_epsilon = 1e-06
rope_base = 1000000.0


def unpack_bytes(packed, byte_index):
    return jnp.right_shift(jnp.left_shift(packed, 24 - 8 * byte_index), 24)


def byte_order(block):
    source = lax.broadcasted_iota(jnp.int32, (block, block), 0)
    target = lax.broadcasted_iota(jnp.int32, (block, block), 1)
    return (target == (source % 4) * (block // 4) + source // 4).astype(jnp.bfloat16)


def split_kernel(block, x_ref, order_ref, out_ref):
    lanes = block // 4
    for c in range(x_ref.shape[1] // block):
        moved = jnp.dot(
            x_ref[:, c * block : (c + 1) * block],
            order_ref[...],
            preferred_element_type=jnp.float32,
        ).astype(jnp.bfloat16)
        for j in range(4):
            out_ref[j, :, c * lanes : (c + 1) * lanes] = moved[:, j * lanes : (j + 1) * lanes]


def split_bytes(activations):
    rows, width = activations.shape
    if width % 512:
        return [activations[:, byte_index::4] for byte_index in range(4)]
    split = pl.pallas_call(
        functools.partial(split_kernel, 512),
        out_shape=jax.ShapeDtypeStruct((4, rows, width // 4), jnp.bfloat16),
        cost_estimate=pl.CostEstimate(
            flops=2 * rows * width * 512, bytes_accessed=4 * rows * width, transcendentals=0
        ),
        name="split_bytes",
    )(activations, byte_order(512))
    return [split[byte_index] for byte_index in range(4)]


def byte_product(activations, packed):
    pieces = split_bytes(activations)
    products = [
        jnp.dot(
            pieces[byte_index],
            unpack_bytes(packed, byte_index).astype(jnp.bfloat16),
            preferred_element_type=jnp.float32,
        )
        for byte_index in range(4)
    ]
    return products[0] + products[1] + products[2] + products[3]


def block_of(width):
    return math.gcd(640, width)


def order_kernel(block, x_ref, order_ref, out_ref):
    for c in range(x_ref.shape[1] // block):
        out_ref[:, c * block : (c + 1) * block] = jnp.dot(
            x_ref[:, c * block : (c + 1) * block],
            order_ref[...],
            preferred_element_type=jnp.float32,
        ).astype(jnp.bfloat16)


def order_bytes(activations):
    rows, width = activations.shape
    block = block_of(width)
    if block == width:
        return jnp.dot(activations, byte_order(block), preferred_element_type=jnp.float32).astype(
            jnp.bfloat16
        )
    return pl.pallas_call(
        functools.partial(order_kernel, block),
        out_shape=jax.ShapeDtypeStruct((rows, width), jnp.bfloat16),
        cost_estimate=pl.CostEstimate(
            flops=2 * rows * width * block, bytes_accessed=4 * rows * width, transcendentals=0
        ),
        name="order_bytes",
    )(activations, byte_order(block))


def unpack_ordered(packed):
    rows, columns = packed.shape
    block = block_of(4 * rows) // 4
    blocks = packed.reshape(rows // block, block, columns)
    parts = [unpack_bytes(blocks, j).astype(jnp.bfloat16) for j in range(4)]
    return jnp.stack(parts, axis=1).reshape(4 * rows, columns)


def normalize_rows(values, gain_row):
    return (
        values
        * lax.rsqrt(jnp.mean(values * values, axis=-1, keepdims=True) + norm_epsilon)
        * gain_row
    )


def rotary_embed(values, positions):
    half_dim = values.shape[-1] // 2
    freq_index = jnp.arange(half_dim, dtype=jnp.float32)
    inverse = jnp.exp(freq_index * (-math.log(rope_base) / half_dim))
    angles = positions.astype(jnp.float32)[:, None] * inverse[None, :]
    cosine = jnp.cos(angles)[:, None, :]
    sine_part = jnp.sin(angles)[:, None, :]
    lower_half = values[..., :half_dim]
    upper_half = values[..., half_dim:]
    return jnp.concatenate(
        [
            lower_half * cosine - upper_half * sine_part,
            upper_half * cosine + lower_half * sine_part,
        ],
        axis=-1,
    )


def local_attention(query_key_value_rows, q_gain, k_gain, stored_keys, stored_values, seq_lengths):
    count_of_rows = query_key_value_rows.shape[0]
    cache_length = stored_keys.shape[1]
    query_matrix = (
        query_key_value_rows[:, :QUERY_COLUMNS]
        .astype(jnp.float32)
        .reshape(count_of_rows, QUERY_HEADS, HEAD_SIZE)
    )
    incoming_keys = (
        query_key_value_rows[:, QUERY_COLUMNS : QUERY_COLUMNS + KEY_COLUMNS]
        .astype(jnp.float32)
        .reshape(count_of_rows, KEY_VALUE_HEADS, HEAD_SIZE)
    )
    incoming_values = query_key_value_rows[:, QUERY_COLUMNS + KEY_COLUMNS :].reshape(
        count_of_rows, KEY_VALUE_HEADS, HEAD_SIZE
    )
    query_matrix = rotary_embed(normalize_rows(query_matrix, q_gain), seq_lengths).astype(
        jnp.bfloat16
    )
    incoming_keys = rotary_embed(normalize_rows(incoming_keys, k_gain), seq_lengths).astype(
        jnp.bfloat16
    )
    query_groups = query_matrix.reshape(
        count_of_rows, KEY_VALUE_HEADS, QUERY_HEADS // KEY_VALUE_HEADS, HEAD_SIZE
    )
    key_slices = stored_keys.reshape(count_of_rows, cache_length, KEY_VALUE_HEADS, HEAD_SIZE)
    value_slices = stored_values.reshape(count_of_rows, cache_length, KEY_VALUE_HEADS, HEAD_SIZE)
    logit_scale = 1.0 / math.sqrt(HEAD_SIZE)
    scores = (
        jnp.einsum("bkgd,bpkd->bkgp", query_groups, key_slices, preferred_element_type=jnp.float32)
        * logit_scale
    )
    live_mask = jnp.arange(cache_length, dtype=jnp.int32)[None, :] < seq_lengths[:, None]
    scores = jnp.where(live_mask[:, None, None, :], scores, -jnp.inf)
    self_score = (
        jnp.einsum("nufi,nui->nuf", query_groups, incoming_keys, preferred_element_type=jnp.float32)
        * logit_scale
    )
    row_max = jnp.maximum(jnp.max(scores, axis=-1), self_score)
    soft_weights = jnp.exp(scores - row_max[..., None])
    own_weight = jnp.exp(self_score - row_max)
    denominator = jnp.sum(soft_weights, axis=-1) + own_weight
    own_low = lax.optimization_barrier(own_weight.astype(jnp.bfloat16)).astype(jnp.float32)
    numerator = jnp.einsum(
        "bkgp,bpkd->bkgd",
        soft_weights.astype(jnp.bfloat16),
        value_slices,
        preferred_element_type=jnp.float32,
    )
    numerator = numerator + own_low[..., None] * incoming_values.astype(jnp.float32)[:, :, None, :]
    return (
        (numerator / denominator[..., None])
        .reshape(count_of_rows, QUERY_COLUMNS)
        .astype(jnp.bfloat16)
    )


def summed_share(terms, tp_count):
    rows, columns = terms.shape
    pieces = lax.all_to_all(terms, "tp", split_axis=1, concat_axis=0, tiled=True)
    return jnp.sum(
        pieces.reshape(tp_count, rows, columns // tp_count).astype(jnp.float32), axis=0
    )


def gathered_rows(rows, axis):
    count = lax.axis_size(axis)
    copies = jnp.broadcast_to(rows[None], (count, *rows.shape))
    pieces = lax.all_to_all(copies, axis, split_axis=0, concat_axis=0)
    return pieces.reshape(count * rows.shape[0], rows.shape[1])


def summed_rows(terms, axis):
    count = lax.axis_size(axis)
    rows, columns = terms.shape
    pieces = lax.all_to_all(
        terms.reshape(count, rows // count, columns), axis, split_axis=0, concat_axis=0
    )
    return jnp.sum(pieces.astype(jnp.float32), axis=0)


LANES = 128
MESH = pl.DeviceIdType.MESH


def lane_order(block):
    source = lax.broadcasted_iota(jnp.int32, (block, block), 0)
    target = lax.broadcasted_iota(jnp.int32, (block, block), 1)
    return (target == (source % 4) * (block // 4) + source // 4).astype(jnp.bfloat16)


def unpack_slab(packed):
    rows, columns = packed.shape
    slab = LANES // 4
    parts = []
    for k in range(rows // slab):
        words = packed[k * slab : (k + 1) * slab]
        for j in range(4):
            parts.append(unpack_bytes(words, j).astype(jnp.float32).astype(jnp.bfloat16))
    return jnp.concatenate(parts, axis=0)


def stack_lanes(values):
    blocks = values.shape[1] // LANES
    return jnp.concatenate([values[:, k * LANES : (k + 1) * LANES] for k in range(blocks)], axis=0)


def ordered(stacked, order_ref):
    return jnp.dot(stacked, order_ref[...], preferred_element_type=jnp.float32).astype(jnp.bfloat16)


def row_of(ref):
    return ref[...].reshape(1, ref.shape[0])


def attention_phase(here, inputs, mlp_buffers, scratch, sems):
    g, t, s, count_g, count_t, count_s = here
    (
        hidden_ref,
        attn_gain,
        w_qkv,
        qkv_scale,
        q_gain,
        k_gain,
        keys,
        values,
        lengths,
        w_out,
        out_scale,
        mlp_gain,
        weights,
        order_ref,
    ) = inputs
    gate_v, up_v, down_v, x_v, mid_v = mlp_buffers
    (
        qkv_w,
        out_w,
        out_u,
        keys_v,
        values_v,
        normed_v,
        qkv_acc,
        qkv_send,
        qkv_recv,
        q_v,
        own_v,
        score_v,
        own_e_v,
        denom_v,
        attn_v,
        attn_send,
        attn_recv,
        proj_v,
        proj_recv,
        mid_send,
        x_send,
    ) = scratch
    (
        qkv_w_sem,
        out_w_sem,
        cache_sem,
        swap_send_sem,
        swap_recv_sem,
        load_sem,
        qkv_send_sem,
        qkv_recv_sem,
        attn_send_sem,
        attn_recv_sem,
        proj_send_sem,
        proj_recv_sem,
        mid_send_sem,
        mid_recv_sem,
        z_send_sem,
        x_send_sem,
        x_recv_sem,
    ) = sems
    f32, bf16 = jnp.float32, jnp.bfloat16
    rows, model = hidden_ref.shape
    mine = rows // count_t
    qkv_columns = w_qkv.shape[1]
    steps = qkv_w_sem.shape[0]
    step_rows = w_qkv.shape[0] // steps
    out_steps = out_w_sem.shape[0]
    out_width = model // out_steps
    share = model // count_t
    positions = keys_v.shape[1]
    heads = QUERY_HEADS
    per_kv = QUERY_HEADS // KEY_VALUE_HEADS
    heads_t = heads // count_t

    def qkv_load(i):
        part = pl.ds(pl.multiple_of(i * step_rows, step_rows), step_rows)
        return pltpu.make_async_copy(w_qkv.at[part, :], qkv_w.at[part, :], qkv_w_sem.at[i])

    def out_load(i):
        part = pl.ds(pl.multiple_of(i * out_width, LANES), out_width)
        return pltpu.make_async_copy(w_out.at[:, part], out_w.at[:, part], out_w_sem.at[i])

    for i in range(steps):
        qkv_load(i).start()
    cache = [
        pltpu.make_async_copy(keys.at[0], keys_v, cache_sem.at[0]),
        pltpu.make_async_copy(values.at[0], values_v, cache_sem.at[1]),
    ]
    for copy in cache:
        copy.start()
    for i in range(out_steps):
        out_load(i).start()

    barrier = pltpu.get_barrier_semaphore()
    for tt in range(count_t):
        for ss in range(count_s):

            @pl.when((tt != t) | (ss != s))
            def _():
                pl.semaphore_signal(
                    barrier, inc=1, device_id={"tp": tt, "src": ss}, device_id_type=MESH
                )

    pl.semaphore_signal(barrier, inc=1, device_id={"grp": 1 - g}, device_id_type=MESH)

    normed = normalize_rows(hidden_ref[...].astype(f32), row_of(attn_gain)).astype(bf16)
    moved = ordered(stack_lanes(normed), order_ref)
    for k in range(model // LANES):
        normed_v[:, k * LANES : (k + 1) * LANES] = moved[k * rows : (k + 1) * rows]
    pl.semaphore_wait(barrier, count_t * count_s)

    swaps = [
        pltpu.make_async_remote_copy(
            src_ref=source,
            dst_ref=target.at[1],
            send_sem=swap_send_sem.at[index],
            recv_sem=swap_recv_sem.at[index],
            device_id={"grp": 1 - g},
            device_id_type=MESH,
        )
        for index, (source, target) in enumerate(zip(weights, (gate_v, up_v, down_v)))
    ]
    loads = [
        pltpu.make_async_copy(source, target.at[0], load_sem.at[index])
        for index, (source, target) in enumerate(zip(weights, (gate_v, up_v, down_v)))
    ]

    qkv_acc[...] = jnp.zeros_like(qkv_acc)

    def qkv_step(i, carry):
        qkv_load(i).wait()
        part = pl.ds(pl.multiple_of(i * step_rows, step_rows), step_rows)
        depth = pl.ds(pl.multiple_of(i * 4 * step_rows, LANES), 4 * step_rows)
        qkv_acc[...] += jnp.dot(
            normed_v[:, depth], unpack_slab(qkv_w[part, :]), preferred_element_type=f32
        )
        return carry

    lax.fori_loop(0, steps, qkv_step, 0)
    for copy in swaps + loads:
        copy.start()
    qkv_send[...] = (qkv_acc[...] * row_of(qkv_scale)).astype(bf16)

    def peer_of(shift):
        return lax.rem(t + shift, count_t)

    def rows_of(index):
        return pl.ds(pl.multiple_of(index * mine, mine), mine)

    def qkv_copy(peer, slot):
        return pltpu.make_async_remote_copy(
            src_ref=qkv_send.at[rows_of(peer), :],
            dst_ref=qkv_recv.at[slot],
            send_sem=qkv_send_sem.at[peer],
            recv_sem=qkv_recv_sem.at[slot],
            device_id={"tp": peer},
            device_id_type=MESH,
        )

    for shift in range(1, count_t):
        qkv_copy(peer_of(shift), t).start()
    qkv_recv[t] = qkv_send[rows_of(t), :]

    def unpack_out(i, carry):
        out_load(i).wait()
        part = pl.ds(pl.multiple_of(i * out_width, LANES), out_width)
        out_u[:, part] = unpack_slab(out_w[:, part])
        return carry

    lax.fori_loop(0, out_steps, unpack_out, 0)

    row_index = lax.broadcasted_iota(jnp.int32, (mine, HEAD_SIZE), 0)
    lane = lax.broadcasted_iota(jnp.int32, (mine, HEAD_SIZE), 1)
    place = jnp.zeros((mine, HEAD_SIZE), f32)
    for b in range(mine):
        place = jnp.where(row_index == b, lengths[0, b].astype(f32), place)
    half_dim = HEAD_SIZE // 2
    low = lane < half_dim
    frequency = jnp.where(low, lane, lane - half_dim).astype(f32)
    angle = place * jnp.exp(frequency * (-math.log(rope_base) / half_dim))
    cosine = jnp.cos(angle)
    sine = jnp.sin(angle)
    sine = jnp.where(low, -sine, sine)

    for shift in range(1, count_t):
        qkv_copy(t, peer_of(shift)).wait_recv()

    per_share = qkv_columns // HEAD_SIZE

    def head_of(h):
        column = (h % per_share) * HEAD_SIZE
        return qkv_recv[h // per_share, :, column : column + HEAD_SIZE]

    def turned(h, gain):
        value = normalize_rows(head_of(h).astype(f32), gain)
        other = pltpu.roll(value, half_dim, 1)
        return (value * cosine + other * sine).astype(bf16).astype(f32)

    logit_scale = 1.0 / math.sqrt(HEAD_SIZE)
    q_row, k_row = row_of(q_gain), row_of(k_gain)
    for kv in range(KEY_VALUE_HEADS):
        new_key = turned(heads + kv, k_row)
        for h in range(kv * per_kv, (kv + 1) * per_kv):
            query = turned(h, q_row)
            q_v[h * mine : (h + 1) * mine] = query
            own = jnp.sum(query * new_key, axis=1, keepdims=True) * logit_scale
            own_v[h * mine : (h + 1) * mine] = jnp.broadcast_to(own, (mine, HEAD_SIZE))
    for copy in cache:
        copy.wait()

    zeros = jnp.zeros((per_kv, HEAD_SIZE), f32)
    for b in range(mine):
        query = q_v[pl.ds(b, heads, stride=mine), :]
        spread = jnp.concatenate(
            [
                jnp.concatenate(
                    [
                        query[kv * per_kv : (kv + 1) * per_kv] if kv == place_of else zeros
                        for place_of in range(KEY_VALUE_HEADS)
                    ],
                    axis=1,
                )
                for kv in range(KEY_VALUE_HEADS)
            ],
            axis=0,
        ).astype(bf16)
        score_v[b * heads : (b + 1) * heads] = lax.dot_general(
            spread, keys_v[b], (((1,), (1,)), ((), ())), preferred_element_type=f32
        )
    position = lax.broadcasted_iota(jnp.int32, (heads, positions), 1)
    for b in range(mine):
        strided = pl.ds(b, heads, stride=mine)
        scores = score_v[b * heads : (b + 1) * heads] * logit_scale
        scores = jnp.where(position < lengths[0, b], scores, -jnp.inf)
        own = own_v[strided, :][:, :1]
        top = jnp.maximum(jnp.max(scores, axis=1, keepdims=True), own)
        weight = jnp.exp(scores - top)
        own_e = jnp.exp(own - top)
        denominator = jnp.sum(weight, axis=1, keepdims=True) + own_e
        score_v[b * heads : (b + 1) * heads] = weight
        own_e_v[strided, :] = jnp.broadcast_to(own_e, (heads, HEAD_SIZE))
        denom_v[strided, :] = jnp.broadcast_to(denominator, (heads, HEAD_SIZE))
    for b in range(mine):
        mixed = jnp.dot(
            score_v[b * heads : (b + 1) * heads].astype(bf16),
            values_v[b],
            preferred_element_type=f32,
        )
        attn_v[pl.ds(b, heads, stride=mine), :] = jnp.concatenate(
            [
                mixed[kv * per_kv : (kv + 1) * per_kv, kv * HEAD_SIZE : (kv + 1) * HEAD_SIZE]
                for kv in range(KEY_VALUE_HEADS)
            ],
            axis=0,
        )
    finished = []
    for h in range(heads):
        part = slice(h * mine, (h + 1) * mine)
        new_value = head_of(heads + KEY_VALUE_HEADS + h // per_kv).astype(f32)
        own_low = own_e_v[part].astype(bf16).astype(f32)
        finished.append(((attn_v[part] + own_low * new_value) / denom_v[part]).astype(bf16))
    attn_send[...] = ordered(jnp.concatenate(finished, axis=0), order_ref)

    head_rows = heads_t * mine

    def attn_copy(peer, slot):
        return pltpu.make_async_remote_copy(
            src_ref=attn_send.at[pl.ds(pl.multiple_of(peer * head_rows, head_rows), head_rows), :],
            dst_ref=attn_recv.at[slot],
            send_sem=attn_send_sem.at[peer],
            recv_sem=attn_recv_sem.at[slot],
            device_id={"tp": peer},
            device_id_type=MESH,
        )

    for shift in range(1, count_t):
        attn_copy(peer_of(shift), t).start()
    attn_recv[t] = attn_send[pl.ds(pl.multiple_of(t * head_rows, head_rows), head_rows), :]
    for shift in range(1, count_t):
        attn_copy(t, peer_of(shift)).wait_recv()

    def proj_copy(peer, slot, i):
        part = pl.ds(pl.multiple_of(i * out_width, LANES), out_width)
        return pltpu.make_async_remote_copy(
            src_ref=proj_v.at[rows_of(peer), part],
            dst_ref=proj_recv.at[slot, :, part],
            send_sem=proj_send_sem.at[peer, i],
            recv_sem=proj_recv_sem.at[slot, i],
            device_id={"tp": peer},
            device_id_type=MESH,
        )

    def out_step(i, carry):
        part = pl.ds(pl.multiple_of(i * out_width, LANES), out_width)
        left = jnp.concatenate(
            [
                jnp.concatenate(
                    [attn_recv[tt, h * mine : (h + 1) * mine] for tt in range(count_t)], axis=0
                )
                for h in range(heads_t)
            ],
            axis=1,
        )
        product = jnp.dot(left, out_u[:, part], preferred_element_type=f32)
        proj_v[:, part] = (product * out_scale[part].reshape(1, out_width)).astype(bf16)
        for shift in range(1, count_t):
            proj_copy(peer_of(shift), t, i).start()
        return carry

    lax.fori_loop(0, out_steps, out_step, 0)

    total = hidden_ref[rows_of(t), :].astype(f32) + proj_v[rows_of(t), :].astype(f32)
    for shift in range(1, count_t):
        slot = peer_of(shift)

        def wait_part(i, carry):
            proj_copy(t, slot, i).wait_recv()
            return carry

        lax.fori_loop(0, out_steps, wait_part, 0)
        total += proj_recv[slot].astype(f32)
    mid = total.astype(bf16)
    for tt in range(count_t):
        mid_send[tt] = mid[:, tt * share : (tt + 1) * share]
    moved = ordered(
        stack_lanes(normalize_rows(mid.astype(f32), row_of(mlp_gain)).astype(bf16)), order_ref
    )
    block = model // (count_g * count_s) // LANES
    for number in range(count_g * count_s):
        owner = number % count_s
        first = jnp.where(number // count_s == g, 0, block)
        for k in range(block):
            column = pl.multiple_of((first + k) * LANES, LANES)
            source = number * block + k
            x_send[owner, :, pl.ds(column, LANES)] = moved[source * mine : (source + 1) * mine]

    def x_rows(ss, tt):
        return pl.ds(pl.multiple_of((ss * count_t + tt) * mine, mine), mine)

    def z_copy(peer, ss):
        return pltpu.make_async_remote_copy(
            src_ref=x_send.at[peer],
            dst_ref=x_v.at[x_rows(ss, t), :],
            send_sem=z_send_sem.at[peer],
            recv_sem=x_recv_sem.at[ss, t],
            device_id={"src": peer},
            device_id_type=MESH,
        )

    def x_copy(peer, ss, tt):
        return pltpu.make_async_remote_copy(
            src_ref=x_v.at[x_rows(ss, tt), :],
            dst_ref=x_v.at[x_rows(ss, tt), :],
            send_sem=x_send_sem.at[ss, peer],
            recv_sem=x_recv_sem.at[ss, tt],
            device_id={"tp": peer},
            device_id_type=MESH,
        )

    def own_copy(peer):
        return pltpu.make_async_remote_copy(
            src_ref=x_send.at[s],
            dst_ref=x_v.at[x_rows(s, t), :],
            send_sem=x_send_sem.at[s, peer],
            recv_sem=x_recv_sem.at[s, t],
            device_id={"tp": peer},
            device_id_type=MESH,
        )

    def mid_copy(peer, slot):
        return pltpu.make_async_remote_copy(
            src_ref=mid_send.at[peer],
            dst_ref=mid_v.at[rows_of(slot), :],
            send_sem=mid_send_sem.at[peer],
            recv_sem=mid_recv_sem.at[slot],
            device_id={"tp": peer},
            device_id_type=MESH,
        )

    for shift in range(1, count_s):
        z_copy(lax.rem(s + shift, count_s), s).start()
    for shift in range(1, count_t):
        own_copy(peer_of(shift)).start()
    x_v[x_rows(s, t), :] = x_send[s]
    for shift in range(1, count_s):
        ss = lax.rem(s + shift, count_s)
        z_copy(s, ss).wait_recv()
        for turn in range(1, count_t):
            x_copy(peer_of(turn), ss, t).start()
    for shift in range(1, count_t):
        mid_copy(peer_of(shift), t).start()
    mid_v[rows_of(t), :] = mid_send[t]
    for ss in range(count_s):
        for turn in range(1, count_t):
            x_copy(t, ss, peer_of(turn)).wait_recv()

    def finish():
        for shift in range(1, count_t):
            peer = peer_of(shift)
            qkv_copy(peer, t).wait_send()
            attn_copy(peer, t).wait_send()
            mid_copy(peer, t).wait_send()

            def wait_part(i, carry):
                proj_copy(peer, t, i).wait_send()
                return carry

            lax.fori_loop(0, out_steps, wait_part, 0)
            for ss in range(count_s):
                x_copy(peer, ss, t).wait_send()
        for shift in range(1, count_s):
            z_copy(lax.rem(s + shift, count_s), s).wait_send()
        for copy in swaps:
            copy.wait_send()

    def mid_wait():
        for shift in range(1, count_t):
            mid_copy(t, peer_of(shift)).wait_recv()

    return swaps, loads, mid_wait, finish


def mlp_phase(here, lag, scales, mlp_buffers, scratch, sems, attention, out_ref):
    g, t, s, count_g, count_t, count_s = here
    gate_scale, up_scale, down_scale, order_ref = scales
    gate_v, up_v, down_v, x_v, mid_v = mlp_buffers
    partial, sum_recv, act, total, part_send, part_recv = scratch
    (
        sum_send_sem,
        sum_recv_sem,
        act_send_sem,
        act_recv_sem,
        part_send_sem,
        part_recv_sem,
    ) = sems
    swaps, loads, mid_wait, finish = attention
    rows = x_v.shape[0]
    half = rows // 2
    hidden = gate_v.shape[2]
    block = down_v.shape[2]
    chunks = hidden // LANES
    group_rows = rows // count_s
    total[...] = jnp.zeros_like(total)

    last = count_s - 1
    far = last * lag
    toward = (s - 1, s + 1)

    def sum_copy(side, j):
        return pltpu.make_async_remote_copy(
            src_ref=partial.at[j, side],
            dst_ref=sum_recv.at[side, j],
            send_sem=sum_send_sem.at[side, j],
            recv_sem=sum_recv_sem.at[side, j],
            device_id={"src": toward[side]},
            device_id_type=MESH,
        )

    def act_copy(side, j):
        return pltpu.make_async_remote_copy(
            src_ref=act.at[j, side],
            dst_ref=act.at[j, side],
            send_sem=act_send_sem.at[side, j],
            recv_sem=act_recv_sem.at[side, j],
            device_id={"src": toward[1 - side]},
            device_id_type=MESH,
        )

    def depth_of(side):
        return last - s if side == 0 else s

    def sum_step(side, j):
        depth = depth_of(side)
        at_end = depth == last

        @pl.when(depth > 0)
        def _():
            sum_copy(side, j).wait_recv()

        @pl.when(depth == 0)
        def _():
            sum_copy(side, j).start()

        @pl.when((depth > 0) & jnp.logical_not(at_end))
        def _():
            partial[j, side] = (
                partial[j, side].astype(jnp.float32) + sum_recv[side, j].astype(jnp.float32)
            ).astype(jnp.bfloat16)
            sum_copy(side, j).start()

        @pl.when(at_end)
        def _():
            value = partial[j, side].astype(jnp.float32) + sum_recv[side, j].astype(jnp.float32)
            columns = pl.ds(pl.multiple_of(j * LANES, LANES), LANES)
            gate_value = value[:, :LANES] * gate_scale[columns].reshape(1, LANES)
            up_value = value[:, LANES:] * up_scale[columns].reshape(1, LANES)
            activated = (gate_value / (1.0 + jnp.exp(-gate_value)) * up_value).astype(jnp.bfloat16)
            act[j, side] = jnp.dot(
                activated, order_ref[...], preferred_element_type=jnp.float32
            ).astype(jnp.bfloat16)
            act_copy(side, j).start()

    def act_step(side, j):
        depth = last - depth_of(side)
        act_copy(side, j).wait_recv()

        @pl.when(depth < last)
        def _():
            act_copy(side, j).start()

    def step(i, carry):
        @pl.when(i < chunks)
        def _():
            @pl.when(i == 0)
            def _():
                for index in range(2):
                    loads[index].wait()
                    swaps[index].wait_recv()

            columns = pl.ds(pl.multiple_of(i * LANES, LANES), LANES)
            gate_w = [unpack_slab(gate_v[index, :, columns]) for index in range(2)]
            up_w = [unpack_slab(up_v[index, :, columns]) for index in range(2)]
            weights = jnp.concatenate(
                [jnp.concatenate(gate_w, axis=0), jnp.concatenate(up_w, axis=0)], axis=1
            )
            product = jnp.dot(x_v[...], weights, preferred_element_type=jnp.float32)
            product = product.astype(jnp.bfloat16)
            partial[i, 0] = product[:half]
            partial[i, 1] = product[half:]

        for side in range(2):
            j = i - depth_of(side) * lag

            @pl.when((j >= 0) & (j < chunks))
            def _():
                sum_step(side, j)

        for side in range(2):
            depth = last - depth_of(side)
            j = i - far - depth * lag

            @pl.when((depth > 0) & (j >= 0) & (j < chunks))
            def _():
                act_step(side, j)

        j = i - far - jnp.maximum(s, last - s) * lag

        @pl.when((j >= 0) & (j < chunks))
        def _():
            @pl.when(j == 0)
            def _():
                loads[2].wait()
                swaps[2].wait_recv()

            slab = LANES // 4
            words = pl.ds(pl.multiple_of(j * slab, slab), slab)
            weights = jnp.concatenate(
                [unpack_slab(down_v[index, words, :]) for index in range(2)], axis=1
            )
            for side in range(2):
                total[side * half : (side + 1) * half] += jnp.dot(
                    act[j, side], weights, preferred_element_type=jnp.float32
                )

        return carry

    lax.fori_loop(0, chunks + 2 * far, step, 0)

    per_share = count_g * count_s // count_t

    def part_copy(index, ss):
        number = jnp.where(index == 0, g, count_g - 1 - g) * count_s + s
        owner = number // per_share
        slot = t * per_share + lax.rem(number, per_share)
        return owner, slot, pltpu.make_async_remote_copy(
            src_ref=part_send.at[index, ss],
            dst_ref=part_recv.at[slot],
            send_sem=part_send_sem.at[index, ss],
            recv_sem=part_recv_sem.at[slot],
            device_id={"tp": owner, "src": ss},
            device_id_type=MESH,
        )

    for shift in range(count_s):
        ss = lax.rem(s + 1 + shift, count_s)
        row = pl.ds(pl.multiple_of(ss * group_rows, group_rows), group_rows)
        for index in range(2):
            owner, slot, copy = part_copy(index, ss)
            piece = total[row, index * block : (index + 1) * block].astype(jnp.bfloat16)
            mine = (owner == t) & (ss == s)

            @pl.when(mine)
            def _():
                part_recv[slot] = piece

            @pl.when(jnp.logical_not(mine))
            def _():
                part_send[index, ss] = piece
                copy.start()

    for slot in range(count_t * per_share):
        number = t * per_share + slot % per_share
        from_me = (slot // per_share == t) & (lax.rem(number, count_s) == s)

        @pl.when(jnp.logical_not(from_me))
        def _():
            pltpu.make_async_remote_copy(
                src_ref=part_send.at[0, 0],
                dst_ref=part_recv.at[slot],
                send_sem=part_send_sem.at[0, 0],
                recv_sem=part_recv_sem.at[slot],
                device_id={"tp": t, "src": s},
                device_id_type=MESH,
            ).wait_recv()

    mid_wait()
    for place in range(per_share):
        value = part_recv[place].astype(jnp.float32)
        for tt in range(1, count_t):
            value += part_recv[tt * per_share + place].astype(jnp.float32)
        columns = slice(place * block, (place + 1) * block)
        scale_at = pl.ds(pl.multiple_of((t * per_share + place) * block, LANES), block)
        out_ref[:, columns] = (
            mid_v[:, columns].astype(jnp.float32) + value * down_scale[scale_at].reshape(1, block)
        ).astype(jnp.bfloat16)

    for ss in range(count_s):
        for index in range(2):
            owner, slot, copy = part_copy(index, ss)

            @pl.when((owner != t) | (ss != s))
            def _():
                copy.wait_send()

    def drain(j, carry):
        for side in range(2):
            depth = depth_of(side)

            @pl.when(depth < last)
            def _():
                sum_copy(side, j).wait_send()

            @pl.when(depth > 0)
            def _():
                act_copy(side, j).wait_send()

        return carry

    lax.fori_loop(0, chunks, drain, 0)
    finish()


def layer_kernel(lag, counts, *refs):
    count_in, count_buffers, count_a, count_asem, count_b, count_bsem = counts
    take = iter(refs)

    def some(count):
        return [next(take) for _ in range(count)]

    (
        hidden_ref,
        attn_gain,
        w_qkv,
        qkv_scale,
        q_gain,
        k_gain,
        keys,
        values,
        lengths,
        w_out,
        out_scale,
        mlp_gain,
        w_gate,
        w_up,
        gate_scale,
        up_scale,
        w_down,
        down_scale,
        order_ref,
    ) = some(count_in)
    out_ref = next(take)
    mlp_buffers = some(count_buffers)
    scratch_a, sems_a = some(count_a), some(count_asem)
    scratch_b, sems_b = some(count_b), some(count_bsem)
    here = tuple(lax.axis_index(name) for name in ("grp", "tp", "src")) + tuple(
        lax.axis_size(name) for name in ("grp", "tp", "src")
    )
    attention = attention_phase(
        here,
        (
            hidden_ref,
            attn_gain,
            w_qkv,
            qkv_scale,
            q_gain,
            k_gain,
            keys,
            values,
            lengths,
            w_out,
            out_scale,
            mlp_gain,
            (w_gate, w_up, w_down),
            order_ref,
        ),
        mlp_buffers,
        scratch_a,
        sems_a,
    )
    mlp_phase(
        here,
        lag,
        (gate_scale, up_scale, down_scale, order_ref),
        mlp_buffers,
        scratch_b,
        sems_b,
        attention,
        out_ref,
    )


def layer(args, lag):
    (
        hidden_in,
        attn_gain,
        w_qkv,
        qkv_scale,
        q_gain,
        k_gain,
        key_cache,
        value_cache,
        lengths,
        w_out,
        out_scale,
        mlp_gain,
        w_gate,
        w_up,
        gate_scale,
        up_scale,
        w_down,
        down_scale,
    ) = args
    count_g, count_t, count_s = (lax.axis_size(name) for name in ("grp", "tp", "src"))
    group_rows, model = hidden_in.shape
    rows = group_rows * count_s
    half = rows // 2
    mine = group_rows // count_t
    packed_rows, hidden = w_gate.shape
    packed_hidden, block = w_down.shape
    depth = 2 * block
    chunks = hidden // LANES
    share = model // count_t
    slots = count_g * count_s
    steps = 10 if w_qkv.shape[0] % 320 == 0 else w_qkv.shape[0] // 32
    out_steps = 10 if model % (10 * LANES) == 0 else model // LANES
    qkv_columns = w_qkv.shape[1]
    head_rows = QUERY_HEADS * mine
    bf16, f32, i32 = jnp.bfloat16, jnp.float32, jnp.int32
    dma = pltpu.SemaphoreType.DMA
    vmem = pl.BlockSpec(memory_space=pltpu.VMEM)
    smem = pl.BlockSpec(memory_space=pltpu.SMEM)
    hbm = pl.BlockSpec(memory_space=pl.ANY)
    buffers = [
        pltpu.VMEM((2, packed_rows, hidden), i32),
        pltpu.VMEM((2, packed_rows, hidden), i32),
        pltpu.VMEM((2, packed_hidden, block), i32),
        pltpu.VMEM((rows, depth), bf16),
        pltpu.VMEM((group_rows, share), bf16),
    ]
    scratch_a = [
        pltpu.VMEM(w_qkv.shape, i32),
        pltpu.VMEM(w_out.shape, i32),
        pltpu.VMEM((4 * w_out.shape[0], model), bf16),
        pltpu.VMEM(key_cache.shape[1:], bf16),
        pltpu.VMEM(value_cache.shape[1:], bf16),
        pltpu.VMEM((group_rows, model), bf16),
        pltpu.VMEM((group_rows, qkv_columns), f32),
        pltpu.VMEM((group_rows, qkv_columns), bf16),
        pltpu.VMEM((count_t, mine, qkv_columns), bf16),
        pltpu.VMEM((head_rows, HEAD_SIZE), f32),
        pltpu.VMEM((head_rows, HEAD_SIZE), f32),
        pltpu.VMEM((head_rows, key_cache.shape[2]), f32),
        pltpu.VMEM((head_rows, HEAD_SIZE), f32),
        pltpu.VMEM((head_rows, HEAD_SIZE), f32),
        pltpu.VMEM((head_rows, HEAD_SIZE), f32),
        pltpu.VMEM((head_rows, HEAD_SIZE), bf16),
        pltpu.VMEM((count_t, head_rows // count_t, HEAD_SIZE), bf16),
        pltpu.VMEM((group_rows, model), bf16),
        pltpu.VMEM((count_t, mine, model), bf16),
        pltpu.VMEM((count_t, mine, share), bf16),
        pltpu.VMEM((count_s, mine, depth), bf16),
    ]
    sems_a = [
        dma((steps,)),
        dma((out_steps,)),
        dma((2,)),
        dma((3,)),
        dma((3,)),
        dma((3,)),
        dma((count_t,)),
        dma((count_t,)),
        dma((count_t,)),
        dma((count_t,)),
        dma((count_t, out_steps)),
        dma((count_t, out_steps)),
        dma((count_t,)),
        dma((count_t,)),
        dma((count_s,)),
        dma((count_s, count_t)),
        dma((count_s, count_t)),
    ]
    scratch_b = [
        pltpu.VMEM((chunks, 2, half, 2 * LANES), bf16),
        pltpu.VMEM((2, chunks, half, 2 * LANES), bf16),
        pltpu.VMEM((chunks, 2, half, LANES), bf16),
        pltpu.VMEM((rows, depth), f32),
        pltpu.VMEM((2, count_s, group_rows, block), bf16),
        pltpu.VMEM((slots, group_rows, block), bf16),
    ]
    sems_b = [
        dma((2, chunks)),
        dma((2, chunks)),
        dma((2, chunks)),
        dma((2, chunks)),
        dma((2, count_s)),
        dma((slots,)),
    ]
    specs = [vmem] * (len(args) + 1)
    for place in (2, 6, 7, 9, 12, 13, 16):
        specs[place] = hbm
    specs[8] = smem
    counts = (
        len(specs),
        len(buffers),
        len(scratch_a),
        len(sems_a),
        len(scratch_b),
        len(sems_b),
    )
    return pl.pallas_call(
        functools.partial(layer_kernel, lag, counts),
        out_shape=jax.ShapeDtypeStruct((group_rows, share), bf16),
        in_specs=specs,
        out_specs=vmem,
        scratch_shapes=buffers + scratch_a + sems_a + scratch_b + sems_b,
        compiler_params=pltpu.CompilerParams(
            collective_id=1, has_side_effects=True, vmem_limit_bytes=63 * 1024 * 1024
        ),
        name="layer",
    )(*args, lane_order(LANES))


def fast_layer(args):
    hidden_in, w_qkv, w_out, w_gate, w_down = (args[k] for k in (0, 2, 9, 12, 16))
    grp, tp, src = (lax.axis_size(name) for name in ("grp", "tp", "src"))
    rows, model = hidden_in.shape
    return (
        grp == 2
        and src > 1
        and tp > 1
        and (grp * src) % tp == 0
        and rows % (16 * tp) == 0
        and QUERY_HEADS % tp == 0
        and model % (LANES * tp) == 0
        and w_qkv.shape[0] % 32 == 0
        and w_qkv.shape[1] % HEAD_SIZE == 0
        and w_out.shape[0] % 32 == 0
        and w_gate.shape[0] % 32 == 0
        and w_gate.shape[1] % LANES == 0
        and w_down.shape[1] % LANES == 0
        and args[6].shape[2] == LANES
        and HEAD_SIZE == LANES
    )


def local(
    hidden_in,
    attn_gain,
    w_qkv,
    qkv_scale,
    q_gain,
    k_gain,
    key_cache,
    value_cache,
    lengths,
    w_out,
    out_scale,
    mlp_gain,
    w_gate,
    w_up,
    gate_scale,
    up_scale,
    w_down,
    down_scale,
):
    args = (
        hidden_in,
        attn_gain,
        w_qkv,
        qkv_scale,
        q_gain,
        k_gain,
        key_cache,
        value_cache,
        lengths,
        w_out,
        out_scale,
        mlp_gain,
        w_gate,
        w_up,
        gate_scale,
        up_scale,
        w_down,
        down_scale,
    )
    if fast_layer(args):
        return layer(args, 2)
    tp_count = lax.axis_size("tp")
    tp_index = lax.axis_index("tp")
    share_cols = D // tp_count
    residual = hidden_in.astype(jnp.float32)
    normed = normalize_rows(residual, attn_gain).astype(jnp.bfloat16)
    qkv_part = (byte_product(normed, w_qkv) * qkv_scale).astype(jnp.bfloat16)
    query_key_value_rows = lax.all_to_all(qkv_part, "tp", split_axis=0, concat_axis=1, tiled=True)
    heads_out = local_attention(
        query_key_value_rows, q_gain, k_gain, key_cache[0], value_cache[0], lengths[0]
    )
    head_rows = lax.all_to_all(heads_out, "tp", split_axis=1, concat_axis=0, tiled=True)
    partial_value = (byte_product(head_rows, w_out) * out_scale).astype(jnp.bfloat16)
    residual_share = lax.dynamic_slice_in_dim(hidden_in, tp_index * share_cols, share_cols, 1)
    mid_share = (
        residual_share.astype(jnp.float32) + summed_share(partial_value, tp_count)
    ).astype(jnp.bfloat16)
    mid_full = lax.all_gather(mid_share, "tp", axis=1, tiled=True)
    normed_mlp = normalize_rows(mid_full.astype(jnp.float32), mlp_gain).astype(jnp.bfloat16)
    mlp_columns = order_bytes(
        lax.all_to_all(normed_mlp, ("grp", "src"), split_axis=1, concat_axis=0, tiled=True)
    )
    gate_terms = jnp.dot(mlp_columns, unpack_ordered(w_gate), preferred_element_type=jnp.float32)
    up_terms = jnp.dot(mlp_columns, unpack_ordered(w_up), preferred_element_type=jnp.float32)
    both_terms = jnp.concatenate(
        [gate_terms.astype(jnp.bfloat16), up_terms.astype(jnp.bfloat16)], axis=1
    )
    both = summed_rows(summed_rows(both_terms, "grp").astype(jnp.bfloat16), "src")
    hidden = gate_scale.shape[0]
    gate_value = both[:, :hidden] * gate_scale
    up_value = both[:, hidden:] * up_scale
    activated = order_bytes((jax.nn.silu(gate_value) * up_value).astype(jnp.bfloat16))
    all_activated = gathered_rows(gathered_rows(activated, "src"), "grp")
    down_columns = jnp.dot(
        all_activated, unpack_ordered(w_down), preferred_element_type=jnp.float32
    ).astype(jnp.bfloat16)
    down_rows = lax.all_to_all(
        down_columns, ("grp", "src"), split_axis=0, concat_axis=1, tiled=True
    )
    down_share = lax.dynamic_slice_in_dim(down_scale, tp_index * share_cols, share_cols, 0)
    mlp_share = summed_share(down_rows, tp_count) * down_share
    return (mid_share.astype(jnp.float32) + mlp_share).astype(jnp.bfloat16)


def solution(mesh):
    return jax.shard_map(
        local,
        mesh=mesh,
        in_specs=(
            P(("grp", "src"), None),
            P(),
            P(None, "tp"),
            P("tp"),
            P(),
            P(),
            P(("grp", "src"), "tp", None, None),
            P(("grp", "src"), "tp", None, None),
            P(("grp", "src"), "tp"),
            P("tp", None),
            P(),
            P(),
            P(("grp", "src"), "tp"),
            P(("grp", "src"), "tp"),
            P("tp"),
            P("tp"),
            P("tp", ("grp", "src")),
            P(),
        ),
        out_specs=P(("grp", "src"), "tp"),
        check_vma=False,
    )
```

```python
import functools
import math

import jax
import jax.numpy as jnp
from jax import lax
from jax.experimental import pallas as pl
from jax.experimental.pallas import tpu as pltpu
from jax.sharding import PartitionSpec as P

D = 5120
QUERY_HEADS = 32
KEY_VALUE_HEADS = 4
HEAD_SIZE = 128
QUERY_COLUMNS = 4096
KEY_COLUMNS = 512


norm_epsilon = 1e-06
rope_base = 1000000.0


def unpack_bytes(packed, byte_index):
    return jnp.right_shift(jnp.left_shift(packed, 24 - 8 * byte_index), 24)


def byte_order(block):
    source = lax.broadcasted_iota(jnp.int32, (block, block), 0)
    target = lax.broadcasted_iota(jnp.int32, (block, block), 1)
    return (target == (source % 4) * (block // 4) + source // 4).astype(jnp.bfloat16)


def split_kernel(block, x_ref, order_ref, out_ref):
    lanes = block // 4
    for c in range(x_ref.shape[1] // block):
        moved = jnp.dot(
            x_ref[:, c * block : (c + 1) * block],
            order_ref[...],
            preferred_element_type=jnp.float32,
        ).astype(jnp.bfloat16)
        for j in range(4):
            out_ref[j, :, c * lanes : (c + 1) * lanes] = moved[:, j * lanes : (j + 1) * lanes]


def split_bytes(activations):
    rows, width = activations.shape
    if width % 512:
        return [activations[:, byte_index::4] for byte_index in range(4)]
    split = pl.pallas_call(
        functools.partial(split_kernel, 512),
        out_shape=jax.ShapeDtypeStruct((4, rows, width // 4), jnp.bfloat16),
        cost_estimate=pl.CostEstimate(
            flops=2 * rows * width * 512, bytes_accessed=4 * rows * width, transcendentals=0
        ),
        name="split_bytes",
    )(activations, byte_order(512))
    return [split[byte_index] for byte_index in range(4)]


def byte_product(activations, packed):
    pieces = split_bytes(activations)
    products = [
        jnp.dot(
            pieces[byte_index],
            unpack_bytes(packed, byte_index).astype(jnp.bfloat16),
            preferred_element_type=jnp.float32,
        )
        for byte_index in range(4)
    ]
    return products[0] + products[1] + products[2] + products[3]


def block_of(width):
    return math.gcd(640, width)


def order_kernel(block, x_ref, order_ref, out_ref):
    for c in range(x_ref.shape[1] // block):
        out_ref[:, c * block : (c + 1) * block] = jnp.dot(
            x_ref[:, c * block : (c + 1) * block],
            order_ref[...],
            preferred_element_type=jnp.float32,
        ).astype(jnp.bfloat16)


def order_bytes(activations):
    rows, width = activations.shape
    block = block_of(width)
    if block == width:
        return jnp.dot(activations, byte_order(block), preferred_element_type=jnp.float32).astype(
            jnp.bfloat16
        )
    return pl.pallas_call(
        functools.partial(order_kernel, block),
        out_shape=jax.ShapeDtypeStruct((rows, width), jnp.bfloat16),
        cost_estimate=pl.CostEstimate(
            flops=2 * rows * width * block, bytes_accessed=4 * rows * width, transcendentals=0
        ),
        name="order_bytes",
    )(activations, byte_order(block))


def unpack_ordered(packed):
    rows, columns = packed.shape
    block = block_of(4 * rows) // 4
    blocks = packed.reshape(rows // block, block, columns)
    parts = [unpack_bytes(blocks, j).astype(jnp.bfloat16) for j in range(4)]
    return jnp.stack(parts, axis=1).reshape(4 * rows, columns)


def normalize_rows(values, gain_row):
    return (
        values
        * lax.rsqrt(jnp.mean(values * values, axis=-1, keepdims=True) + norm_epsilon)
        * gain_row
    )


def rotary_embed(values, positions):
    half_dim = values.shape[-1] // 2
    freq_index = jnp.arange(half_dim, dtype=jnp.float32)
    inverse = jnp.exp(freq_index * (-math.log(rope_base) / half_dim))
    angles = positions.astype(jnp.float32)[:, None] * inverse[None, :]
    cosine = jnp.cos(angles)[:, None, :]
    sine_part = jnp.sin(angles)[:, None, :]
    lower_half = values[..., :half_dim]
    upper_half = values[..., half_dim:]
    return jnp.concatenate(
        [
            lower_half * cosine - upper_half * sine_part,
            upper_half * cosine + lower_half * sine_part,
        ],
        axis=-1,
    )


def local_attention(query_key_value_rows, q_gain, k_gain, stored_keys, stored_values, seq_lengths):
    count_of_rows = query_key_value_rows.shape[0]
    cache_length = stored_keys.shape[1]
    query_matrix = (
        query_key_value_rows[:, :QUERY_COLUMNS]
        .astype(jnp.float32)
        .reshape(count_of_rows, QUERY_HEADS, HEAD_SIZE)
    )
    incoming_keys = (
        query_key_value_rows[:, QUERY_COLUMNS : QUERY_COLUMNS + KEY_COLUMNS]
        .astype(jnp.float32)
        .reshape(count_of_rows, KEY_VALUE_HEADS, HEAD_SIZE)
    )
    incoming_values = query_key_value_rows[:, QUERY_COLUMNS + KEY_COLUMNS :].reshape(
        count_of_rows, KEY_VALUE_HEADS, HEAD_SIZE
    )
    query_matrix = rotary_embed(normalize_rows(query_matrix, q_gain), seq_lengths).astype(
        jnp.bfloat16
    )
    incoming_keys = rotary_embed(normalize_rows(incoming_keys, k_gain), seq_lengths).astype(
        jnp.bfloat16
    )
    query_groups = query_matrix.reshape(
        count_of_rows, KEY_VALUE_HEADS, QUERY_HEADS // KEY_VALUE_HEADS, HEAD_SIZE
    )
    key_slices = stored_keys.reshape(count_of_rows, cache_length, KEY_VALUE_HEADS, HEAD_SIZE)
    value_slices = stored_values.reshape(count_of_rows, cache_length, KEY_VALUE_HEADS, HEAD_SIZE)
    logit_scale = 1.0 / math.sqrt(HEAD_SIZE)
    scores = (
        jnp.einsum("bkgd,bpkd->bkgp", query_groups, key_slices, preferred_element_type=jnp.float32)
        * logit_scale
    )
    live_mask = jnp.arange(cache_length, dtype=jnp.int32)[None, :] < seq_lengths[:, None]
    scores = jnp.where(live_mask[:, None, None, :], scores, -jnp.inf)
    self_score = (
        jnp.einsum("nufi,nui->nuf", query_groups, incoming_keys, preferred_element_type=jnp.float32)
        * logit_scale
    )
    row_max = jnp.maximum(jnp.max(scores, axis=-1), self_score)
    soft_weights = jnp.exp(scores - row_max[..., None])
    own_weight = jnp.exp(self_score - row_max)
    denominator = jnp.sum(soft_weights, axis=-1) + own_weight
    own_low = lax.optimization_barrier(own_weight.astype(jnp.bfloat16)).astype(jnp.float32)
    numerator = jnp.einsum(
        "bkgp,bpkd->bkgd",
        soft_weights.astype(jnp.bfloat16),
        value_slices,
        preferred_element_type=jnp.float32,
    )
    numerator = numerator + own_low[..., None] * incoming_values.astype(jnp.float32)[:, :, None, :]
    return (
        (numerator / denominator[..., None])
        .reshape(count_of_rows, QUERY_COLUMNS)
        .astype(jnp.bfloat16)
    )


def summed_share(terms, tp_count):
    rows, columns = terms.shape
    pieces = lax.all_to_all(terms, "tp", split_axis=1, concat_axis=0, tiled=True)
    return jnp.sum(
        pieces.reshape(tp_count, rows, columns // tp_count).astype(jnp.float32), axis=0
    )


def gathered_rows(rows, axis):
    count = lax.axis_size(axis)
    copies = jnp.broadcast_to(rows[None], (count, *rows.shape))
    pieces = lax.all_to_all(copies, axis, split_axis=0, concat_axis=0)
    return pieces.reshape(count * rows.shape[0], rows.shape[1])


def summed_rows(terms, axis):
    count = lax.axis_size(axis)
    rows, columns = terms.shape
    pieces = lax.all_to_all(
        terms.reshape(count, rows // count, columns), axis, split_axis=0, concat_axis=0
    )
    return jnp.sum(pieces.astype(jnp.float32), axis=0)


LANES = 128
MESH = pl.DeviceIdType.MESH


def lane_order(block):
    source = lax.broadcasted_iota(jnp.int32, (block, block), 0)
    target = lax.broadcasted_iota(jnp.int32, (block, block), 1)
    return (target == (source % 4) * (block // 4) + source // 4).astype(jnp.bfloat16)


def unpack_slab(packed):
    rows, columns = packed.shape
    slab = LANES // 4
    parts = []
    for k in range(rows // slab):
        words = packed[k * slab : (k + 1) * slab]
        for j in range(4):
            parts.append(unpack_bytes(words, j).astype(jnp.float32).astype(jnp.bfloat16))
    return jnp.concatenate(parts, axis=0)


def stack_lanes(values):
    blocks = values.shape[1] // LANES
    return jnp.concatenate([values[:, k * LANES : (k + 1) * LANES] for k in range(blocks)], axis=0)


def ordered(stacked, order_ref):
    return jnp.dot(stacked, order_ref[...], preferred_element_type=jnp.float32).astype(jnp.bfloat16)


def row_of(ref):
    return ref[...].reshape(1, ref.shape[0])


def attention_phase(here, inputs, mlp_buffers, scratch, sems):
    g, t, s, count_g, count_t, count_s = here
    (
        hidden_ref,
        attn_gain,
        w_qkv,
        qkv_scale,
        q_gain,
        k_gain,
        keys,
        values,
        lengths,
        w_out,
        out_scale,
        mlp_gain,
        weights,
        order_ref,
    ) = inputs
    gate_v, up_v, down_v, x_v, mid_v = mlp_buffers
    (
        qkv_w,
        out_w,
        out_u,
        keys_v,
        values_v,
        normed_v,
        qkv_acc,
        qkv_send,
        qkv_recv,
        q_v,
        own_v,
        score_v,
        own_e_v,
        denom_v,
        attn_v,
        attn_send,
        attn_recv,
        proj_v,
        proj_recv,
        mid_send,
        x_send,
    ) = scratch
    (
        qkv_w_sem,
        out_w_sem,
        cache_sem,
        swap_send_sem,
        swap_recv_sem,
        load_sem,
        qkv_send_sem,
        qkv_recv_sem,
        attn_send_sem,
        attn_recv_sem,
        proj_send_sem,
        proj_recv_sem,
        mid_send_sem,
        mid_recv_sem,
        z_send_sem,
        x_send_sem,
        x_recv_sem,
    ) = sems
    f32, bf16 = jnp.float32, jnp.bfloat16
    rows, model = hidden_ref.shape
    mine = rows // count_t
    qkv_columns = w_qkv.shape[1]
    steps = qkv_w_sem.shape[0]
    step_rows = w_qkv.shape[0] // steps
    out_steps = out_w_sem.shape[0]
    out_width = model // out_steps
    share = model // count_t
    positions = keys_v.shape[1]
    heads = QUERY_HEADS
    per_kv = QUERY_HEADS // KEY_VALUE_HEADS
    heads_t = heads // count_t

    def qkv_load(i):
        part = pl.ds(pl.multiple_of(i * step_rows, step_rows), step_rows)
        return pltpu.make_async_copy(w_qkv.at[part, :], qkv_w.at[part, :], qkv_w_sem.at[i])

    def out_load(i):
        part = pl.ds(pl.multiple_of(i * out_width, LANES), out_width)
        return pltpu.make_async_copy(w_out.at[:, part], out_w.at[:, part], out_w_sem.at[i])

    for i in range(steps):
        qkv_load(i).start()
    cache = [
        pltpu.make_async_copy(keys.at[0], keys_v, cache_sem.at[0]),
        pltpu.make_async_copy(values.at[0], values_v, cache_sem.at[1]),
    ]
    for copy in cache:
        copy.start()
    for i in range(out_steps):
        out_load(i).start()

    barrier = pltpu.get_barrier_semaphore()
    for tt in range(count_t):
        for ss in range(count_s):

            @pl.when((tt != t) | (ss != s))
            def _():
                pl.semaphore_signal(
                    barrier, inc=1, device_id={"tp": tt, "src": ss}, device_id_type=MESH
                )

    pl.semaphore_signal(barrier, inc=1, device_id={"grp": 1 - g}, device_id_type=MESH)

    with jax.named_scope("norm"):
        normed = normalize_rows(hidden_ref[...].astype(f32), row_of(attn_gain)).astype(bf16)
        moved = ordered(stack_lanes(normed), order_ref)
        for k in range(model // LANES):
            normed_v[:, k * LANES : (k + 1) * LANES] = moved[k * rows : (k + 1) * rows]

    swaps = [
        pltpu.make_async_remote_copy(
            src_ref=source,
            dst_ref=target.at[1],
            send_sem=swap_send_sem.at[index],
            recv_sem=swap_recv_sem.at[index],
            device_id={"grp": 1 - g},
            device_id_type=MESH,
        )
        for index, (source, target) in enumerate(zip(weights, (gate_v, up_v, down_v)))
    ]
    loads = [
        pltpu.make_async_copy(source, target.at[0], load_sem.at[index])
        for index, (source, target) in enumerate(zip(weights, (gate_v, up_v, down_v)))
    ]

    qkv_acc[...] = jnp.zeros_like(qkv_acc)

    def qkv_step(i, carry):
        qkv_load(i).wait()
        part = pl.ds(pl.multiple_of(i * step_rows, step_rows), step_rows)
        depth = pl.ds(pl.multiple_of(i * 4 * step_rows, LANES), 4 * step_rows)
        qkv_acc[...] += jnp.dot(
            normed_v[:, depth], unpack_slab(qkv_w[part, :]), preferred_element_type=f32
        )
        return carry

    with jax.named_scope("qkv"):
        lax.fori_loop(0, steps, qkv_step, 0)
        pl.semaphore_wait(barrier, count_t * count_s)
        for copy in swaps + loads:
            copy.start()
        qkv_send[...] = (qkv_acc[...] * row_of(qkv_scale)).astype(bf16)

    def peer_of(shift):
        return lax.rem(t + shift, count_t)

    def rows_of(index):
        return pl.ds(pl.multiple_of(index * mine, mine), mine)

    def qkv_copy(peer, slot):
        return pltpu.make_async_remote_copy(
            src_ref=qkv_send.at[rows_of(peer), :],
            dst_ref=qkv_recv.at[slot],
            send_sem=qkv_send_sem.at[peer],
            recv_sem=qkv_recv_sem.at[slot],
            device_id={"tp": peer},
            device_id_type=MESH,
        )

    for shift in range(1, count_t):
        qkv_copy(peer_of(shift), t).start()
    qkv_recv[t] = qkv_send[rows_of(t), :]

    def unpack_out(i, carry):
        out_load(i).wait()
        part = pl.ds(pl.multiple_of(i * out_width, LANES), out_width)
        out_u[:, part] = unpack_slab(out_w[:, part])
        return carry

    with jax.named_scope("unpack_out"):
        lax.fori_loop(0, out_steps, unpack_out, 0)

    row_index = lax.broadcasted_iota(jnp.int32, (mine, HEAD_SIZE), 0)
    lane = lax.broadcasted_iota(jnp.int32, (mine, HEAD_SIZE), 1)
    place = jnp.zeros((mine, HEAD_SIZE), f32)
    for b in range(mine):
        place = jnp.where(row_index == b, lengths[0, b].astype(f32), place)
    half_dim = HEAD_SIZE // 2
    low = lane < half_dim
    frequency = jnp.where(low, lane, lane - half_dim).astype(f32)
    angle = place * jnp.exp(frequency * (-math.log(rope_base) / half_dim))
    cosine = jnp.cos(angle)
    sine = jnp.sin(angle)
    sine = jnp.where(low, -sine, sine)

    with jax.named_scope("wait_qkv"):
        for shift in range(1, count_t):
            qkv_copy(t, peer_of(shift)).wait_recv()

    per_share = qkv_columns // HEAD_SIZE

    def head_of(h):
        column = (h % per_share) * HEAD_SIZE
        return qkv_recv[h // per_share, :, column : column + HEAD_SIZE]

    def turned(first, count, gain):
        stacked = jnp.concatenate([head_of(first + k) for k in range(count)], axis=0)
        value = normalize_rows(stacked.astype(f32), gain)
        other = pltpu.roll(value, half_dim, 1)
        wide = [jnp.concatenate([table] * count, axis=0) for table in (cosine, sine)]
        return (value * wide[0] + other * wide[1]).astype(bf16).astype(f32)

    logit_scale = 1.0 / math.sqrt(HEAD_SIZE)
    q_row, k_row = row_of(q_gain), row_of(k_gain)
    with jax.named_scope("rope"):
        new_keys = turned(heads, KEY_VALUE_HEADS, k_row)
        for kv in range(KEY_VALUE_HEADS):
            part = slice(kv * per_kv * mine, (kv + 1) * per_kv * mine)
            query = turned(kv * per_kv, per_kv, q_row)
            q_v[part] = query
            new_key = jnp.concatenate([new_keys[kv * mine : (kv + 1) * mine]] * per_kv, axis=0)
            own = jnp.sum(query * new_key, axis=1, keepdims=True) * logit_scale
            own_v[part] = jnp.broadcast_to(own, query.shape)
    for copy in cache:
            copy.wait()

    zeros = jnp.zeros((per_kv, HEAD_SIZE), f32)
    with jax.named_scope("scores"):
        for b in range(mine):
            query = q_v[pl.ds(b, heads, stride=mine), :]
            spread = jnp.concatenate(
                [
                    jnp.concatenate(
                        [
                            query[kv * per_kv : (kv + 1) * per_kv] if kv == place_of else zeros
                            for place_of in range(KEY_VALUE_HEADS)
                        ],
                        axis=1,
                    )
                    for kv in range(KEY_VALUE_HEADS)
                ],
                axis=0,
            ).astype(bf16)
            score_v[b * heads : (b + 1) * heads] = lax.dot_general(
                spread, keys_v[b], (((1,), (1,)), ((), ())), preferred_element_type=f32
            )
    position = lax.broadcasted_iota(jnp.int32, (heads, positions), 1)
    with jax.named_scope("softmax"):
        for b in range(mine):
            strided = pl.ds(b, heads, stride=mine)
            scores = score_v[b * heads : (b + 1) * heads] * logit_scale
            scores = jnp.where(position < lengths[0, b], scores, -jnp.inf)
            own = own_v[strided, :][:, :1]
            top = jnp.maximum(jnp.max(scores, axis=1, keepdims=True), own)
            weight = jnp.exp(scores - top)
            own_e = jnp.exp(own - top)
            denominator = jnp.sum(weight, axis=1, keepdims=True) + own_e
            score_v[b * heads : (b + 1) * heads] = weight
            own_e_v[strided, :] = jnp.broadcast_to(own_e, (heads, HEAD_SIZE))
            denom_v[strided, :] = jnp.broadcast_to(denominator, (heads, HEAD_SIZE))
    with jax.named_scope("mix"):
        for b in range(mine):
            mixed = jnp.dot(
                score_v[b * heads : (b + 1) * heads].astype(bf16),
                values_v[b],
                preferred_element_type=f32,
            )
            attn_v[pl.ds(b, heads, stride=mine), :] = jnp.concatenate(
                [
                    mixed[kv * per_kv : (kv + 1) * per_kv, kv * HEAD_SIZE : (kv + 1) * HEAD_SIZE]
                    for kv in range(KEY_VALUE_HEADS)
                ],
                axis=0,
            )
    with jax.named_scope("finish_attn"):
        finished = []
        for h in range(heads):
            part = slice(h * mine, (h + 1) * mine)
            new_value = head_of(heads + KEY_VALUE_HEADS + h // per_kv).astype(f32)
            own_low = own_e_v[part].astype(bf16).astype(f32)
            finished.append(((attn_v[part] + own_low * new_value) / denom_v[part]).astype(bf16))
        attn_send[...] = ordered(jnp.concatenate(finished, axis=0), order_ref)

    head_rows = heads_t * mine

    def attn_copy(peer, slot):
        return pltpu.make_async_remote_copy(
            src_ref=attn_send.at[pl.ds(pl.multiple_of(peer * head_rows, head_rows), head_rows), :],
            dst_ref=attn_recv.at[slot],
            send_sem=attn_send_sem.at[peer],
            recv_sem=attn_recv_sem.at[slot],
            device_id={"tp": peer},
            device_id_type=MESH,
        )

    for shift in range(1, count_t):
        attn_copy(peer_of(shift), t).start()
    attn_recv[t] = attn_send[pl.ds(pl.multiple_of(t * head_rows, head_rows), head_rows), :]
    with jax.named_scope("wait_attn"):
        for shift in range(1, count_t):
            attn_copy(t, peer_of(shift)).wait_recv()

    def proj_copy(peer, slot, i):
        part = pl.ds(pl.multiple_of(i * out_width, LANES), out_width)
        return pltpu.make_async_remote_copy(
            src_ref=proj_v.at[rows_of(peer), part],
            dst_ref=proj_recv.at[slot, :, part],
            send_sem=proj_send_sem.at[peer],
            recv_sem=proj_recv_sem.at[slot],
            device_id={"tp": peer},
            device_id_type=MESH,
        )

    def proj_whole(peer, slot):
        return pltpu.make_async_remote_copy(
            src_ref=proj_v.at[rows_of(peer), :],
            dst_ref=proj_recv.at[slot],
            send_sem=proj_send_sem.at[peer],
            recv_sem=proj_recv_sem.at[slot],
            device_id={"tp": peer},
            device_id_type=MESH,
        )

    def out_step(i, carry):
        part = pl.ds(pl.multiple_of(i * out_width, LANES), out_width)
        left = jnp.concatenate(
            [
                jnp.concatenate(
                    [attn_recv[tt, h * mine : (h + 1) * mine] for tt in range(count_t)], axis=0
                )
                for h in range(heads_t)
            ],
            axis=1,
        )
        product = jnp.dot(left, out_u[:, part], preferred_element_type=f32)
        proj_v[:, part] = (product * out_scale[part].reshape(1, out_width)).astype(bf16)
        for shift in range(1, count_t):
            proj_copy(peer_of(shift), t, i).start()
        return carry

    with jax.named_scope("proj"):
        lax.fori_loop(0, out_steps, out_step, 0)

    with jax.named_scope("mid"):
        total = hidden_ref[rows_of(t), :].astype(f32) + proj_v[rows_of(t), :].astype(f32)
        for shift in range(1, count_t):
            slot = peer_of(shift)

            proj_whole(t, slot).wait_recv()
            total += proj_recv[slot].astype(f32)
        mid = total.astype(bf16)
        for tt in range(count_t):
            mid_send[tt] = mid[:, tt * share : (tt + 1) * share]
        moved = ordered(
            stack_lanes(normalize_rows(mid.astype(f32), row_of(mlp_gain)).astype(bf16)), order_ref
        )
    block = model // (count_g * count_s) // LANES
    with jax.named_scope("order_x"):
        for number in range(count_g * count_s):
            owner = number % count_s
            first = jnp.where(number // count_s == g, 0, block)
            for k in range(block):
                column = pl.multiple_of((first + k) * LANES, LANES)
                source = number * block + k
                x_send[owner, :, pl.ds(column, LANES)] = moved[source * mine : (source + 1) * mine]

    def x_rows(ss, tt):
        return pl.ds(pl.multiple_of((ss * count_t + tt) * mine, mine), mine)

    def z_copy(peer, ss):
        return pltpu.make_async_remote_copy(
            src_ref=x_send.at[peer],
            dst_ref=x_v.at[x_rows(ss, t), :],
            send_sem=z_send_sem.at[peer],
            recv_sem=x_recv_sem.at[ss, t],
            device_id={"src": peer},
            device_id_type=MESH,
        )

    def x_copy(peer, ss, tt):
        return pltpu.make_async_remote_copy(
            src_ref=x_v.at[x_rows(ss, tt), :],
            dst_ref=x_v.at[x_rows(ss, tt), :],
            send_sem=x_send_sem.at[peer],
            recv_sem=x_recv_sem.at[ss, tt],
            device_id={"tp": peer},
            device_id_type=MESH,
        )

    def own_copy(peer):
        return pltpu.make_async_remote_copy(
            src_ref=x_send.at[s],
            dst_ref=x_v.at[x_rows(s, t), :],
            send_sem=x_send_sem.at[peer],
            recv_sem=x_recv_sem.at[s, t],
            device_id={"tp": peer},
            device_id_type=MESH,
        )

    def x_whole(peer):
        return pltpu.make_async_remote_copy(
            src_ref=x_send,
            dst_ref=x_send,
            send_sem=x_send_sem.at[peer],
            recv_sem=x_recv_sem.at[s, t],
            device_id={"tp": peer},
            device_id_type=MESH,
        )

    def mid_copy(peer, slot):
        return pltpu.make_async_remote_copy(
            src_ref=mid_send.at[peer],
            dst_ref=mid_v.at[rows_of(slot), :],
            send_sem=mid_send_sem.at[peer],
            recv_sem=mid_recv_sem.at[slot],
            device_id={"tp": peer},
            device_id_type=MESH,
        )

    with jax.named_scope("spread_z"):
        def near(distance, action):
            for other in (s + distance, s - distance):

                @pl.when((other >= 0) & (other < count_s))
                def _():
                    action(other)

        for distance in range(count_s - 1, 0, -1):
            near(distance, lambda other: z_copy(other, s).start())
        for shift in range(1, count_t):
            own_copy(peer_of(shift)).start()
        x_v[x_rows(s, t), :] = x_send[s]

        def forward(ss):
            z_copy(s, ss).wait_recv()
            for turn in range(1, count_t):
                x_copy(peer_of(turn), ss, t).start()

        for distance in range(1, count_s):
            near(distance, forward)
    for shift in range(1, count_t):
        mid_copy(peer_of(shift), t).start()
    mid_v[rows_of(t), :] = mid_send[t]
    with jax.named_scope("spread_t"):
        for ss in range(count_s):
            for turn in range(1, count_t):
                x_copy(t, ss, peer_of(turn)).wait_recv()

    def finish():
        for shift in range(1, count_t):
            peer = peer_of(shift)
            qkv_copy(peer, t).wait_send()
            attn_copy(peer, t).wait_send()
            mid_copy(peer, t).wait_send()

            proj_whole(peer, t).wait_send()
            x_whole(peer).wait_send()
        for shift in range(1, count_s):
            z_copy(lax.rem(s + shift, count_s), s).wait_send()
        for copy in swaps:
            copy.wait_send()

    def mid_wait():
        for shift in range(1, count_t):
            mid_copy(t, peer_of(shift)).wait_recv()

    return swaps, loads, mid_wait, finish


def mlp_phase(here, lags, scales, mlp_buffers, scratch, sems, attention, out_ref):
    g, t, s, count_g, count_t, count_s = here
    gate_scale, up_scale, down_scale, order_ref = scales
    lag, back_lag = lags
    gate_v, up_v, down_v, x_v, mid_v = mlp_buffers
    partial, sum_recv, act, total, part_send, part_recv = scratch
    (
        sum_send_sem,
        sum_recv_sem,
        act_send_sem,
        act_recv_sem,
        part_send_sem,
        part_recv_sem,
    ) = sems
    swaps, loads, mid_wait, finish = attention
    rows = x_v.shape[0]
    half = rows // 2
    hidden = gate_v.shape[2]
    block = down_v.shape[2]
    chunks = hidden // LANES
    group_rows = rows // count_s
    total[...] = jnp.zeros_like(total)

    last = count_s - 1
    far = (last - 1) * lag
    toward = (s - 1, s + 1)

    def sum_copy(side, j):
        return pltpu.make_async_remote_copy(
            src_ref=partial.at[side, j],
            dst_ref=sum_recv.at[side, j],
            send_sem=sum_send_sem.at[side],
            recv_sem=sum_recv_sem.at[side, j],
            device_id={"src": toward[side]},
            device_id_type=MESH,
        )

    def act_copy(side, j):
        return pltpu.make_async_remote_copy(
            src_ref=act.at[side, j],
            dst_ref=act.at[side, j],
            send_sem=act_send_sem.at[side],
            recv_sem=act_recv_sem.at[side, j],
            device_id={"src": toward[1 - side]},
            device_id_type=MESH,
        )

    def whole_copy(array, side, sem):
        return pltpu.make_async_remote_copy(
            src_ref=array.at[side],
            dst_ref=array.at[side],
            send_sem=sem.at[side],
            recv_sem=sum_recv_sem.at[side, 0],
            device_id={"src": toward[side]},
            device_id_type=MESH,
        )

    def depth_of(side):
        return last - s if side == 0 else s

    def pass_step(side, j):
        depth = depth_of(side)

        @pl.when(depth > 0)
        def _():
            sum_copy(side, j).wait_recv()
            partial[side, j] = (
                partial[side, j].astype(jnp.float32) + sum_recv[side, j].astype(jnp.float32)
            ).astype(jnp.bfloat16)

        sum_copy(side, j).start()

    def end_step(side, j):
        sum_copy(side, j).wait_recv()
        value = partial[side, j].astype(jnp.float32) + sum_recv[side, j].astype(jnp.float32)
        columns = pl.ds(pl.multiple_of(j * LANES, LANES), LANES)
        gate_value = value[:, :LANES] * gate_scale[columns].reshape(1, LANES)
        up_value = value[:, LANES:] * up_scale[columns].reshape(1, LANES)
        activated = (gate_value / (1.0 + jnp.exp(-gate_value)) * up_value).astype(jnp.bfloat16)
        act[side, j] = jnp.dot(
            activated, order_ref[...], preferred_element_type=jnp.float32
        ).astype(jnp.bfloat16)
        act_copy(side, j).start()

    def act_step(side, j):
        depth = last - depth_of(side)
        act_copy(side, j).wait_recv()

        @pl.when(depth < last)
        def _():
            act_copy(side, j).start()

    def step(i, carry):
        @pl.when(i < chunks)
        def _():
            @pl.when(i == 0)
            def _():
                for index in range(2):
                    loads[index].wait()
                    swaps[index].wait_recv()

            columns = pl.ds(pl.multiple_of(i * LANES, LANES), LANES)
            gate_w = [unpack_slab(gate_v[index, :, columns]) for index in range(2)]
            up_w = [unpack_slab(up_v[index, :, columns]) for index in range(2)]
            weights = jnp.concatenate(
                [jnp.concatenate(gate_w, axis=0), jnp.concatenate(up_w, axis=0)], axis=1
            )
            product = jnp.dot(x_v[...], weights, preferred_element_type=jnp.float32)
            product = product.astype(jnp.bfloat16)
            partial[0, i] = product[:half]
            partial[1, i] = product[half:]

        for side in range(2):
            depth = depth_of(side)
            j = i - depth * lag

            @pl.when((depth < last) & (j >= 0) & (j < chunks))
            def _():
                pass_step(side, j)

        return carry

    def end_loop(j, carry):
        for side in range(2):

            @pl.when(depth_of(side) == last)
            def _():
                end_step(side, j)

        return carry

    def back_step(i, carry):
        for side in range(2):
            depth = last - depth_of(side)
            j = i - depth * back_lag

            @pl.when((depth > 0) & (j >= 0) & (j < chunks))
            def _():
                act_step(side, j)

        j = i - jnp.maximum(s, last - s) * back_lag

        @pl.when((j >= 0) & (j < chunks))
        def _():
            @pl.when(j == 0)
            def _():
                loads[2].wait()
                swaps[2].wait_recv()

            slab = LANES // 4
            words = pl.ds(pl.multiple_of(j * slab, slab), slab)
            weights = jnp.concatenate(
                [unpack_slab(down_v[index, words, :]) for index in range(2)], axis=1
            )
            for side in range(2):
                total[side * half : (side + 1) * half] += jnp.dot(
                    act[side, j], weights, preferred_element_type=jnp.float32
                )

        return carry

    with jax.named_scope("mlp_loop"):
        lax.fori_loop(0, chunks + far, step, 0)
    with jax.named_scope("end_loop"):
        lax.fori_loop(0, chunks, end_loop, 0)
    with jax.named_scope("back_loop"):
        lax.fori_loop(0, chunks + last * back_lag, back_step, 0)

    per_share = count_g * count_s // count_t

    def part_copy(index, ss):
        number = jnp.where(index == 0, g, count_g - 1 - g) * count_s + s
        owner = number // per_share
        slot = t * per_share + lax.rem(number, per_share)
        return owner, slot, pltpu.make_async_remote_copy(
            src_ref=part_send.at[index, ss],
            dst_ref=part_recv.at[slot],
            send_sem=part_send_sem.at[index, ss],
            recv_sem=part_recv_sem.at[slot],
            device_id={"tp": owner, "src": ss},
            device_id_type=MESH,
        )

    with jax.named_scope("part_send"):
        for shift in range(count_s):
            ss = send_order(s, count_s, shift)
            row = pl.ds(pl.multiple_of(ss * group_rows, group_rows), group_rows)
            for index in range(2):
                owner, slot, copy = part_copy(index, ss)
                piece = total[row, index * block : (index + 1) * block].astype(jnp.bfloat16)
                mine = (owner == t) & (ss == s)

                @pl.when(mine)
                def _():
                    part_recv[slot] = piece

                @pl.when(jnp.logical_not(mine))
                def _():
                    part_send[index, ss] = piece
                    copy.start()

    with jax.named_scope("drain"):
        finish()
        for side in range(2):
            depth = depth_of(side)

            @pl.when(depth < last)
            def _():
                whole_copy(partial, side, sum_send_sem).wait_send()

            @pl.when(depth > 0)
            def _():
                whole_copy(act, side, act_send_sem).wait_send()

    with jax.named_scope("part_wait"):
        for slot in range(count_t * per_share):
            number = t * per_share + slot % per_share
            from_me = (slot // per_share == t) & (lax.rem(number, count_s) == s)

            @pl.when(jnp.logical_not(from_me))
            def _():
                pltpu.make_async_remote_copy(
                    src_ref=part_send.at[0, 0],
                    dst_ref=part_recv.at[slot],
                    send_sem=part_send_sem.at[0, 0],
                    recv_sem=part_recv_sem.at[slot],
                    device_id={"tp": t, "src": s},
                    device_id_type=MESH,
                ).wait_recv()

    mid_wait()
    with jax.named_scope("part_sum"):
        for place in range(per_share):
            value = part_recv[place].astype(jnp.float32)
            for tt in range(1, count_t):
                value += part_recv[tt * per_share + place].astype(jnp.float32)
            columns = slice(place * block, (place + 1) * block)
            scale_at = pl.ds(pl.multiple_of((t * per_share + place) * block, LANES), block)
            out_ref[:, columns] = (
                mid_v[:, columns].astype(jnp.float32) + value * down_scale[scale_at].reshape(1, block)
            )

    for ss in range(count_s):
        for index in range(2):
            owner, slot, copy = part_copy(index, ss)

            @pl.when((owner != t) | (ss != s))
            def _():
                copy.wait_send()


def send_order(s, count_s, shift):
    if count_s % 2:
        return lax.rem(s + 1 + shift, count_s)
    size = count_s // 2
    other = jnp.where(s < size, size, 0)
    base = other if shift < size else size - other
    return base + lax.rem(s + 1 + shift, size)


def layer_kernel(lags, counts, *refs):
    count_in, count_buffers, count_a, count_asem, count_b, count_bsem = counts
    take = iter(refs)

    def some(count):
        return [next(take) for _ in range(count)]

    (
        hidden_ref,
        attn_gain,
        w_qkv,
        qkv_scale,
        q_gain,
        k_gain,
        keys,
        values,
        lengths,
        w_out,
        out_scale,
        mlp_gain,
        w_gate,
        w_up,
        gate_scale,
        up_scale,
        w_down,
        down_scale,
    ) = some(count_in)
    out_ref = next(take)
    order_ref = next(take)
    order_ref[...] = lane_order(LANES)
    mlp_buffers = some(count_buffers)
    scratch_a, sems_a = some(count_a), some(count_asem)
    scratch_b, sems_b = some(count_b), some(count_bsem)
    here = tuple(lax.axis_index(name) for name in ("grp", "tp", "src")) + tuple(
        lax.axis_size(name) for name in ("grp", "tp", "src")
    )
    attention = attention_phase(
        here,
        (
            hidden_ref,
            attn_gain,
            w_qkv,
            qkv_scale,
            q_gain,
            k_gain,
            keys,
            values,
            lengths,
            w_out,
            out_scale,
            mlp_gain,
            (w_gate, w_up, w_down),
            order_ref,
        ),
        mlp_buffers,
        scratch_a,
        sems_a,
    )
    mlp_phase(
        here,
        lags,
        (gate_scale, up_scale, down_scale, order_ref),
        mlp_buffers,
        scratch_b,
        sems_b,
        attention,
        out_ref,
    )


def layer(args, lags):
    (
        hidden_in,
        attn_gain,
        w_qkv,
        qkv_scale,
        q_gain,
        k_gain,
        key_cache,
        value_cache,
        lengths,
        w_out,
        out_scale,
        mlp_gain,
        w_gate,
        w_up,
        gate_scale,
        up_scale,
        w_down,
        down_scale,
    ) = args
    count_g, count_t, count_s = (lax.axis_size(name) for name in ("grp", "tp", "src"))
    group_rows, model = hidden_in.shape
    rows = group_rows * count_s
    half = rows // 2
    mine = group_rows // count_t
    packed_rows, hidden = w_gate.shape
    packed_hidden, block = w_down.shape
    depth = 2 * block
    chunks = hidden // LANES
    share = model // count_t
    slots = count_g * count_s
    steps = 10 if w_qkv.shape[0] % 320 == 0 else w_qkv.shape[0] // 32
    out_steps = 10 if model % (10 * LANES) == 0 else model // LANES
    qkv_columns = w_qkv.shape[1]
    head_rows = QUERY_HEADS * mine
    bf16, f32, i32 = jnp.bfloat16, jnp.float32, jnp.int32
    dma = pltpu.SemaphoreType.DMA
    vmem = pl.BlockSpec(memory_space=pltpu.VMEM)
    smem = pl.BlockSpec(memory_space=pltpu.SMEM)
    hbm = pl.BlockSpec(memory_space=pl.ANY)
    buffers = [
        pltpu.VMEM((2, packed_rows, hidden), i32),
        pltpu.VMEM((2, packed_rows, hidden), i32),
        pltpu.VMEM((2, packed_hidden, block), i32),
        pltpu.VMEM((rows, depth), bf16),
        pltpu.VMEM((group_rows, share), bf16),
    ]
    scratch_a = [
        pltpu.VMEM(w_qkv.shape, i32),
        pltpu.VMEM(w_out.shape, i32),
        pltpu.VMEM((4 * w_out.shape[0], model), bf16),
        pltpu.VMEM(key_cache.shape[1:], bf16),
        pltpu.VMEM(value_cache.shape[1:], bf16),
        pltpu.VMEM((group_rows, model), bf16),
        pltpu.VMEM((group_rows, qkv_columns), f32),
        pltpu.VMEM((group_rows, qkv_columns), bf16),
        pltpu.VMEM((count_t, mine, qkv_columns), bf16),
        pltpu.VMEM((head_rows, HEAD_SIZE), f32),
        pltpu.VMEM((head_rows, HEAD_SIZE), f32),
        pltpu.VMEM((head_rows, key_cache.shape[2]), f32),
        pltpu.VMEM((head_rows, HEAD_SIZE), f32),
        pltpu.VMEM((head_rows, HEAD_SIZE), f32),
        pltpu.VMEM((head_rows, HEAD_SIZE), f32),
        pltpu.VMEM((head_rows, HEAD_SIZE), bf16),
        pltpu.VMEM((count_t, head_rows // count_t, HEAD_SIZE), bf16),
        pltpu.VMEM((group_rows, model), bf16),
        pltpu.VMEM((count_t, mine, model), bf16),
        pltpu.VMEM((count_t, mine, share), bf16),
        pltpu.VMEM((count_s, mine, depth), bf16),
    ]
    sems_a = [
        dma((steps,)),
        dma((out_steps,)),
        dma((2,)),
        dma((3,)),
        dma((3,)),
        dma((3,)),
        dma((count_t,)),
        dma((count_t,)),
        dma((count_t,)),
        dma((count_t,)),
        dma((count_t,)),
        dma((count_t,)),
        dma((count_t,)),
        dma((count_t,)),
        dma((count_s,)),
        dma((count_t,)),
        dma((count_s, count_t)),
    ]
    scratch_b = [
        pltpu.VMEM((2, chunks, half, 2 * LANES), bf16),
        pltpu.VMEM((2, chunks, half, 2 * LANES), bf16),
        pltpu.VMEM((2, chunks, half, LANES), bf16),
        pltpu.VMEM((rows, depth), f32),
        pltpu.VMEM((2, count_s, group_rows, block), bf16),
        pltpu.VMEM((slots, group_rows, block), bf16),
    ]
    sems_b = [
        dma((2,)),
        dma((2, chunks)),
        dma((2,)),
        dma((2, chunks)),
        dma((2, count_s)),
        dma((slots,)),
    ]
    specs = [vmem] * len(args)
    for place in (2, 6, 7, 9, 12, 13, 16):
        specs[place] = hbm
    specs[8] = smem
    counts = (
        len(specs),
        len(buffers),
        len(scratch_a),
        len(sems_a),
        len(scratch_b),
        len(sems_b),
    )
    return pl.pallas_call(
        functools.partial(layer_kernel, lags, counts),
        out_shape=jax.ShapeDtypeStruct((group_rows, share), f32),
        in_specs=specs,
        out_specs=vmem,
        scratch_shapes=[pltpu.VMEM((LANES, LANES), bf16)] + buffers + scratch_a + sems_a + scratch_b + sems_b,
        compiler_params=pltpu.CompilerParams(
            collective_id=1, has_side_effects=True, vmem_limit_bytes=63 * 1024 * 1024
        ),
        name="layer",
    )(*args).astype(bf16)


def fast_layer(args):
    hidden_in, w_qkv, w_out, w_gate, w_down = (args[k] for k in (0, 2, 9, 12, 16))
    grp, tp, src = (lax.axis_size(name) for name in ("grp", "tp", "src"))
    rows, model = hidden_in.shape
    return (
        grp == 2
        and src > 1
        and tp > 1
        and (grp * src) % tp == 0
        and rows % (16 * tp) == 0
        and QUERY_HEADS % tp == 0
        and model % (LANES * tp) == 0
        and w_qkv.shape[0] % 32 == 0
        and w_qkv.shape[1] % HEAD_SIZE == 0
        and w_out.shape[0] % 32 == 0
        and w_gate.shape[0] % 32 == 0
        and w_gate.shape[1] % LANES == 0
        and w_down.shape[1] % LANES == 0
        and args[6].shape[2] == LANES
        and HEAD_SIZE == LANES
    )


def local(
    hidden_in,
    attn_gain,
    w_qkv,
    qkv_scale,
    q_gain,
    k_gain,
    key_cache,
    value_cache,
    lengths,
    w_out,
    out_scale,
    mlp_gain,
    w_gate,
    w_up,
    gate_scale,
    up_scale,
    w_down,
    down_scale,
):
    args = (
        hidden_in,
        attn_gain,
        w_qkv,
        qkv_scale,
        q_gain,
        k_gain,
        key_cache,
        value_cache,
        lengths,
        w_out,
        out_scale,
        mlp_gain,
        w_gate,
        w_up,
        gate_scale,
        up_scale,
        w_down,
        down_scale,
    )
    if fast_layer(args):
        return layer(args, (4, 6))
    tp_count = lax.axis_size("tp")
    tp_index = lax.axis_index("tp")
    share_cols = D // tp_count
    residual = hidden_in.astype(jnp.float32)
    normed = normalize_rows(residual, attn_gain).astype(jnp.bfloat16)
    qkv_part = (byte_product(normed, w_qkv) * qkv_scale).astype(jnp.bfloat16)
    query_key_value_rows = lax.all_to_all(qkv_part, "tp", split_axis=0, concat_axis=1, tiled=True)
    heads_out = local_attention(
        query_key_value_rows, q_gain, k_gain, key_cache[0], value_cache[0], lengths[0]
    )
    head_rows = lax.all_to_all(heads_out, "tp", split_axis=1, concat_axis=0, tiled=True)
    partial_value = (byte_product(head_rows, w_out) * out_scale).astype(jnp.bfloat16)
    residual_share = lax.dynamic_slice_in_dim(hidden_in, tp_index * share_cols, share_cols, 1)
    mid_share = (
        residual_share.astype(jnp.float32) + summed_share(partial_value, tp_count)
    ).astype(jnp.bfloat16)
    mid_full = lax.all_gather(mid_share, "tp", axis=1, tiled=True)
    normed_mlp = normalize_rows(mid_full.astype(jnp.float32), mlp_gain).astype(jnp.bfloat16)
    mlp_columns = order_bytes(
        lax.all_to_all(normed_mlp, ("grp", "src"), split_axis=1, concat_axis=0, tiled=True)
    )
    gate_terms = jnp.dot(mlp_columns, unpack_ordered(w_gate), preferred_element_type=jnp.float32)
    up_terms = jnp.dot(mlp_columns, unpack_ordered(w_up), preferred_element_type=jnp.float32)
    both_terms = jnp.concatenate(
        [gate_terms.astype(jnp.bfloat16), up_terms.astype(jnp.bfloat16)], axis=1
    )
    both = summed_rows(summed_rows(both_terms, "grp").astype(jnp.bfloat16), "src")
    hidden = gate_scale.shape[0]
    gate_value = both[:, :hidden] * gate_scale
    up_value = both[:, hidden:] * up_scale
    activated = order_bytes((jax.nn.silu(gate_value) * up_value).astype(jnp.bfloat16))
    all_activated = gathered_rows(gathered_rows(activated, "src"), "grp")
    down_columns = jnp.dot(
        all_activated, unpack_ordered(w_down), preferred_element_type=jnp.float32
    ).astype(jnp.bfloat16)
    down_rows = lax.all_to_all(
        down_columns, ("grp", "src"), split_axis=0, concat_axis=1, tiled=True
    )
    down_share = lax.dynamic_slice_in_dim(down_scale, tp_index * share_cols, share_cols, 0)
    mlp_share = summed_share(down_rows, tp_count) * down_share
    return (mid_share.astype(jnp.float32) + mlp_share).astype(jnp.bfloat16)


def solution(mesh):
    return jax.shard_map(
        local,
        mesh=mesh,
        in_specs=(
            P(("grp", "src"), None),
            P(),
            P(None, "tp"),
            P("tp"),
            P(),
            P(),
            P(("grp", "src"), "tp", None, None),
            P(("grp", "src"), "tp", None, None),
            P(("grp", "src"), "tp"),
            P("tp", None),
            P(),
            P(),
            P(("grp", "src"), "tp"),
            P(("grp", "src"), "tp"),
            P("tp"),
            P("tp"),
            P("tp", ("grp", "src")),
            P(),
        ),
        out_specs=P(("grp", "src"), "tp"),
        check_vma=False,
    )
```

```python
import functools
import math

import jax
import jax.numpy as jnp
from jax import lax
from jax.experimental import pallas as pl
from jax.experimental.pallas import tpu as pltpu
from jax.sharding import PartitionSpec as P

D = 5120
QUERY_HEADS = 32
KEY_VALUE_HEADS = 4
HEAD_SIZE = 128
QUERY_COLUMNS = 4096
KEY_COLUMNS = 512


norm_epsilon = 1e-06
rope_base = 1000000.0


def unpack_bytes(packed, byte_index):
    return jnp.right_shift(jnp.left_shift(packed, 24 - 8 * byte_index), 24)


def byte_order(block):
    source = lax.broadcasted_iota(jnp.int32, (block, block), 0)
    target = lax.broadcasted_iota(jnp.int32, (block, block), 1)
    return (target == (source % 4) * (block // 4) + source // 4).astype(jnp.bfloat16)


def split_kernel(block, x_ref, order_ref, out_ref):
    lanes = block // 4
    for c in range(x_ref.shape[1] // block):
        moved = jnp.dot(
            x_ref[:, c * block : (c + 1) * block],
            order_ref[...],
            preferred_element_type=jnp.float32,
        ).astype(jnp.bfloat16)
        for j in range(4):
            out_ref[j, :, c * lanes : (c + 1) * lanes] = moved[:, j * lanes : (j + 1) * lanes]


def split_bytes(activations):
    rows, width = activations.shape
    if width % 512:
        return [activations[:, byte_index::4] for byte_index in range(4)]
    split = pl.pallas_call(
        functools.partial(split_kernel, 512),
        out_shape=jax.ShapeDtypeStruct((4, rows, width // 4), jnp.bfloat16),
        cost_estimate=pl.CostEstimate(
            flops=2 * rows * width * 512, bytes_accessed=4 * rows * width, transcendentals=0
        ),
        name="split_bytes",
    )(activations, byte_order(512))
    return [split[byte_index] for byte_index in range(4)]


def byte_product(activations, packed):
    pieces = split_bytes(activations)
    products = [
        jnp.dot(
            pieces[byte_index],
            unpack_bytes(packed, byte_index).astype(jnp.bfloat16),
            preferred_element_type=jnp.float32,
        )
        for byte_index in range(4)
    ]
    return products[0] + products[1] + products[2] + products[3]


def block_of(width):
    return math.gcd(640, width)


def order_kernel(block, x_ref, order_ref, out_ref):
    for c in range(x_ref.shape[1] // block):
        out_ref[:, c * block : (c + 1) * block] = jnp.dot(
            x_ref[:, c * block : (c + 1) * block],
            order_ref[...],
            preferred_element_type=jnp.float32,
        ).astype(jnp.bfloat16)


def order_bytes(activations):
    rows, width = activations.shape
    block = block_of(width)
    if block == width:
        return jnp.dot(activations, byte_order(block), preferred_element_type=jnp.float32).astype(
            jnp.bfloat16
        )
    return pl.pallas_call(
        functools.partial(order_kernel, block),
        out_shape=jax.ShapeDtypeStruct((rows, width), jnp.bfloat16),
        cost_estimate=pl.CostEstimate(
            flops=2 * rows * width * block, bytes_accessed=4 * rows * width, transcendentals=0
        ),
        name="order_bytes",
    )(activations, byte_order(block))


def unpack_ordered(packed):
    rows, columns = packed.shape
    block = block_of(4 * rows) // 4
    blocks = packed.reshape(rows // block, block, columns)
    parts = [unpack_bytes(blocks, j).astype(jnp.bfloat16) for j in range(4)]
    return jnp.stack(parts, axis=1).reshape(4 * rows, columns)


def normalize_rows(values, gain_row):
    return (
        values
        * lax.rsqrt(jnp.mean(values * values, axis=-1, keepdims=True) + norm_epsilon)
        * gain_row
    )


def rotary_embed(values, positions):
    half_dim = values.shape[-1] // 2
    freq_index = jnp.arange(half_dim, dtype=jnp.float32)
    inverse = jnp.exp(freq_index * (-math.log(rope_base) / half_dim))
    angles = positions.astype(jnp.float32)[:, None] * inverse[None, :]
    cosine = jnp.cos(angles)[:, None, :]
    sine_part = jnp.sin(angles)[:, None, :]
    lower_half = values[..., :half_dim]
    upper_half = values[..., half_dim:]
    return jnp.concatenate(
        [
            lower_half * cosine - upper_half * sine_part,
            upper_half * cosine + lower_half * sine_part,
        ],
        axis=-1,
    )


def local_attention(query_key_value_rows, q_gain, k_gain, stored_keys, stored_values, seq_lengths):
    count_of_rows = query_key_value_rows.shape[0]
    cache_length = stored_keys.shape[1]
    query_matrix = (
        query_key_value_rows[:, :QUERY_COLUMNS]
        .astype(jnp.float32)
        .reshape(count_of_rows, QUERY_HEADS, HEAD_SIZE)
    )
    incoming_keys = (
        query_key_value_rows[:, QUERY_COLUMNS : QUERY_COLUMNS + KEY_COLUMNS]
        .astype(jnp.float32)
        .reshape(count_of_rows, KEY_VALUE_HEADS, HEAD_SIZE)
    )
    incoming_values = query_key_value_rows[:, QUERY_COLUMNS + KEY_COLUMNS :].reshape(
        count_of_rows, KEY_VALUE_HEADS, HEAD_SIZE
    )
    query_matrix = rotary_embed(normalize_rows(query_matrix, q_gain), seq_lengths).astype(
        jnp.bfloat16
    )
    incoming_keys = rotary_embed(normalize_rows(incoming_keys, k_gain), seq_lengths).astype(
        jnp.bfloat16
    )
    query_groups = query_matrix.reshape(
        count_of_rows, KEY_VALUE_HEADS, QUERY_HEADS // KEY_VALUE_HEADS, HEAD_SIZE
    )
    key_slices = stored_keys.reshape(count_of_rows, cache_length, KEY_VALUE_HEADS, HEAD_SIZE)
    value_slices = stored_values.reshape(count_of_rows, cache_length, KEY_VALUE_HEADS, HEAD_SIZE)
    logit_scale = 1.0 / math.sqrt(HEAD_SIZE)
    scores = (
        jnp.einsum("bkgd,bpkd->bkgp", query_groups, key_slices, preferred_element_type=jnp.float32)
        * logit_scale
    )
    live_mask = jnp.arange(cache_length, dtype=jnp.int32)[None, :] < seq_lengths[:, None]
    scores = jnp.where(live_mask[:, None, None, :], scores, -jnp.inf)
    self_score = (
        jnp.einsum("nufi,nui->nuf", query_groups, incoming_keys, preferred_element_type=jnp.float32)
        * logit_scale
    )
    row_max = jnp.maximum(jnp.max(scores, axis=-1), self_score)
    soft_weights = jnp.exp(scores - row_max[..., None])
    own_weight = jnp.exp(self_score - row_max)
    denominator = jnp.sum(soft_weights, axis=-1) + own_weight
    own_low = lax.optimization_barrier(own_weight.astype(jnp.bfloat16)).astype(jnp.float32)
    numerator = jnp.einsum(
        "bkgp,bpkd->bkgd",
        soft_weights.astype(jnp.bfloat16),
        value_slices,
        preferred_element_type=jnp.float32,
    )
    numerator = numerator + own_low[..., None] * incoming_values.astype(jnp.float32)[:, :, None, :]
    return (
        (numerator / denominator[..., None])
        .reshape(count_of_rows, QUERY_COLUMNS)
        .astype(jnp.bfloat16)
    )


def summed_share(terms, tp_count):
    rows, columns = terms.shape
    pieces = lax.all_to_all(terms, "tp", split_axis=1, concat_axis=0, tiled=True)
    return jnp.sum(
        pieces.reshape(tp_count, rows, columns // tp_count).astype(jnp.float32), axis=0
    )


def gathered_rows(rows, axis):
    count = lax.axis_size(axis)
    copies = jnp.broadcast_to(rows[None], (count, *rows.shape))
    pieces = lax.all_to_all(copies, axis, split_axis=0, concat_axis=0)
    return pieces.reshape(count * rows.shape[0], rows.shape[1])


def summed_rows(terms, axis):
    count = lax.axis_size(axis)
    rows, columns = terms.shape
    pieces = lax.all_to_all(
        terms.reshape(count, rows // count, columns), axis, split_axis=0, concat_axis=0
    )
    return jnp.sum(pieces.astype(jnp.float32), axis=0)


LANES = 128
MESH = pl.DeviceIdType.MESH


def lane_order(block):
    source = lax.broadcasted_iota(jnp.int32, (block, block), 0)
    target = lax.broadcasted_iota(jnp.int32, (block, block), 1)
    return (target == (source % 4) * (block // 4) + source // 4).astype(jnp.bfloat16)


def unpack_slab(packed):
    rows, columns = packed.shape
    slab = LANES // 4
    parts = []
    for k in range(rows // slab):
        words = packed[k * slab : (k + 1) * slab]
        for j in range(4):
            parts.append(jnp.right_shift(words, 8 * j).astype(jnp.int8).astype(jnp.bfloat16))
    return jnp.concatenate(parts, axis=0)


def stack_lanes(values):
    blocks = values.shape[1] // LANES
    return jnp.concatenate([values[:, k * LANES : (k + 1) * LANES] for k in range(blocks)], axis=0)


def ordered(stacked, order_ref):
    return jnp.dot(stacked, order_ref[...], preferred_element_type=jnp.float32).astype(jnp.bfloat16)


def row_of(ref):
    return ref[...].reshape(1, ref.shape[0])


def attention_phase(here, inputs, mlp_buffers, scratch, sems):
    g, t, s, count_g, count_t, count_s = here
    (
        hidden_ref,
        attn_gain,
        w_qkv,
        qkv_scale,
        q_gain,
        k_gain,
        keys,
        values,
        lengths,
        w_out,
        out_scale,
        mlp_gain,
        weights,
        order_ref,
    ) = inputs
    gate_v, up_v, down_v, x_v, mid_v = mlp_buffers
    (
        qkv_w,
        out_w,
        out_u,
        keys_v,
        values_v,
        normed_v,
        qkv_acc,
        qkv_send,
        qkv_recv,
        q_v,
        own_v,
        score_v,
        own_e_v,
        denom_v,
        attn_v,
        attn_send,
        attn_recv,
        proj_v,
        proj_recv,
        mid_send,
        x_send,
    ) = scratch
    (
        qkv_w_sem,
        out_w_sem,
        cache_sem,
        swap_send_sem,
        swap_recv_sem,
        load_sem,
        qkv_send_sem,
        qkv_recv_sem,
        attn_send_sem,
        attn_recv_sem,
        proj_send_sem,
        proj_recv_sem,
        mid_send_sem,
        mid_recv_sem,
        z_send_sem,
        x_send_sem,
        x_recv_sem,
    ) = sems
    f32, bf16 = jnp.float32, jnp.bfloat16
    rows, model = hidden_ref.shape
    mine = rows // count_t
    qkv_columns = w_qkv.shape[1]
    steps = qkv_w_sem.shape[0]
    step_rows = w_qkv.shape[0] // steps
    out_steps = out_w_sem.shape[0]
    out_width = model // out_steps
    share = model // count_t
    positions = keys_v.shape[1]
    heads = QUERY_HEADS
    per_kv = QUERY_HEADS // KEY_VALUE_HEADS
    heads_t = heads // count_t

    def qkv_load(i):
        part = pl.ds(pl.multiple_of(i * step_rows, step_rows), step_rows)
        return pltpu.make_async_copy(w_qkv.at[part, :], qkv_w.at[part, :], qkv_w_sem.at[i])

    def out_load(i):
        part = pl.ds(pl.multiple_of(i * out_width, LANES), out_width)
        return pltpu.make_async_copy(w_out.at[:, part], out_w.at[:, part], out_w_sem.at[i])

    for i in range(steps):
        qkv_load(i).start()
    cache = [
        pltpu.make_async_copy(keys.at[0], keys_v, cache_sem.at[0]),
        pltpu.make_async_copy(values.at[0], values_v, cache_sem.at[1]),
    ]
    for copy in cache:
        copy.start()
    for i in range(out_steps):
        out_load(i).start()

    barrier = pltpu.get_barrier_semaphore()
    for tt in range(count_t):
        for ss in range(count_s):

            @pl.when((tt != t) | (ss != s))
            def _():
                pl.semaphore_signal(
                    barrier, inc=1, device_id={"tp": tt, "src": ss}, device_id_type=MESH
                )

    pl.semaphore_signal(barrier, inc=1, device_id={"grp": 1 - g}, device_id_type=MESH)

    with jax.named_scope("norm"):
        normed = normalize_rows(hidden_ref[...].astype(f32), row_of(attn_gain)).astype(bf16)
        moved = ordered(stack_lanes(normed), order_ref)
        for k in range(model // LANES):
            normed_v[:, k * LANES : (k + 1) * LANES] = moved[k * rows : (k + 1) * rows]

    swaps = [
        pltpu.make_async_remote_copy(
            src_ref=source,
            dst_ref=target.at[1],
            send_sem=swap_send_sem.at[index],
            recv_sem=swap_recv_sem.at[index],
            device_id={"grp": 1 - g},
            device_id_type=MESH,
        )
        for index, (source, target) in enumerate(zip(weights, (gate_v, up_v, down_v)))
    ]
    loads = [
        pltpu.make_async_copy(source, target.at[0], load_sem.at[index])
        for index, (source, target) in enumerate(zip(weights, (gate_v, up_v, down_v)))
    ]

    qkv_acc[...] = jnp.zeros_like(qkv_acc)

    def qkv_step(i, carry):
        qkv_load(i).wait()
        part = pl.ds(pl.multiple_of(i * step_rows, step_rows), step_rows)
        depth = pl.ds(pl.multiple_of(i * 4 * step_rows, LANES), 4 * step_rows)
        qkv_acc[...] += jnp.dot(
            normed_v[:, depth], unpack_slab(qkv_w[part, :]), preferred_element_type=f32
        )
        return carry

    with jax.named_scope("qkv"):
        lax.fori_loop(0, steps, qkv_step, 0)
        pl.semaphore_wait(barrier, count_t * count_s)
        for copy in swaps + loads:
            copy.start()
        qkv_send[...] = (qkv_acc[...] * row_of(qkv_scale)).astype(bf16)

    def peer_of(shift):
        return lax.rem(t + shift, count_t)

    def rows_of(index):
        return pl.ds(pl.multiple_of(index * mine, mine), mine)

    def qkv_copy(peer, slot):
        return pltpu.make_async_remote_copy(
            src_ref=qkv_send.at[rows_of(peer), :],
            dst_ref=qkv_recv.at[slot],
            send_sem=qkv_send_sem.at[peer],
            recv_sem=qkv_recv_sem.at[slot],
            device_id={"tp": peer},
            device_id_type=MESH,
        )

    for shift in range(1, count_t):
        qkv_copy(peer_of(shift), t).start()
    qkv_recv[t] = qkv_send[rows_of(t), :]

    def unpack_out(i, carry):
        out_load(i).wait()
        part = pl.ds(pl.multiple_of(i * out_width, LANES), out_width)
        out_u[:, part] = unpack_slab(out_w[:, part])
        return carry

    with jax.named_scope("unpack_out"):
        lax.fori_loop(0, out_steps, unpack_out, 0)

    row_index = lax.broadcasted_iota(jnp.int32, (mine, HEAD_SIZE), 0)
    lane = lax.broadcasted_iota(jnp.int32, (mine, HEAD_SIZE), 1)
    place = jnp.zeros((mine, HEAD_SIZE), f32)
    for b in range(mine):
        place = jnp.where(row_index == b, lengths[0, b].astype(f32), place)
    half_dim = HEAD_SIZE // 2
    low = lane < half_dim
    frequency = jnp.where(low, lane, lane - half_dim).astype(f32)
    angle = place * jnp.exp(frequency * (-math.log(rope_base) / half_dim))
    cosine = jnp.cos(angle)
    sine = jnp.sin(angle)
    sine = jnp.where(low, -sine, sine)

    with jax.named_scope("wait_qkv"):
        for shift in range(1, count_t):
            qkv_copy(t, peer_of(shift)).wait_recv()

    per_share = qkv_columns // HEAD_SIZE

    def head_of(h):
        column = (h % per_share) * HEAD_SIZE
        return qkv_recv[h // per_share, :, column : column + HEAD_SIZE]

    def turned(first, count, gain):
        stacked = jnp.concatenate([head_of(first + k) for k in range(count)], axis=0)
        value = normalize_rows(stacked.astype(f32), gain)
        other = pltpu.roll(value, half_dim, 1)
        wide = [jnp.concatenate([table] * count, axis=0) for table in (cosine, sine)]
        return (value * wide[0] + other * wide[1]).astype(bf16).astype(f32)

    logit_scale = 1.0 / math.sqrt(HEAD_SIZE)
    q_row, k_row = row_of(q_gain), row_of(k_gain)
    with jax.named_scope("rope"):
        new_keys = turned(heads, KEY_VALUE_HEADS, k_row)
        for kv in range(KEY_VALUE_HEADS):
            part = slice(kv * per_kv * mine, (kv + 1) * per_kv * mine)
            query = turned(kv * per_kv, per_kv, q_row)
            q_v[part] = query
            new_key = jnp.concatenate([new_keys[kv * mine : (kv + 1) * mine]] * per_kv, axis=0)
            own = jnp.sum(query * new_key, axis=1, keepdims=True) * logit_scale
            own_v[part] = jnp.broadcast_to(own, query.shape)
    for copy in cache:
            copy.wait()

    zeros = jnp.zeros((per_kv, HEAD_SIZE), f32)
    with jax.named_scope("scores"):
        for b in range(mine):
            query = q_v[pl.ds(b, heads, stride=mine), :]
            spread = jnp.concatenate(
                [
                    jnp.concatenate(
                        [
                            query[kv * per_kv : (kv + 1) * per_kv] if kv == place_of else zeros
                            for place_of in range(KEY_VALUE_HEADS)
                        ],
                        axis=1,
                    )
                    for kv in range(KEY_VALUE_HEADS)
                ],
                axis=0,
            ).astype(bf16)
            score_v[b * heads : (b + 1) * heads] = lax.dot_general(
                spread, keys_v[b], (((1,), (1,)), ((), ())), preferred_element_type=f32
            )
    position = lax.broadcasted_iota(jnp.int32, (heads, positions), 1)
    with jax.named_scope("softmax"):
        for b in range(mine):
            strided = pl.ds(b, heads, stride=mine)
            scores = score_v[b * heads : (b + 1) * heads] * logit_scale
            scores = jnp.where(position < lengths[0, b], scores, -jnp.inf)
            own = own_v[strided, :]
            top = jnp.maximum(jnp.max(scores, axis=1, keepdims=True), own)
            weight = jnp.exp(scores - top)
            own_e = jnp.exp(own - top)
            denominator = jnp.sum(weight, axis=1, keepdims=True) + own_e
            score_v[b * heads : (b + 1) * heads] = weight
            own_e_v[strided, :] = own_e
            denom_v[strided, :] = denominator
    with jax.named_scope("mix"):
        for b in range(mine):
            mixed = jnp.dot(
                score_v[b * heads : (b + 1) * heads].astype(bf16),
                values_v[b],
                preferred_element_type=f32,
            )
            attn_v[pl.ds(b, heads, stride=mine), :] = jnp.concatenate(
                [
                    mixed[kv * per_kv : (kv + 1) * per_kv, kv * HEAD_SIZE : (kv + 1) * HEAD_SIZE]
                    for kv in range(KEY_VALUE_HEADS)
                ],
                axis=0,
            )
    with jax.named_scope("finish_attn"):
        finished = []
        for h in range(heads):
            part = slice(h * mine, (h + 1) * mine)
            new_value = head_of(heads + KEY_VALUE_HEADS + h // per_kv).astype(f32)
            own_low = own_e_v[part].astype(bf16).astype(f32)
            finished.append(((attn_v[part] + own_low * new_value) / denom_v[part]).astype(bf16))
        attn_send[...] = ordered(jnp.concatenate(finished, axis=0), order_ref)

    head_rows = heads_t * mine

    def attn_copy(peer, slot):
        return pltpu.make_async_remote_copy(
            src_ref=attn_send.at[pl.ds(pl.multiple_of(peer * head_rows, head_rows), head_rows), :],
            dst_ref=attn_recv.at[slot],
            send_sem=attn_send_sem.at[peer],
            recv_sem=attn_recv_sem.at[slot],
            device_id={"tp": peer},
            device_id_type=MESH,
        )

    for shift in range(1, count_t):
        attn_copy(peer_of(shift), t).start()
    attn_recv[t] = attn_send[pl.ds(pl.multiple_of(t * head_rows, head_rows), head_rows), :]
    with jax.named_scope("wait_attn"):
        for shift in range(1, count_t):
            attn_copy(t, peer_of(shift)).wait_recv()

    def proj_copy(peer, slot, i):
        part = pl.ds(pl.multiple_of(i * out_width, LANES), out_width)
        return pltpu.make_async_remote_copy(
            src_ref=proj_v.at[rows_of(peer), part],
            dst_ref=proj_recv.at[slot, :, part],
            send_sem=proj_send_sem.at[peer],
            recv_sem=proj_recv_sem.at[slot],
            device_id={"tp": peer},
            device_id_type=MESH,
        )

    def proj_whole(peer, slot):
        return pltpu.make_async_remote_copy(
            src_ref=proj_v.at[rows_of(peer), :],
            dst_ref=proj_recv.at[slot],
            send_sem=proj_send_sem.at[peer],
            recv_sem=proj_recv_sem.at[slot],
            device_id={"tp": peer},
            device_id_type=MESH,
        )

    def out_step(i, carry):
        part = pl.ds(pl.multiple_of(i * out_width, LANES), out_width)
        left = jnp.concatenate(
            [
                jnp.concatenate(
                    [attn_recv[tt, h * mine : (h + 1) * mine] for tt in range(count_t)], axis=0
                )
                for h in range(heads_t)
            ],
            axis=1,
        )
        product = jnp.dot(left, out_u[:, part], preferred_element_type=f32)
        proj_v[:, part] = (product * out_scale[part].reshape(1, out_width)).astype(bf16)
        for shift in range(1, count_t):
            proj_copy(peer_of(shift), t, i).start()
        return carry

    with jax.named_scope("proj"):
        lax.fori_loop(0, out_steps, out_step, 0)

    with jax.named_scope("mid"):
        total = hidden_ref[rows_of(t), :].astype(f32) + proj_v[rows_of(t), :].astype(f32)
        for shift in range(1, count_t):
            slot = peer_of(shift)

            proj_whole(t, slot).wait_recv()
            total += proj_recv[slot].astype(f32)
        mid = total.astype(bf16)
        for tt in range(count_t):
            mid_send[tt] = mid[:, tt * share : (tt + 1) * share]
        moved = ordered(
            stack_lanes(normalize_rows(mid.astype(f32), row_of(mlp_gain)).astype(bf16)), order_ref
        )
    block = model // (count_g * count_s) // LANES
    with jax.named_scope("order_x"):
        for number in range(count_g * count_s):
            owner = number % count_s
            first = jnp.where(number // count_s == g, 0, block)
            for k in range(block):
                column = pl.multiple_of((first + k) * LANES, LANES)
                source = number * block + k
                x_send[owner, :, pl.ds(column, LANES)] = moved[source * mine : (source + 1) * mine]

    def x_rows(ss, tt):
        return pl.ds(pl.multiple_of((ss * count_t + tt) * mine, mine), mine)

    def z_copy(peer, ss):
        return pltpu.make_async_remote_copy(
            src_ref=x_send.at[peer],
            dst_ref=x_v.at[x_rows(ss, t), :],
            send_sem=z_send_sem.at[peer],
            recv_sem=x_recv_sem.at[ss, t],
            device_id={"src": peer},
            device_id_type=MESH,
        )

    def x_copy(peer, ss, tt):
        return pltpu.make_async_remote_copy(
            src_ref=x_v.at[x_rows(ss, tt), :],
            dst_ref=x_v.at[x_rows(ss, tt), :],
            send_sem=x_send_sem.at[peer],
            recv_sem=x_recv_sem.at[ss, tt],
            device_id={"tp": peer},
            device_id_type=MESH,
        )

    def own_copy(peer):
        return pltpu.make_async_remote_copy(
            src_ref=x_send.at[s],
            dst_ref=x_v.at[x_rows(s, t), :],
            send_sem=x_send_sem.at[peer],
            recv_sem=x_recv_sem.at[s, t],
            device_id={"tp": peer},
            device_id_type=MESH,
        )

    def x_whole(peer):
        return pltpu.make_async_remote_copy(
            src_ref=x_send,
            dst_ref=x_send,
            send_sem=x_send_sem.at[peer],
            recv_sem=x_recv_sem.at[s, t],
            device_id={"tp": peer},
            device_id_type=MESH,
        )

    def mid_copy(peer, slot):
        return pltpu.make_async_remote_copy(
            src_ref=mid_send.at[peer],
            dst_ref=mid_v.at[rows_of(slot), :],
            send_sem=mid_send_sem.at[peer],
            recv_sem=mid_recv_sem.at[slot],
            device_id={"tp": peer},
            device_id_type=MESH,
        )

    with jax.named_scope("spread_z"):
        def near(distance, action):
            for other in (s + distance, s - distance):

                @pl.when((other >= 0) & (other < count_s))
                def _():
                    action(other)

        for distance in range(count_s - 1, 0, -1):
            near(distance, lambda other: z_copy(other, s).start())
        for shift in range(1, count_t):
            own_copy(peer_of(shift)).start()
        x_v[x_rows(s, t), :] = x_send[s]

        def forward(ss):
            z_copy(s, ss).wait_recv()
            for turn in range(1, count_t):
                x_copy(peer_of(turn), ss, t).start()

        for distance in range(1, count_s):
            near(distance, forward)
    for shift in range(1, count_t):
        mid_copy(peer_of(shift), t).start()
    mid_v[rows_of(t), :] = mid_send[t]
    def x_wait(side):
        groups = count_s // 2
        base = jnp.where(side == 1, 0, groups)
        for k in range(groups):
            for turn in range(1, count_t):
                x_copy(t, base + k, peer_of(turn)).wait_recv()


    def finish():
        for shift in range(1, count_t):
            peer = peer_of(shift)
            qkv_copy(peer, t).wait_send()
            attn_copy(peer, t).wait_send()
            mid_copy(peer, t).wait_send()

            proj_whole(peer, t).wait_send()
            x_whole(peer).wait_send()
        for shift in range(1, count_s):
            z_copy(lax.rem(s + shift, count_s), s).wait_send()
        for copy in swaps:
            copy.wait_send()

    def mid_wait():
        for shift in range(1, count_t):
            mid_copy(t, peer_of(shift)).wait_recv()

    return swaps, loads, mid_wait, x_wait, finish


def mlp_phase(here, lags, scales, mlp_buffers, scratch, sems, attention, out_ref):
    g, t, s, count_g, count_t, count_s = here
    gate_scale, up_scale, down_scale, order_ref = scales
    lag, back_lag, far_lag, back_start = lags
    gate_v, up_v, down_v, x_v, mid_v = mlp_buffers
    partial, sum_recv, act, total, part_send, part_recv = scratch
    (
        sum_send_sem,
        sum_recv_sem,
        act_send_sem,
        act_recv_sem,
        part_send_sem,
        part_recv_sem,
    ) = sems
    swaps, loads, mid_wait, x_wait, finish = attention
    rows = x_v.shape[0]
    half = rows // 2
    hidden = gate_v.shape[2]
    block = down_v.shape[2]
    chunks = hidden // LANES
    group_rows = rows // count_s
    total[...] = jnp.zeros_like(total)

    last = count_s - 1
    far = (last - 1) * lag

    def toward(side):
        return s - 1 + 2 * side

    def sum_copy(side, j):
        return pltpu.make_async_remote_copy(
            src_ref=partial.at[side, j],
            dst_ref=sum_recv.at[side, j],
            send_sem=sum_send_sem.at[side],
            recv_sem=sum_recv_sem.at[side, j],
            device_id={"src": toward(side)},
            device_id_type=MESH,
        )

    def act_copy(side, j):
        return pltpu.make_async_remote_copy(
            src_ref=act.at[side, j],
            dst_ref=act.at[side, j],
            send_sem=act_send_sem.at[side],
            recv_sem=act_recv_sem.at[side, j],
            device_id={"src": toward(1 - side)},
            device_id_type=MESH,
        )

    def whole_copy(array, side, sem):
        return pltpu.make_async_remote_copy(
            src_ref=array.at[side],
            dst_ref=array.at[side],
            send_sem=sem.at[side],
            recv_sem=sum_recv_sem.at[side, 0],
            device_id={"src": toward(side)},
            device_id_type=MESH,
        )

    def depth_of(side):
        if isinstance(side, int):
            return last - s if side == 0 else s
        return jnp.where(side == 0, last - s, s)

    def pass_step(side, j):
        depth = depth_of(side)

        @pl.when(depth > 0)
        def _():
            sum_copy(side, j).wait_recv()
            partial[side, j] = (
                partial[side, j].astype(jnp.float32) + sum_recv[side, j].astype(jnp.float32)
            ).astype(jnp.bfloat16)

        sum_copy(side, j).start()

    def end_step(side, j):
        sum_copy(side, j).wait_recv()
        value = partial[side, j].astype(jnp.float32) + sum_recv[side, j].astype(jnp.float32)
        columns = pl.ds(pl.multiple_of(j * LANES, LANES), LANES)
        gate_value = value[:, :LANES] * gate_scale[columns].reshape(1, LANES)
        up_value = value[:, LANES:] * up_scale[columns].reshape(1, LANES)
        activated = (gate_value / (1.0 + jnp.exp(-gate_value)) * up_value).astype(jnp.bfloat16)
        act[side, j] = jnp.dot(
            activated, order_ref[...], preferred_element_type=jnp.float32
        ).astype(jnp.bfloat16)
        act_copy(side, j).start()

    def act_step(side, j):
        depth = last - depth_of(side)
        act_copy(side, j).wait_recv()

        @pl.when(depth < last)
        def _():
            act_copy(side, j).start()

    near = jnp.where(2 * s < count_s, 1, 0)
    is_end = (s == 0) | (s == last)

    def product_step(side, i):
        columns = pl.ds(pl.multiple_of(i * LANES, LANES), LANES)
        gate_w = [unpack_slab(gate_v[index, :, columns]) for index in range(2)]
        up_w = [unpack_slab(up_v[index, :, columns]) for index in range(2)]
        weights = jnp.concatenate(
            [jnp.concatenate(gate_w, axis=0), jnp.concatenate(up_w, axis=0)], axis=1
        )
        row = pl.ds(pl.multiple_of((1 - side) * half, half), half)
        partial[side, i] = jnp.dot(
            x_v[row, :], weights, preferred_element_type=jnp.float32
        ).astype(jnp.bfloat16)

    def step(i, carry):
        for side, wait in ((near, 0), (1 - near, far_lag)):
            k = i - wait

            @pl.when((k >= 0) & (k < chunks))
            def _():
                @pl.when(k == 0)
                def _():
                    x_wait(side)

                product_step(side, k)

            depth = depth_of(side)
            j = i - depth * lag

            @pl.when((depth < last) & (j >= 0) & (j < chunks))
            def _():
                pass_step(side, j)

        return carry

    def end_loop(j, carry):
        for side in range(2):

            @pl.when(depth_of(side) == last)
            def _():
                end_step(side, j)

        return carry

    def back_step(i, carry):
        for side in range(2):
            depth = last - depth_of(side)
            j = i - depth * back_lag

            @pl.when((depth > 0) & (j >= 0) & (j < chunks))
            def _():
                act_step(side, j)

        j = i - jnp.maximum(s, last - s) * back_lag

        @pl.when((j >= 0) & (j < chunks))
        def _():
            @pl.when(j == 0)
            def _():
                loads[2].wait()
                swaps[2].wait_recv()

            slab = LANES // 4
            words = pl.ds(pl.multiple_of(j * slab, slab), slab)
            weights = jnp.concatenate(
                [unpack_slab(down_v[index, words, :]) for index in range(2)], axis=1
            )
            for side in range(2):
                total[(1 - side) * half : (2 - side) * half] += jnp.dot(
                    act[side, j], weights, preferred_element_type=jnp.float32
                )

        return carry

    for index in range(2):
        loads[index].wait()
        swaps[index].wait_recv()
    with jax.named_scope("mlp_loop"):
        lax.fori_loop(0, chunks + far, step, 0)
    with jax.named_scope("end_loop"):
        lax.fori_loop(0, chunks, end_loop, 0)
    with jax.named_scope("back_loop"):
        lax.fori_loop(0, chunks + last * back_lag, back_step, 0)

    per_share = count_g * count_s // count_t

    def part_copy(index, ss):
        number = jnp.where(index == 0, g, count_g - 1 - g) * count_s + s
        owner = number // per_share
        slot = t * per_share + lax.rem(number, per_share)
        return owner, slot, pltpu.make_async_remote_copy(
            src_ref=part_send.at[index, ss],
            dst_ref=part_recv.at[slot],
            send_sem=part_send_sem.at[index, ss],
            recv_sem=part_recv_sem.at[slot],
            device_id={"tp": owner, "src": ss},
            device_id_type=MESH,
        )

    with jax.named_scope("part_send"):
        for shift in range(count_s):
            ss = send_order(s, count_s, shift)
            row = pl.ds(pl.multiple_of(ss * group_rows, group_rows), group_rows)
            for index in range(2):
                owner, slot, copy = part_copy(index, ss)
                piece = total[row, index * block : (index + 1) * block].astype(jnp.bfloat16)
                mine = (owner == t) & (ss == s)

                @pl.when(mine)
                def _():
                    part_recv[slot] = piece

                @pl.when(jnp.logical_not(mine))
                def _():
                    part_send[index, ss] = piece
                    copy.start()

    with jax.named_scope("drain"):
        finish()
        for side in range(2):
            depth = depth_of(side)

            @pl.when(depth < last)
            def _():
                whole_copy(partial, side, sum_send_sem).wait_send()

            @pl.when(depth > 0)
            def _():
                whole_copy(act, side, act_send_sem).wait_send()

    with jax.named_scope("part_wait"):
        for slot in range(count_t * per_share):
            number = t * per_share + slot % per_share
            from_me = (slot // per_share == t) & (lax.rem(number, count_s) == s)

            @pl.when(jnp.logical_not(from_me))
            def _():
                pltpu.make_async_remote_copy(
                    src_ref=part_send.at[0, 0],
                    dst_ref=part_recv.at[slot],
                    send_sem=part_send_sem.at[0, 0],
                    recv_sem=part_recv_sem.at[slot],
                    device_id={"tp": t, "src": s},
                    device_id_type=MESH,
                ).wait_recv()

    mid_wait()
    with jax.named_scope("part_sum"):
        for place in range(per_share):
            value = part_recv[place].astype(jnp.float32)
            for tt in range(1, count_t):
                value += part_recv[tt * per_share + place].astype(jnp.float32)
            columns = slice(place * block, (place + 1) * block)
            scale_at = pl.ds(pl.multiple_of((t * per_share + place) * block, LANES), block)
            out_ref[:, columns] = (
                mid_v[:, columns].astype(jnp.float32) + value * down_scale[scale_at].reshape(1, block)
            )

    for ss in range(count_s):
        for index in range(2):
            owner, slot, copy = part_copy(index, ss)

            @pl.when((owner != t) | (ss != s))
            def _():
                copy.wait_send()


def send_order(s, count_s, shift):
    if count_s % 2:
        return lax.rem(s + 1 + shift, count_s)
    size = count_s // 2
    other = jnp.where(s < size, size, 0)
    base = other if shift < size else size - other
    return base + lax.rem(s + 1 + shift, size)


def layer_kernel(lags, counts, *refs):
    count_in, count_buffers, count_a, count_asem, count_b, count_bsem = counts
    take = iter(refs)

    def some(count):
        return [next(take) for _ in range(count)]

    (
        hidden_ref,
        attn_gain,
        w_qkv,
        qkv_scale,
        q_gain,
        k_gain,
        keys,
        values,
        lengths,
        w_out,
        out_scale,
        mlp_gain,
        w_gate,
        w_up,
        gate_scale,
        up_scale,
        w_down,
        down_scale,
    ) = some(count_in)
    out_ref = next(take)
    order_ref = next(take)
    order_ref[...] = lane_order(LANES)
    mlp_buffers = some(count_buffers)
    scratch_a, sems_a = some(count_a), some(count_asem)
    scratch_b, sems_b = some(count_b), some(count_bsem)
    here = tuple(lax.axis_index(name) for name in ("grp", "tp", "src")) + tuple(
        lax.axis_size(name) for name in ("grp", "tp", "src")
    )
    attention = attention_phase(
        here,
        (
            hidden_ref,
            attn_gain,
            w_qkv,
            qkv_scale,
            q_gain,
            k_gain,
            keys,
            values,
            lengths,
            w_out,
            out_scale,
            mlp_gain,
            (w_gate, w_up, w_down),
            order_ref,
        ),
        mlp_buffers,
        scratch_a,
        sems_a,
    )
    mlp_phase(
        here,
        lags,
        (gate_scale, up_scale, down_scale, order_ref),
        mlp_buffers,
        scratch_b,
        sems_b,
        attention,
        out_ref,
    )


def layer(args, lags):
    (
        hidden_in,
        attn_gain,
        w_qkv,
        qkv_scale,
        q_gain,
        k_gain,
        key_cache,
        value_cache,
        lengths,
        w_out,
        out_scale,
        mlp_gain,
        w_gate,
        w_up,
        gate_scale,
        up_scale,
        w_down,
        down_scale,
    ) = args
    count_g, count_t, count_s = (lax.axis_size(name) for name in ("grp", "tp", "src"))
    group_rows, model = hidden_in.shape
    rows = group_rows * count_s
    half = rows // 2
    mine = group_rows // count_t
    packed_rows, hidden = w_gate.shape
    packed_hidden, block = w_down.shape
    depth = 2 * block
    chunks = hidden // LANES
    share = model // count_t
    slots = count_g * count_s
    steps = 10 if w_qkv.shape[0] % 320 == 0 else w_qkv.shape[0] // 32
    out_steps = 10 if model % (10 * LANES) == 0 else model // LANES
    qkv_columns = w_qkv.shape[1]
    head_rows = QUERY_HEADS * mine
    bf16, f32, i32 = jnp.bfloat16, jnp.float32, jnp.int32
    dma = pltpu.SemaphoreType.DMA
    vmem = pl.BlockSpec(memory_space=pltpu.VMEM)
    smem = pl.BlockSpec(memory_space=pltpu.SMEM)
    hbm = pl.BlockSpec(memory_space=pl.ANY)
    buffers = [
        pltpu.VMEM((2, packed_rows, hidden), i32),
        pltpu.VMEM((2, packed_rows, hidden), i32),
        pltpu.VMEM((2, packed_hidden, block), i32),
        pltpu.VMEM((rows, depth), bf16),
        pltpu.VMEM((group_rows, share), bf16),
    ]
    scratch_a = [
        pltpu.VMEM(w_qkv.shape, i32),
        pltpu.VMEM(w_out.shape, i32),
        pltpu.VMEM((4 * w_out.shape[0], model), bf16),
        pltpu.VMEM(key_cache.shape[1:], bf16),
        pltpu.VMEM(value_cache.shape[1:], bf16),
        pltpu.VMEM((group_rows, model), bf16),
        pltpu.VMEM((group_rows, qkv_columns), f32),
        pltpu.VMEM((group_rows, qkv_columns), bf16),
        pltpu.VMEM((count_t, mine, qkv_columns), bf16),
        pltpu.VMEM((head_rows, HEAD_SIZE), f32),
        pltpu.VMEM((head_rows, HEAD_SIZE), f32),
        pltpu.VMEM((head_rows, key_cache.shape[2]), f32),
        pltpu.VMEM((head_rows, HEAD_SIZE), f32),
        pltpu.VMEM((head_rows, HEAD_SIZE), f32),
        pltpu.VMEM((head_rows, HEAD_SIZE), f32),
        pltpu.VMEM((head_rows, HEAD_SIZE), bf16),
        pltpu.VMEM((count_t, head_rows // count_t, HEAD_SIZE), bf16),
        pltpu.VMEM((group_rows, model), bf16),
        pltpu.VMEM((count_t, mine, model), bf16),
        pltpu.VMEM((count_t, mine, share), bf16),
        pltpu.VMEM((count_s, mine, depth), bf16),
    ]
    sems_a = [
        dma((steps,)),
        dma((out_steps,)),
        dma((2,)),
        dma((3,)),
        dma((3,)),
        dma((3,)),
        dma((count_t,)),
        dma((count_t,)),
        dma((count_t,)),
        dma((count_t,)),
        dma((count_t,)),
        dma((count_t,)),
        dma((count_t,)),
        dma((count_t,)),
        dma((count_s,)),
        dma((count_t,)),
        dma((count_s, count_t)),
    ]
    scratch_b = [
        pltpu.VMEM((2, chunks, half, 2 * LANES), bf16),
        pltpu.VMEM((2, chunks, half, 2 * LANES), bf16),
        pltpu.VMEM((2, chunks, half, LANES), bf16),
        pltpu.VMEM((rows, depth), f32),
        pltpu.VMEM((2, count_s, group_rows, block), bf16),
        pltpu.VMEM((slots, group_rows, block), bf16),
    ]
    sems_b = [
        dma((2,)),
        dma((2, chunks)),
        dma((2,)),
        dma((2, chunks)),
        dma((2, count_s)),
        dma((slots,)),
    ]
    specs = [vmem] * len(args)
    for place in (2, 6, 7, 9, 12, 13, 16):
        specs[place] = hbm
    specs[8] = smem
    counts = (
        len(specs),
        len(buffers),
        len(scratch_a),
        len(sems_a),
        len(scratch_b),
        len(sems_b),
    )
    return pl.pallas_call(
        functools.partial(layer_kernel, lags, counts),
        out_shape=pltpu.VMEM((group_rows, share), f32),
        in_specs=specs,
        out_specs=vmem,
        scratch_shapes=[pltpu.VMEM((LANES, LANES), bf16)] + buffers + scratch_a + sems_a + scratch_b + sems_b,
        compiler_params=pltpu.CompilerParams(
            collective_id=1, has_side_effects=True, vmem_limit_bytes=63 * 1024 * 1024
        ),
        name="layer",
    )(*args).astype(bf16)


def fast_layer(args):
    hidden_in, w_qkv, w_out, w_gate, w_down = (args[k] for k in (0, 2, 9, 12, 16))
    grp, tp, src = (lax.axis_size(name) for name in ("grp", "tp", "src"))
    rows, model = hidden_in.shape
    return (
        grp == 2
        and src > 1
        and tp > 1
        and (grp * src) % tp == 0
        and rows % (16 * tp) == 0
        and QUERY_HEADS % tp == 0
        and model % (LANES * tp) == 0
        and w_qkv.shape[0] % 32 == 0
        and w_qkv.shape[1] % HEAD_SIZE == 0
        and w_out.shape[0] % 32 == 0
        and w_gate.shape[0] % 32 == 0
        and w_gate.shape[1] % LANES == 0
        and w_down.shape[1] % LANES == 0
        and args[6].shape[2] == LANES
        and HEAD_SIZE == LANES
    )


def local(
    hidden_in,
    attn_gain,
    w_qkv,
    qkv_scale,
    q_gain,
    k_gain,
    key_cache,
    value_cache,
    lengths,
    w_out,
    out_scale,
    mlp_gain,
    w_gate,
    w_up,
    gate_scale,
    up_scale,
    w_down,
    down_scale,
):
    args = (
        hidden_in,
        attn_gain,
        w_qkv,
        qkv_scale,
        q_gain,
        k_gain,
        key_cache,
        value_cache,
        lengths,
        w_out,
        out_scale,
        mlp_gain,
        w_gate,
        w_up,
        gate_scale,
        up_scale,
        w_down,
        down_scale,
    )
    if fast_layer(args):
        return layer(args, (4, 6, 4, 4))
    tp_count = lax.axis_size("tp")
    tp_index = lax.axis_index("tp")
    share_cols = D // tp_count
    residual = hidden_in.astype(jnp.float32)
    normed = normalize_rows(residual, attn_gain).astype(jnp.bfloat16)
    qkv_part = (byte_product(normed, w_qkv) * qkv_scale).astype(jnp.bfloat16)
    query_key_value_rows = lax.all_to_all(qkv_part, "tp", split_axis=0, concat_axis=1, tiled=True)
    heads_out = local_attention(
        query_key_value_rows, q_gain, k_gain, key_cache[0], value_cache[0], lengths[0]
    )
    head_rows = lax.all_to_all(heads_out, "tp", split_axis=1, concat_axis=0, tiled=True)
    partial_value = (byte_product(head_rows, w_out) * out_scale).astype(jnp.bfloat16)
    residual_share = lax.dynamic_slice_in_dim(hidden_in, tp_index * share_cols, share_cols, 1)
    mid_share = (
        residual_share.astype(jnp.float32) + summed_share(partial_value, tp_count)
    ).astype(jnp.bfloat16)
    mid_full = lax.all_gather(mid_share, "tp", axis=1, tiled=True)
    normed_mlp = normalize_rows(mid_full.astype(jnp.float32), mlp_gain).astype(jnp.bfloat16)
    mlp_columns = order_bytes(
        lax.all_to_all(normed_mlp, ("grp", "src"), split_axis=1, concat_axis=0, tiled=True)
    )
    gate_terms = jnp.dot(mlp_columns, unpack_ordered(w_gate), preferred_element_type=jnp.float32)
    up_terms = jnp.dot(mlp_columns, unpack_ordered(w_up), preferred_element_type=jnp.float32)
    both_terms = jnp.concatenate(
        [gate_terms.astype(jnp.bfloat16), up_terms.astype(jnp.bfloat16)], axis=1
    )
    both = summed_rows(summed_rows(both_terms, "grp").astype(jnp.bfloat16), "src")
    hidden = gate_scale.shape[0]
    gate_value = both[:, :hidden] * gate_scale
    up_value = both[:, hidden:] * up_scale
    activated = order_bytes((jax.nn.silu(gate_value) * up_value).astype(jnp.bfloat16))
    all_activated = gathered_rows(gathered_rows(activated, "src"), "grp")
    down_columns = jnp.dot(
        all_activated, unpack_ordered(w_down), preferred_element_type=jnp.float32
    ).astype(jnp.bfloat16)
    down_rows = lax.all_to_all(
        down_columns, ("grp", "src"), split_axis=0, concat_axis=1, tiled=True
    )
    down_share = lax.dynamic_slice_in_dim(down_scale, tp_index * share_cols, share_cols, 0)
    mlp_share = summed_share(down_rows, tp_count) * down_share
    return (mid_share.astype(jnp.float32) + mlp_share).astype(jnp.bfloat16)


def solution(mesh):
    return jax.shard_map(
        local,
        mesh=mesh,
        in_specs=(
            P(("grp", "src"), None),
            P(),
            P(None, "tp"),
            P("tp"),
            P(),
            P(),
            P(("grp", "src"), "tp", None, None),
            P(("grp", "src"), "tp", None, None),
            P(("grp", "src"), "tp"),
            P("tp", None),
            P(),
            P(),
            P(("grp", "src"), "tp"),
            P(("grp", "src"), "tp"),
            P("tp"),
            P("tp"),
            P("tp", ("grp", "src")),
            P(),
        ),
        out_specs=P(("grp", "src"), "tp"),
        check_vma=False,
    )
```

```python
import functools
import math

import jax
import jax.numpy as jnp
from jax import lax
from jax.experimental import pallas as pl
from jax.experimental.pallas import tpu as pltpu
from jax.sharding import PartitionSpec as P

D = 5120
QUERY_HEADS = 32
KEY_VALUE_HEADS = 4
HEAD_SIZE = 128
QUERY_COLUMNS = 4096
KEY_COLUMNS = 512


norm_epsilon = 1e-06
rope_base = 1000000.0


def unpack_bytes(packed, byte_index):
    return jnp.right_shift(jnp.left_shift(packed, 24 - 8 * byte_index), 24)


def byte_order(block):
    source = lax.broadcasted_iota(jnp.int32, (block, block), 0)
    target = lax.broadcasted_iota(jnp.int32, (block, block), 1)
    return (target == (source % 4) * (block // 4) + source // 4).astype(jnp.bfloat16)


def split_kernel(block, x_ref, order_ref, out_ref):
    lanes = block // 4
    for c in range(x_ref.shape[1] // block):
        moved = jnp.dot(
            x_ref[:, c * block : (c + 1) * block],
            order_ref[...],
            preferred_element_type=jnp.float32,
        ).astype(jnp.bfloat16)
        for j in range(4):
            out_ref[j, :, c * lanes : (c + 1) * lanes] = moved[:, j * lanes : (j + 1) * lanes]


def split_bytes(activations):
    rows, width = activations.shape
    if width % 512:
        return [activations[:, byte_index::4] for byte_index in range(4)]
    split = pl.pallas_call(
        functools.partial(split_kernel, 512),
        out_shape=jax.ShapeDtypeStruct((4, rows, width // 4), jnp.bfloat16),
        cost_estimate=pl.CostEstimate(
            flops=2 * rows * width * 512, bytes_accessed=4 * rows * width, transcendentals=0
        ),
        name="split_bytes",
    )(activations, byte_order(512))
    return [split[byte_index] for byte_index in range(4)]


def byte_product(activations, packed):
    pieces = split_bytes(activations)
    products = [
        jnp.dot(
            pieces[byte_index],
            unpack_bytes(packed, byte_index).astype(jnp.bfloat16),
            preferred_element_type=jnp.float32,
        )
        for byte_index in range(4)
    ]
    return products[0] + products[1] + products[2] + products[3]


def block_of(width):
    return math.gcd(640, width)


def order_kernel(block, x_ref, order_ref, out_ref):
    for c in range(x_ref.shape[1] // block):
        out_ref[:, c * block : (c + 1) * block] = jnp.dot(
            x_ref[:, c * block : (c + 1) * block],
            order_ref[...],
            preferred_element_type=jnp.float32,
        ).astype(jnp.bfloat16)


def order_bytes(activations):
    rows, width = activations.shape
    block = block_of(width)
    if block == width:
        return jnp.dot(activations, byte_order(block), preferred_element_type=jnp.float32).astype(
            jnp.bfloat16
        )
    return pl.pallas_call(
        functools.partial(order_kernel, block),
        out_shape=jax.ShapeDtypeStruct((rows, width), jnp.bfloat16),
        cost_estimate=pl.CostEstimate(
            flops=2 * rows * width * block, bytes_accessed=4 * rows * width, transcendentals=0
        ),
        name="order_bytes",
    )(activations, byte_order(block))


def unpack_ordered(packed):
    rows, columns = packed.shape
    block = block_of(4 * rows) // 4
    blocks = packed.reshape(rows // block, block, columns)
    parts = [unpack_bytes(blocks, j).astype(jnp.bfloat16) for j in range(4)]
    return jnp.stack(parts, axis=1).reshape(4 * rows, columns)


def normalize_rows(values, gain_row):
    return (
        values
        * lax.rsqrt(jnp.mean(values * values, axis=-1, keepdims=True) + norm_epsilon)
        * gain_row
    )


def rotary_embed(values, positions):
    half_dim = values.shape[-1] // 2
    freq_index = jnp.arange(half_dim, dtype=jnp.float32)
    inverse = jnp.exp(freq_index * (-math.log(rope_base) / half_dim))
    angles = positions.astype(jnp.float32)[:, None] * inverse[None, :]
    cosine = jnp.cos(angles)[:, None, :]
    sine_part = jnp.sin(angles)[:, None, :]
    lower_half = values[..., :half_dim]
    upper_half = values[..., half_dim:]
    return jnp.concatenate(
        [
            lower_half * cosine - upper_half * sine_part,
            upper_half * cosine + lower_half * sine_part,
        ],
        axis=-1,
    )


def local_attention(query_key_value_rows, q_gain, k_gain, stored_keys, stored_values, seq_lengths):
    count_of_rows = query_key_value_rows.shape[0]
    cache_length = stored_keys.shape[1]
    query_matrix = (
        query_key_value_rows[:, :QUERY_COLUMNS]
        .astype(jnp.float32)
        .reshape(count_of_rows, QUERY_HEADS, HEAD_SIZE)
    )
    incoming_keys = (
        query_key_value_rows[:, QUERY_COLUMNS : QUERY_COLUMNS + KEY_COLUMNS]
        .astype(jnp.float32)
        .reshape(count_of_rows, KEY_VALUE_HEADS, HEAD_SIZE)
    )
    incoming_values = query_key_value_rows[:, QUERY_COLUMNS + KEY_COLUMNS :].reshape(
        count_of_rows, KEY_VALUE_HEADS, HEAD_SIZE
    )
    query_matrix = rotary_embed(normalize_rows(query_matrix, q_gain), seq_lengths).astype(
        jnp.bfloat16
    )
    incoming_keys = rotary_embed(normalize_rows(incoming_keys, k_gain), seq_lengths).astype(
        jnp.bfloat16
    )
    query_groups = query_matrix.reshape(
        count_of_rows, KEY_VALUE_HEADS, QUERY_HEADS // KEY_VALUE_HEADS, HEAD_SIZE
    )
    key_slices = stored_keys.reshape(count_of_rows, cache_length, KEY_VALUE_HEADS, HEAD_SIZE)
    value_slices = stored_values.reshape(count_of_rows, cache_length, KEY_VALUE_HEADS, HEAD_SIZE)
    logit_scale = 1.0 / math.sqrt(HEAD_SIZE)
    scores = (
        jnp.einsum("bkgd,bpkd->bkgp", query_groups, key_slices, preferred_element_type=jnp.float32)
        * logit_scale
    )
    live_mask = jnp.arange(cache_length, dtype=jnp.int32)[None, :] < seq_lengths[:, None]
    scores = jnp.where(live_mask[:, None, None, :], scores, -jnp.inf)
    self_score = (
        jnp.einsum("nufi,nui->nuf", query_groups, incoming_keys, preferred_element_type=jnp.float32)
        * logit_scale
    )
    row_max = jnp.maximum(jnp.max(scores, axis=-1), self_score)
    soft_weights = jnp.exp(scores - row_max[..., None])
    own_weight = jnp.exp(self_score - row_max)
    denominator = jnp.sum(soft_weights, axis=-1) + own_weight
    own_low = lax.optimization_barrier(own_weight.astype(jnp.bfloat16)).astype(jnp.float32)
    numerator = jnp.einsum(
        "bkgp,bpkd->bkgd",
        soft_weights.astype(jnp.bfloat16),
        value_slices,
        preferred_element_type=jnp.float32,
    )
    numerator = numerator + own_low[..., None] * incoming_values.astype(jnp.float32)[:, :, None, :]
    return (
        (numerator / denominator[..., None])
        .reshape(count_of_rows, QUERY_COLUMNS)
        .astype(jnp.bfloat16)
    )


def summed_share(terms, tp_count):
    rows, columns = terms.shape
    pieces = lax.all_to_all(terms, "tp", split_axis=1, concat_axis=0, tiled=True)
    return jnp.sum(
        pieces.reshape(tp_count, rows, columns // tp_count).astype(jnp.float32), axis=0
    )


def gathered_rows(rows, axis):
    count = lax.axis_size(axis)
    copies = jnp.broadcast_to(rows[None], (count, *rows.shape))
    pieces = lax.all_to_all(copies, axis, split_axis=0, concat_axis=0)
    return pieces.reshape(count * rows.shape[0], rows.shape[1])


def summed_rows(terms, axis):
    count = lax.axis_size(axis)
    rows, columns = terms.shape
    pieces = lax.all_to_all(
        terms.reshape(count, rows // count, columns), axis, split_axis=0, concat_axis=0
    )
    return jnp.sum(pieces.astype(jnp.float32), axis=0)


LANES = 128
MESH = pl.DeviceIdType.MESH


def lane_order(block):
    source = lax.broadcasted_iota(jnp.int32, (block, block), 0)
    target = lax.broadcasted_iota(jnp.int32, (block, block), 1)
    return (target == (source % 4) * (block // 4) + source // 4).astype(jnp.bfloat16)


def unpack_slab(packed):
    rows, columns = packed.shape
    slab = LANES // 4
    parts = []
    for k in range(rows // slab):
        words = packed[k * slab : (k + 1) * slab]
        for j in range(4):
            parts.append(jnp.right_shift(words, 8 * j).astype(jnp.int8).astype(jnp.bfloat16))
    return jnp.concatenate(parts, axis=0)


def stack_lanes(values):
    blocks = values.shape[1] // LANES
    return jnp.concatenate([values[:, k * LANES : (k + 1) * LANES] for k in range(blocks)], axis=0)


def ordered(stacked, order_ref):
    return jnp.dot(stacked, order_ref[...], preferred_element_type=jnp.float32).astype(jnp.bfloat16)


def row_of(ref):
    return ref[...].reshape(1, ref.shape[0])


def attention_phase(here, inputs, mlp_buffers, scratch, sems):
    g, t, s, count_g, count_t, count_s = here
    (
        hidden_ref,
        attn_gain,
        w_qkv,
        qkv_scale,
        q_gain,
        k_gain,
        keys,
        values,
        lengths,
        w_out,
        out_scale,
        mlp_gain,
        weights,
        order_ref,
    ) = inputs
    gate_v, up_v, down_v, x_v, mid_v = mlp_buffers
    (
        qkv_w,
        out_w,
        out_u,
        keys_v,
        values_v,
        normed_v,
        qkv_acc,
        qkv_send,
        qkv_recv,
        q_v,
        own_v,
        score_v,
        own_e_v,
        denom_v,
        attn_v,
        attn_send,
        attn_recv,
        proj_v,
        proj_recv,
        mid_send,
        x_send,
    ) = scratch
    (
        qkv_w_sem,
        out_w_sem,
        cache_sem,
        swap_send_sem,
        swap_recv_sem,
        load_sem,
        qkv_send_sem,
        qkv_recv_sem,
        attn_send_sem,
        attn_recv_sem,
        proj_send_sem,
        proj_recv_sem,
        mid_send_sem,
        mid_recv_sem,
        z_send_sem,
        x_send_sem,
        x_recv_sem,
    ) = sems
    f32, bf16 = jnp.float32, jnp.bfloat16
    rows, model = hidden_ref.shape
    mine = rows // count_t
    qkv_columns = w_qkv.shape[1]
    steps = qkv_w_sem.shape[0]
    step_rows = w_qkv.shape[0] // steps
    out_steps = out_w_sem.shape[0]
    out_width = model // out_steps
    share = model // count_t
    positions = keys_v.shape[1]
    heads = QUERY_HEADS
    per_kv = QUERY_HEADS // KEY_VALUE_HEADS
    heads_t = heads // count_t

    def qkv_load(i):
        part = pl.ds(pl.multiple_of(i * step_rows, step_rows), step_rows)
        return pltpu.make_async_copy(w_qkv.at[part, :], qkv_w.at[part, :], qkv_w_sem.at[i])

    def out_load(i):
        part = pl.ds(pl.multiple_of(i * out_width, LANES), out_width)
        return pltpu.make_async_copy(w_out.at[:, part], out_w.at[:, part], out_w_sem.at[i])

    for i in range(steps):
        qkv_load(i).start()
    cache = [
        pltpu.make_async_copy(keys.at[0], keys_v, cache_sem.at[0]),
        pltpu.make_async_copy(values.at[0], values_v, cache_sem.at[1]),
    ]
    for copy in cache:
        copy.start()
    for i in range(out_steps):
        out_load(i).start()

    barrier = pltpu.get_barrier_semaphore()
    for tt in range(count_t):
        for ss in range(count_s):

            @pl.when((tt != t) | (ss != s))
            def _():
                pl.semaphore_signal(
                    barrier, inc=1, device_id={"tp": tt, "src": ss}, device_id_type=MESH
                )

    pl.semaphore_signal(barrier, inc=1, device_id={"grp": 1 - g}, device_id_type=MESH)

    with jax.named_scope("norm"):
        normed = normalize_rows(hidden_ref[...].astype(f32), row_of(attn_gain)).astype(bf16)
        moved = ordered(stack_lanes(normed), order_ref)
        for k in range(model // LANES):
            normed_v[:, k * LANES : (k + 1) * LANES] = moved[k * rows : (k + 1) * rows]

    swaps = [
        pltpu.make_async_remote_copy(
            src_ref=source,
            dst_ref=target.at[1],
            send_sem=swap_send_sem.at[index],
            recv_sem=swap_recv_sem.at[index],
            device_id={"grp": 1 - g},
            device_id_type=MESH,
        )
        for index, (source, target) in enumerate(zip(weights, (gate_v, up_v, down_v)))
    ]
    loads = [
        pltpu.make_async_copy(source, target.at[0], load_sem.at[index])
        for index, (source, target) in enumerate(zip(weights, (gate_v, up_v, down_v)))
    ]

    qkv_acc[...] = jnp.zeros_like(qkv_acc)

    def qkv_step(i, carry):
        qkv_load(i).wait()
        part = pl.ds(pl.multiple_of(i * step_rows, step_rows), step_rows)
        depth = pl.ds(pl.multiple_of(i * 4 * step_rows, LANES), 4 * step_rows)
        qkv_acc[...] += jnp.dot(
            normed_v[:, depth], unpack_slab(qkv_w[part, :]), preferred_element_type=f32
        )
        return carry

    with jax.named_scope("qkv"):
        lax.fori_loop(0, steps, qkv_step, 0)
        pl.semaphore_wait(barrier, count_t * count_s)
        for copy in swaps + loads:
            copy.start()
        qkv_send[...] = (qkv_acc[...] * row_of(qkv_scale)).astype(bf16)

    def peer_of(shift):
        return lax.rem(t + shift, count_t)

    def rows_of(index):
        return pl.ds(pl.multiple_of(index * mine, mine), mine)

    def qkv_copy(peer, slot):
        return pltpu.make_async_remote_copy(
            src_ref=qkv_send.at[rows_of(peer), :],
            dst_ref=qkv_recv.at[slot],
            send_sem=qkv_send_sem.at[peer],
            recv_sem=qkv_recv_sem.at[slot],
            device_id={"tp": peer},
            device_id_type=MESH,
        )

    for shift in range(1, count_t):
        qkv_copy(peer_of(shift), t).start()
    qkv_recv[t] = qkv_send[rows_of(t), :]

    def unpack_out(i, carry):
        out_load(i).wait()
        part = pl.ds(pl.multiple_of(i * out_width, LANES), out_width)
        out_u[:, part] = unpack_slab(out_w[:, part])
        return carry

    with jax.named_scope("unpack_out"):
        lax.fori_loop(0, out_steps, unpack_out, 0)

    row_index = lax.broadcasted_iota(jnp.int32, (mine, HEAD_SIZE), 0)
    lane = lax.broadcasted_iota(jnp.int32, (mine, HEAD_SIZE), 1)
    place = jnp.zeros((mine, HEAD_SIZE), f32)
    for b in range(mine):
        place = jnp.where(row_index == b, lengths[0, b].astype(f32), place)
    half_dim = HEAD_SIZE // 2
    low = lane < half_dim
    frequency = jnp.where(low, lane, lane - half_dim).astype(f32)
    angle = place * jnp.exp(frequency * (-math.log(rope_base) / half_dim))
    cosine = jnp.cos(angle)
    sine = jnp.sin(angle)
    sine = jnp.where(low, -sine, sine)

    with jax.named_scope("wait_qkv"):
        for shift in range(1, count_t):
            qkv_copy(t, peer_of(shift)).wait_recv()

    per_share = qkv_columns // HEAD_SIZE

    def head_of(h):
        column = (h % per_share) * HEAD_SIZE
        return qkv_recv[h // per_share, :, column : column + HEAD_SIZE]

    def turned(first, count, gain):
        stacked = jnp.concatenate([head_of(first + k) for k in range(count)], axis=0)
        value = normalize_rows(stacked.astype(f32), gain)
        other = pltpu.roll(value, half_dim, 1)
        wide = [jnp.concatenate([table] * count, axis=0) for table in (cosine, sine)]
        return (value * wide[0] + other * wide[1]).astype(bf16).astype(f32)

    logit_scale = 1.0 / math.sqrt(HEAD_SIZE)
    q_row, k_row = row_of(q_gain), row_of(k_gain)
    with jax.named_scope("rope"):
        new_keys = turned(heads, KEY_VALUE_HEADS, k_row)
        for kv in range(KEY_VALUE_HEADS):
            part = slice(kv * per_kv * mine, (kv + 1) * per_kv * mine)
            query = turned(kv * per_kv, per_kv, q_row)
            q_v[part] = query
            new_key = jnp.concatenate([new_keys[kv * mine : (kv + 1) * mine]] * per_kv, axis=0)
            own = jnp.sum(query * new_key, axis=1, keepdims=True) * logit_scale
            own_v[part] = jnp.broadcast_to(own, query.shape)
    for copy in cache:
            copy.wait()

    zeros = jnp.zeros((per_kv, HEAD_SIZE), f32)
    with jax.named_scope("scores"):
        for b in range(mine):
            query = q_v[pl.ds(b, heads, stride=mine), :]
            spread = jnp.concatenate(
                [
                    jnp.concatenate(
                        [
                            query[kv * per_kv : (kv + 1) * per_kv] if kv == place_of else zeros
                            for place_of in range(KEY_VALUE_HEADS)
                        ],
                        axis=1,
                    )
                    for kv in range(KEY_VALUE_HEADS)
                ],
                axis=0,
            ).astype(bf16)
            score_v[b * heads : (b + 1) * heads] = lax.dot_general(
                spread, keys_v[b], (((1,), (1,)), ((), ())), preferred_element_type=f32
            )
    position = lax.broadcasted_iota(jnp.int32, (heads, positions), 1)
    with jax.named_scope("softmax"):
        for b in range(mine):
            strided = pl.ds(b, heads, stride=mine)
            scores = score_v[b * heads : (b + 1) * heads] * logit_scale
            scores = jnp.where(position < lengths[0, b], scores, -jnp.inf)
            own = own_v[strided, :]
            top = jnp.maximum(jnp.max(scores, axis=1, keepdims=True), own)
            weight = jnp.exp(scores - top)
            own_e = jnp.exp(own - top)
            denominator = jnp.sum(weight, axis=1, keepdims=True) + own_e
            score_v[b * heads : (b + 1) * heads] = weight
            own_e_v[strided, :] = own_e
            denom_v[strided, :] = denominator
    with jax.named_scope("mix"):
        for b in range(mine):
            mixed = jnp.dot(
                score_v[b * heads : (b + 1) * heads].astype(bf16),
                values_v[b],
                preferred_element_type=f32,
            )
            attn_v[pl.ds(b, heads, stride=mine), :] = jnp.concatenate(
                [
                    mixed[kv * per_kv : (kv + 1) * per_kv, kv * HEAD_SIZE : (kv + 1) * HEAD_SIZE]
                    for kv in range(KEY_VALUE_HEADS)
                ],
                axis=0,
            )
    with jax.named_scope("finish_attn"):
        finished = []
        for h in range(heads):
            part = slice(h * mine, (h + 1) * mine)
            new_value = head_of(heads + KEY_VALUE_HEADS + h // per_kv).astype(f32)
            own_low = own_e_v[part].astype(bf16).astype(f32)
            finished.append(((attn_v[part] + own_low * new_value) / denom_v[part]).astype(bf16))
        attn_send[...] = ordered(jnp.concatenate(finished, axis=0), order_ref)

    head_rows = heads_t * mine

    def attn_copy(peer, slot):
        return pltpu.make_async_remote_copy(
            src_ref=attn_send.at[pl.ds(pl.multiple_of(peer * head_rows, head_rows), head_rows), :],
            dst_ref=attn_recv.at[slot],
            send_sem=attn_send_sem.at[peer],
            recv_sem=attn_recv_sem.at[slot],
            device_id={"tp": peer},
            device_id_type=MESH,
        )

    for shift in range(1, count_t):
        attn_copy(peer_of(shift), t).start()
    attn_recv[t] = attn_send[pl.ds(pl.multiple_of(t * head_rows, head_rows), head_rows), :]
    with jax.named_scope("wait_attn"):
        for shift in range(1, count_t):
            attn_copy(t, peer_of(shift)).wait_recv()

    def proj_copy(peer, slot, i):
        part = pl.ds(pl.multiple_of(i * out_width, LANES), out_width)
        return pltpu.make_async_remote_copy(
            src_ref=proj_v.at[rows_of(peer), part],
            dst_ref=proj_recv.at[slot, :, part],
            send_sem=proj_send_sem.at[peer],
            recv_sem=proj_recv_sem.at[slot],
            device_id={"tp": peer},
            device_id_type=MESH,
        )

    def proj_whole(peer, slot):
        return pltpu.make_async_remote_copy(
            src_ref=proj_v.at[rows_of(peer), :],
            dst_ref=proj_recv.at[slot],
            send_sem=proj_send_sem.at[peer],
            recv_sem=proj_recv_sem.at[slot],
            device_id={"tp": peer},
            device_id_type=MESH,
        )

    def out_step(i, carry):
        part = pl.ds(pl.multiple_of(i * out_width, LANES), out_width)
        left = jnp.concatenate(
            [
                jnp.concatenate(
                    [attn_recv[tt, h * mine : (h + 1) * mine] for tt in range(count_t)], axis=0
                )
                for h in range(heads_t)
            ],
            axis=1,
        )
        product = jnp.dot(left, out_u[:, part], preferred_element_type=f32)
        proj_v[:, part] = (product * out_scale[part].reshape(1, out_width)).astype(bf16)
        for shift in range(1, count_t):
            proj_copy(peer_of(shift), t, i).start()
        return carry

    with jax.named_scope("proj"):
        lax.fori_loop(0, out_steps, out_step, 0)

    with jax.named_scope("mid"):
        total = hidden_ref[rows_of(t), :].astype(f32) + proj_v[rows_of(t), :].astype(f32)
        for shift in range(1, count_t):
            slot = peer_of(shift)

            proj_whole(t, slot).wait_recv()
            total += proj_recv[slot].astype(f32)
        mid = total.astype(bf16)
        for tt in range(count_t):
            mid_send[tt] = mid[:, tt * share : (tt + 1) * share]
        moved = ordered(
            stack_lanes(normalize_rows(mid.astype(f32), row_of(mlp_gain)).astype(bf16)), order_ref
        )
    block = model // (count_g * count_s) // LANES
    with jax.named_scope("order_x"):
        for number in range(count_g * count_s):
            owner = number % count_s
            first = jnp.where(number // count_s == g, 0, block)
            for k in range(block):
                column = pl.multiple_of((first + k) * LANES, LANES)
                source = number * block + k
                x_send[owner, :, pl.ds(column, LANES)] = moved[source * mine : (source + 1) * mine]

    def x_rows(ss, tt):
        return pl.ds(pl.multiple_of((ss * count_t + tt) * mine, mine), mine)

    def z_copy(peer, ss):
        return pltpu.make_async_remote_copy(
            src_ref=x_send.at[peer],
            dst_ref=x_v.at[x_rows(ss, t), :],
            send_sem=z_send_sem.at[peer],
            recv_sem=x_recv_sem.at[ss, t],
            device_id={"src": peer},
            device_id_type=MESH,
        )

    def x_copy(peer, ss, tt):
        return pltpu.make_async_remote_copy(
            src_ref=x_v.at[x_rows(ss, tt), :],
            dst_ref=x_v.at[x_rows(ss, tt), :],
            send_sem=x_send_sem.at[peer],
            recv_sem=x_recv_sem.at[ss, tt],
            device_id={"tp": peer},
            device_id_type=MESH,
        )

    def own_copy(peer):
        return pltpu.make_async_remote_copy(
            src_ref=x_send.at[s],
            dst_ref=x_v.at[x_rows(s, t), :],
            send_sem=x_send_sem.at[peer],
            recv_sem=x_recv_sem.at[s, t],
            device_id={"tp": peer},
            device_id_type=MESH,
        )

    def x_whole(peer):
        return pltpu.make_async_remote_copy(
            src_ref=x_send,
            dst_ref=x_send,
            send_sem=x_send_sem.at[peer],
            recv_sem=x_recv_sem.at[s, t],
            device_id={"tp": peer},
            device_id_type=MESH,
        )

    def mid_copy(peer, slot):
        return pltpu.make_async_remote_copy(
            src_ref=mid_send.at[peer],
            dst_ref=mid_v.at[rows_of(slot), :],
            send_sem=mid_send_sem.at[peer],
            recv_sem=mid_recv_sem.at[slot],
            device_id={"tp": peer},
            device_id_type=MESH,
        )

    with jax.named_scope("spread_z"):
        def near(distance, action):
            for other in (s + distance, s - distance):

                @pl.when((other >= 0) & (other < count_s))
                def _():
                    action(other)

        for distance in range(count_s - 1, 0, -1):
            near(distance, lambda other: z_copy(other, s).start())
        for shift in range(1, count_t):
            own_copy(peer_of(shift)).start()
        x_v[x_rows(s, t), :] = x_send[s]

        def forward(ss):
            z_copy(s, ss).wait_recv()
            for turn in range(1, count_t):
                x_copy(peer_of(turn), ss, t).start()

        for distance in range(1, count_s):
            near(distance, forward)
    for shift in range(1, count_t):
        mid_copy(peer_of(shift), t).start()
    mid_v[rows_of(t), :] = mid_send[t]
    def x_wait(side):
        groups = count_s // 2
        base = jnp.where(side == 1, 0, groups)
        for k in range(groups):
            for turn in range(1, count_t):
                x_copy(t, base + k, peer_of(turn)).wait_recv()


    def finish():
        for shift in range(1, count_t):
            peer = peer_of(shift)
            qkv_copy(peer, t).wait_send()
            attn_copy(peer, t).wait_send()
            mid_copy(peer, t).wait_send()

            proj_whole(peer, t).wait_send()
            x_whole(peer).wait_send()
        for shift in range(1, count_s):
            z_copy(lax.rem(s + shift, count_s), s).wait_send()
        for copy in swaps:
            copy.wait_send()

    def mid_wait():
        for shift in range(1, count_t):
            mid_copy(t, peer_of(shift)).wait_recv()

    return swaps, loads, mid_wait, x_wait, finish


def mlp_phase(here, lags, scales, mlp_buffers, scratch, sems, attention, out_ref):
    g, t, s, count_g, count_t, count_s = here
    gate_scale, up_scale, down_scale, order_ref = scales
    lag, back_lag, far_lag = lags
    gate_v, up_v, down_v, x_v, mid_v = mlp_buffers
    (
        partial,
        sum_recv,
        act,
        total,
        part_send,
        part_recv,
        stage_send,
        stage_recv,
        last_send,
        last_recv,
    ) = scratch
    (
        sum_send_sem,
        sum_recv_sem,
        act_send_sem,
        act_recv_sem,
        part_send_sem,
        part_recv_sem,
        stage_send_sem,
        stage_recv_sem,
        last_send_sem,
        last_recv_sem,
    ) = sems
    swaps, loads, mid_wait, x_wait, finish = attention
    rows = x_v.shape[0]
    half = rows // 2
    hidden = gate_v.shape[2]
    block = down_v.shape[2]
    chunks = hidden // LANES
    group_rows = rows // count_s
    total[...] = jnp.zeros_like(total)

    last = count_s - 1
    far = (last - 1) * lag

    def toward(side):
        return s - 1 + 2 * side

    def sum_copy(side, j):
        return pltpu.make_async_remote_copy(
            src_ref=partial.at[side, j],
            dst_ref=sum_recv.at[side, j],
            send_sem=sum_send_sem.at[side],
            recv_sem=sum_recv_sem.at[side, j],
            device_id={"src": toward(side)},
            device_id_type=MESH,
        )

    def act_copy(side, j):
        return pltpu.make_async_remote_copy(
            src_ref=act.at[side, j],
            dst_ref=act.at[side, j],
            send_sem=act_send_sem.at[side],
            recv_sem=act_recv_sem.at[side, j],
            device_id={"src": toward(1 - side)},
            device_id_type=MESH,
        )

    def whole_copy(array, side, sem):
        return pltpu.make_async_remote_copy(
            src_ref=array.at[side],
            dst_ref=array.at[side],
            send_sem=sem.at[side],
            recv_sem=sum_recv_sem.at[side, 0],
            device_id={"src": toward(side)},
            device_id_type=MESH,
        )

    def depth_of(side):
        if isinstance(side, int):
            return last - s if side == 0 else s
        return jnp.where(side == 0, last - s, s)

    def pass_step(side, j):
        depth = depth_of(side)

        @pl.when(depth > 0)
        def _():
            sum_copy(side, j).wait_recv()
            partial[side, j] = (
                partial[side, j].astype(jnp.float32) + sum_recv[side, j].astype(jnp.float32)
            ).astype(jnp.bfloat16)

        sum_copy(side, j).start()

    def end_step(side, j):
        sum_copy(side, j).wait_recv()
        value = partial[side, j].astype(jnp.float32) + sum_recv[side, j].astype(jnp.float32)
        columns = pl.ds(pl.multiple_of(j * LANES, LANES), LANES)
        gate_value = value[:, :LANES] * gate_scale[columns].reshape(1, LANES)
        up_value = value[:, LANES:] * up_scale[columns].reshape(1, LANES)
        activated = (gate_value / (1.0 + jnp.exp(-gate_value)) * up_value).astype(jnp.bfloat16)
        act[side, j] = jnp.dot(
            activated, order_ref[...], preferred_element_type=jnp.float32
        ).astype(jnp.bfloat16)
        act_copy(side, j).start()

    def act_step(side, j):
        depth = last - depth_of(side)
        act_copy(side, j).wait_recv()

        @pl.when(depth < last)
        def _():
            act_copy(side, j).start()

    near = jnp.where(2 * s < count_s, 1, 0)
    is_end = (s == 0) | (s == last)

    def product_step(side, i):
        columns = pl.ds(pl.multiple_of(i * LANES, LANES), LANES)
        gate_w = [unpack_slab(gate_v[index, :, columns]) for index in range(2)]
        up_w = [unpack_slab(up_v[index, :, columns]) for index in range(2)]
        weights = jnp.concatenate(
            [jnp.concatenate(gate_w, axis=0), jnp.concatenate(up_w, axis=0)], axis=1
        )
        row = pl.ds(pl.multiple_of((1 - side) * half, half), half)
        partial[side, i] = jnp.dot(
            x_v[row, :], weights, preferred_element_type=jnp.float32
        ).astype(jnp.bfloat16)

    def step(i, carry):
        for side, wait in ((near, 0), (1 - near, far_lag)):
            k = i - wait

            @pl.when((k >= 0) & (k < chunks))
            def _():
                @pl.when(k == 0)
                def _():
                    x_wait(side)

                product_step(side, k)

            depth = depth_of(side)
            j = i - depth * lag

            @pl.when((depth < last) & (j >= 0) & (j < chunks))
            def _():
                pass_step(side, j)

        return carry

    def end_loop(j, carry):
        for side in range(2):

            @pl.when(depth_of(side) == last)
            def _():
                end_step(side, j)

        return carry

    def back_step(i, carry):
        for side in range(2):
            depth = last - depth_of(side)
            j = i - depth * back_lag

            @pl.when((depth > 0) & (j >= 0) & (j < chunks))
            def _():
                act_step(side, j)

        j = i - jnp.maximum(s, last - s) * back_lag

        @pl.when((j >= 0) & (j < chunks))
        def _():
            @pl.when(j == 0)
            def _():
                loads[2].wait()
                swaps[2].wait_recv()

            slab = LANES // 4
            words = pl.ds(pl.multiple_of(j * slab, slab), slab)
            weights = jnp.concatenate(
                [unpack_slab(down_v[index, words, :]) for index in range(2)], axis=1
            )
            for side in range(2):
                total[(1 - side) * half : (2 - side) * half] += jnp.dot(
                    act[side, j], weights, preferred_element_type=jnp.float32
                )

        return carry

    for index in range(2):
        loads[index].wait()
        swaps[index].wait_recv()
    with jax.named_scope("mlp_loop"):
        lax.fori_loop(0, chunks + far, step, 0)
    with jax.named_scope("end_loop"):
        lax.fori_loop(0, chunks, end_loop, 0)
    with jax.named_scope("back_loop"):
        lax.fori_loop(0, chunks + last * back_lag, back_step, 0)

    per_share = count_g * count_s // count_t

    def part_copy(index, ss):
        number = jnp.where(index == 0, g, count_g - 1 - g) * count_s + s
        owner = number // per_share
        slot = t * per_share + lax.rem(number, per_share)
        return owner, slot, pltpu.make_async_remote_copy(
            src_ref=part_send.at[index, ss],
            dst_ref=part_recv.at[slot],
            send_sem=part_send_sem.at[index, ss],
            recv_sem=part_recv_sem.at[slot],
            device_id={"tp": owner, "src": ss},
            device_id_type=MESH,
        )

    def drain():
        with jax.named_scope("drain"):
            finish()
            for side in range(2):
                depth = depth_of(side)

                @pl.when(depth < last)
                def _():
                    whole_copy(partial, side, sum_send_sem).wait_send()

                @pl.when(depth > 0)
                def _():
                    whole_copy(act, side, act_send_sem).wait_send()

    @pl.when(g == 0)
    def _():
        with jax.named_scope("part_send"):
            for shift in range(count_s):
                ss = send_order(s, count_s, shift)
                row = pl.ds(pl.multiple_of(ss * group_rows, group_rows), group_rows)
                for index in range(2):
                    owner, slot, copy = part_copy(index, ss)
                    piece = total[row, index * block : (index + 1) * block].astype(jnp.bfloat16)
                    mine = (owner == t) & (ss == s)

                    @pl.when(mine)
                    def _():
                        part_recv[slot] = piece

                    @pl.when(jnp.logical_not(mine))
                    def _():
                        part_send[index, ss] = piece
                        copy.start()

        drain()
        with jax.named_scope("part_wait"):
            for slot in range(count_t * per_share):
                number = t * per_share + slot % per_share
                from_me = (slot // per_share == t) & (lax.rem(number, count_s) == s)

                @pl.when(jnp.logical_not(from_me))
                def _():
                    pltpu.make_async_remote_copy(
                        src_ref=part_send.at[0, 0],
                        dst_ref=part_recv.at[slot],
                        send_sem=part_send_sem.at[0, 0],
                        recv_sem=part_recv_sem.at[slot],
                        device_id={"tp": t, "src": s},
                        device_id_type=MESH,
                    ).wait_recv()

        mid_wait()
        with jax.named_scope("part_sum"):
            for place in range(per_share):
                value = part_recv[place].astype(jnp.float32)
                for tt in range(1, count_t):
                    value += part_recv[tt * per_share + place].astype(jnp.float32)
                columns = slice(place * block, (place + 1) * block)
                scale_at = pl.ds(pl.multiple_of((t * per_share + place) * block, LANES), block)
                out_ref[:, columns] = (
                    mid_v[:, columns].astype(jnp.float32) + value * down_scale[scale_at].reshape(1, block)
                )

        for ss in range(count_s):
            for index in range(2):
                owner, slot, copy = part_copy(index, ss)

                @pl.when((owner != t) | (ss != s))
                def _():
                    copy.wait_send()

    quarter = group_rows // count_t

    def stage_copy(peer, slot):
        return pltpu.make_async_remote_copy(
            src_ref=stage_send.at[peer],
            dst_ref=stage_recv.at[slot],
            send_sem=stage_send_sem.at[peer],
            recv_sem=stage_recv_sem.at[slot],
            device_id={"tp": peer},
            device_id_type=MESH,
        )

    def last_copy(index, ss, place, slot, owner):
        return pltpu.make_async_remote_copy(
            src_ref=last_send.at[index, ss],
            dst_ref=last_recv.at[place, slot],
            send_sem=last_send_sem.at[index, ss],
            recv_sem=last_recv_sem.at[place, slot],
            device_id={"tp": owner, "src": ss},
            device_id_type=MESH,
        )

    def quarter_rows(ss, tt):
        start = ss * group_rows + tt * quarter
        return pl.ds(pl.multiple_of(start, quarter), quarter)

    def target_of(index):
        number = jnp.where(index == 0, g, count_g - 1 - g) * count_s + s
        return number // per_share, lax.rem(number, per_share)

    @pl.when(g != 0)
    def _():
        with jax.named_scope("stage_send"):
            for shift in range(1, count_t):
                peer = lax.rem(t + shift, count_t)
                for ss in range(count_s):
                    stage_send[peer, ss] = total[quarter_rows(ss, peer), :].astype(jnp.bfloat16)
                stage_copy(peer, t).start()
        drain()
        with jax.named_scope("stage_wait"):
            for shift in range(1, count_t):
                stage_copy(t, lax.rem(t + shift, count_t)).wait_recv()
        for shift in range(count_s):
            ss = send_order(s, count_s, shift)
            value = total[quarter_rows(ss, t), :]
            for turn in range(1, count_t):
                value += stage_recv[lax.rem(t + turn, count_t), ss].astype(jnp.float32)
            for index in range(2):
                owner, place = target_of(index)
                piece = value[:, index * block : (index + 1) * block].astype(jnp.bfloat16)
                mine = (owner == t) & (ss == s)

                @pl.when(mine)
                def _():
                    last_recv[place, t] = piece

                @pl.when(jnp.logical_not(mine))
                def _():
                    last_send[index, ss] = piece
                    last_copy(index, ss, place, t, owner).start()

        with jax.named_scope("part_wait"):
            for place in range(per_share):
                number = t * per_share + place
                for tt in range(count_t):

                    @pl.when((tt != t) | (lax.rem(number, count_s) != s))
                    def _():
                        last_copy(0, 0, place, tt, t).wait_recv()

        mid_wait()
        for place in range(per_share):
            columns = slice(place * block, (place + 1) * block)
            scale_at = pl.ds(pl.multiple_of((t * per_share + place) * block, LANES), block)
            scale = down_scale[scale_at].reshape(1, block)
            for tt in range(count_t):
                row = slice(tt * quarter, (tt + 1) * quarter)
                out_ref[row, columns] = (
                    mid_v[row, columns].astype(jnp.float32)
                    + last_recv[place, tt].astype(jnp.float32) * scale
                )
        for shift in range(1, count_t):
            stage_copy(lax.rem(t + shift, count_t), t).wait_send()
        for ss in range(count_s):
            for index in range(2):
                owner, place = target_of(index)

                @pl.when((owner != t) | (ss != s))
                def _():
                    last_copy(index, ss, place, t, owner).wait_send()


def send_order(s, count_s, shift):
    if count_s % 2:
        return lax.rem(s + 1 + shift, count_s)
    size = count_s // 2
    other = jnp.where(s < size, size, 0)
    base = other if shift < size else size - other
    return base + lax.rem(s + 1 + shift, size)


def layer_kernel(lags, counts, *refs):
    count_in, count_buffers, count_a, count_asem, count_b, count_bsem = counts
    take = iter(refs)

    def some(count):
        return [next(take) for _ in range(count)]

    (
        hidden_ref,
        attn_gain,
        w_qkv,
        qkv_scale,
        q_gain,
        k_gain,
        keys,
        values,
        lengths,
        w_out,
        out_scale,
        mlp_gain,
        w_gate,
        w_up,
        gate_scale,
        up_scale,
        w_down,
        down_scale,
    ) = some(count_in)
    out_ref = next(take)
    order_ref = next(take)
    order_ref[...] = lane_order(LANES)
    mlp_buffers = some(count_buffers)
    scratch_a, sems_a = some(count_a), some(count_asem)
    scratch_b, sems_b = some(count_b), some(count_bsem)
    here = tuple(lax.axis_index(name) for name in ("grp", "tp", "src")) + tuple(
        lax.axis_size(name) for name in ("grp", "tp", "src")
    )
    attention = attention_phase(
        here,
        (
            hidden_ref,
            attn_gain,
            w_qkv,
            qkv_scale,
            q_gain,
            k_gain,
            keys,
            values,
            lengths,
            w_out,
            out_scale,
            mlp_gain,
            (w_gate, w_up, w_down),
            order_ref,
        ),
        mlp_buffers,
        scratch_a,
        sems_a,
    )
    mlp_phase(
        here,
        lags,
        (gate_scale, up_scale, down_scale, order_ref),
        mlp_buffers,
        scratch_b,
        sems_b,
        attention,
        out_ref,
    )


def layer(args, lags):
    (
        hidden_in,
        attn_gain,
        w_qkv,
        qkv_scale,
        q_gain,
        k_gain,
        key_cache,
        value_cache,
        lengths,
        w_out,
        out_scale,
        mlp_gain,
        w_gate,
        w_up,
        gate_scale,
        up_scale,
        w_down,
        down_scale,
    ) = args
    count_g, count_t, count_s = (lax.axis_size(name) for name in ("grp", "tp", "src"))
    group_rows, model = hidden_in.shape
    rows = group_rows * count_s
    half = rows // 2
    mine = group_rows // count_t
    packed_rows, hidden = w_gate.shape
    packed_hidden, block = w_down.shape
    depth = 2 * block
    chunks = hidden // LANES
    share = model // count_t
    slots = count_g * count_s
    steps = 10 if w_qkv.shape[0] % 320 == 0 else w_qkv.shape[0] // 32
    out_steps = 5 if model % (5 * LANES) == 0 else model // LANES
    qkv_columns = w_qkv.shape[1]
    head_rows = QUERY_HEADS * mine
    bf16, f32, i32 = jnp.bfloat16, jnp.float32, jnp.int32
    dma = pltpu.SemaphoreType.DMA
    vmem = pl.BlockSpec(memory_space=pltpu.VMEM)
    smem = pl.BlockSpec(memory_space=pltpu.SMEM)
    hbm = pl.BlockSpec(memory_space=pl.ANY)
    buffers = [
        pltpu.VMEM((2, packed_rows, hidden), i32),
        pltpu.VMEM((2, packed_rows, hidden), i32),
        pltpu.VMEM((2, packed_hidden, block), i32),
        pltpu.VMEM((rows, depth), bf16),
        pltpu.VMEM((group_rows, share), bf16),
    ]
    scratch_a = [
        pltpu.VMEM(w_qkv.shape, i32),
        pltpu.VMEM(w_out.shape, i32),
        pltpu.VMEM((4 * w_out.shape[0], model), bf16),
        pltpu.VMEM(key_cache.shape[1:], bf16),
        pltpu.VMEM(value_cache.shape[1:], bf16),
        pltpu.VMEM((group_rows, model), bf16),
        pltpu.VMEM((group_rows, qkv_columns), f32),
        pltpu.VMEM((group_rows, qkv_columns), bf16),
        pltpu.VMEM((count_t, mine, qkv_columns), bf16),
        pltpu.VMEM((head_rows, HEAD_SIZE), f32),
        pltpu.VMEM((head_rows, HEAD_SIZE), f32),
        pltpu.VMEM((head_rows, key_cache.shape[2]), f32),
        pltpu.VMEM((head_rows, HEAD_SIZE), f32),
        pltpu.VMEM((head_rows, HEAD_SIZE), f32),
        pltpu.VMEM((head_rows, HEAD_SIZE), f32),
        pltpu.VMEM((head_rows, HEAD_SIZE), bf16),
        pltpu.VMEM((count_t, head_rows // count_t, HEAD_SIZE), bf16),
        pltpu.VMEM((group_rows, model), bf16),
        pltpu.VMEM((count_t, mine, model), bf16),
        pltpu.VMEM((count_t, mine, share), bf16),
        pltpu.VMEM((count_s, mine, depth), bf16),
    ]
    sems_a = [
        dma((steps,)),
        dma((out_steps,)),
        dma((2,)),
        dma((3,)),
        dma((3,)),
        dma((3,)),
        dma((count_t,)),
        dma((count_t,)),
        dma((count_t,)),
        dma((count_t,)),
        dma((count_t,)),
        dma((count_t,)),
        dma((count_t,)),
        dma((count_t,)),
        dma((count_s,)),
        dma((count_t,)),
        dma((count_s, count_t)),
    ]
    scratch_b = [
        pltpu.VMEM((2, chunks, half, 2 * LANES), bf16),
        pltpu.VMEM((2, chunks, half, 2 * LANES), bf16),
        pltpu.VMEM((2, chunks, half, LANES), bf16),
        pltpu.VMEM((rows, depth), f32),
        pltpu.VMEM((2, count_s, group_rows, block), bf16),
        pltpu.VMEM((slots, group_rows, block), bf16),
        pltpu.VMEM((count_t, count_s, mine, depth), bf16),
        pltpu.VMEM((count_t, count_s, mine, depth), bf16),
        pltpu.VMEM((2, count_s, mine, block), bf16),
        pltpu.VMEM((slots // count_t, count_t, mine, block), bf16),
    ]
    sems_b = [
        dma((2,)),
        dma((2, chunks)),
        dma((2,)),
        dma((2, chunks)),
        dma((2, count_s)),
        dma((slots,)),
        dma((count_t,)),
        dma((count_t,)),
        dma((2, count_s)),
        dma((slots // count_t, count_t)),
    ]
    specs = [vmem] * len(args)
    for place in (2, 6, 7, 9, 12, 13, 16):
        specs[place] = hbm
    specs[8] = smem
    counts = (
        len(specs),
        len(buffers),
        len(scratch_a),
        len(sems_a),
        len(scratch_b),
        len(sems_b),
    )
    return pl.pallas_call(
        functools.partial(layer_kernel, lags, counts),
        out_shape=pltpu.VMEM((group_rows, share), f32),
        in_specs=specs,
        out_specs=vmem,
        scratch_shapes=[pltpu.VMEM((LANES, LANES), bf16)] + buffers + scratch_a + sems_a + scratch_b + sems_b,
        compiler_params=pltpu.CompilerParams(
            collective_id=1, has_side_effects=True, vmem_limit_bytes=63 * 1024 * 1024
        ),
        name="layer",
    )(*args).astype(bf16)


def fast_layer(args):
    hidden_in, w_qkv, w_out, w_gate, w_down = (args[k] for k in (0, 2, 9, 12, 16))
    grp, tp, src = (lax.axis_size(name) for name in ("grp", "tp", "src"))
    rows, model = hidden_in.shape
    return (
        grp == 2
        and src > 1
        and tp > 1
        and (grp * src) % tp == 0
        and rows % (16 * tp) == 0
        and QUERY_HEADS % tp == 0
        and model % (LANES * tp) == 0
        and w_qkv.shape[0] % 32 == 0
        and w_qkv.shape[1] % HEAD_SIZE == 0
        and w_out.shape[0] % 32 == 0
        and w_gate.shape[0] % 32 == 0
        and w_gate.shape[1] % LANES == 0
        and w_down.shape[1] % LANES == 0
        and args[6].shape[2] == LANES
        and HEAD_SIZE == LANES
    )


def local(
    hidden_in,
    attn_gain,
    w_qkv,
    qkv_scale,
    q_gain,
    k_gain,
    key_cache,
    value_cache,
    lengths,
    w_out,
    out_scale,
    mlp_gain,
    w_gate,
    w_up,
    gate_scale,
    up_scale,
    w_down,
    down_scale,
):
    args = (
        hidden_in,
        attn_gain,
        w_qkv,
        qkv_scale,
        q_gain,
        k_gain,
        key_cache,
        value_cache,
        lengths,
        w_out,
        out_scale,
        mlp_gain,
        w_gate,
        w_up,
        gate_scale,
        up_scale,
        w_down,
        down_scale,
    )
    if fast_layer(args):
        return layer(args, (4, 8, 4))
    tp_count = lax.axis_size("tp")
    tp_index = lax.axis_index("tp")
    share_cols = D // tp_count
    residual = hidden_in.astype(jnp.float32)
    normed = normalize_rows(residual, attn_gain).astype(jnp.bfloat16)
    qkv_part = (byte_product(normed, w_qkv) * qkv_scale).astype(jnp.bfloat16)
    query_key_value_rows = lax.all_to_all(qkv_part, "tp", split_axis=0, concat_axis=1, tiled=True)
    heads_out = local_attention(
        query_key_value_rows, q_gain, k_gain, key_cache[0], value_cache[0], lengths[0]
    )
    head_rows = lax.all_to_all(heads_out, "tp", split_axis=1, concat_axis=0, tiled=True)
    partial_value = (byte_product(head_rows, w_out) * out_scale).astype(jnp.bfloat16)
    residual_share = lax.dynamic_slice_in_dim(hidden_in, tp_index * share_cols, share_cols, 1)
    mid_share = (
        residual_share.astype(jnp.float32) + summed_share(partial_value, tp_count)
    ).astype(jnp.bfloat16)
    mid_full = lax.all_gather(mid_share, "tp", axis=1, tiled=True)
    normed_mlp = normalize_rows(mid_full.astype(jnp.float32), mlp_gain).astype(jnp.bfloat16)
    mlp_columns = order_bytes(
        lax.all_to_all(normed_mlp, ("grp", "src"), split_axis=1, concat_axis=0, tiled=True)
    )
    gate_terms = jnp.dot(mlp_columns, unpack_ordered(w_gate), preferred_element_type=jnp.float32)
    up_terms = jnp.dot(mlp_columns, unpack_ordered(w_up), preferred_element_type=jnp.float32)
    both_terms = jnp.concatenate(
        [gate_terms.astype(jnp.bfloat16), up_terms.astype(jnp.bfloat16)], axis=1
    )
    both = summed_rows(summed_rows(both_terms, "grp").astype(jnp.bfloat16), "src")
    hidden = gate_scale.shape[0]
    gate_value = both[:, :hidden] * gate_scale
    up_value = both[:, hidden:] * up_scale
    activated = order_bytes((jax.nn.silu(gate_value) * up_value).astype(jnp.bfloat16))
    all_activated = gathered_rows(gathered_rows(activated, "src"), "grp")
    down_columns = jnp.dot(
        all_activated, unpack_ordered(w_down), preferred_element_type=jnp.float32
    ).astype(jnp.bfloat16)
    down_rows = lax.all_to_all(
        down_columns, ("grp", "src"), split_axis=0, concat_axis=1, tiled=True
    )
    down_share = lax.dynamic_slice_in_dim(down_scale, tp_index * share_cols, share_cols, 0)
    mlp_share = summed_share(down_rows, tp_count) * down_share
    return (mid_share.astype(jnp.float32) + mlp_share).astype(jnp.bfloat16)


def solution(mesh):
    return jax.shard_map(
        local,
        mesh=mesh,
        in_specs=(
            P(("grp", "src"), None),
            P(),
            P(None, "tp"),
            P("tp"),
            P(),
            P(),
            P(("grp", "src"), "tp", None, None),
            P(("grp", "src"), "tp", None, None),
            P(("grp", "src"), "tp"),
            P("tp", None),
            P(),
            P(),
            P(("grp", "src"), "tp"),
            P(("grp", "src"), "tp"),
            P("tp"),
            P("tp"),
            P("tp", ("grp", "src")),
            P(),
        ),
        out_specs=P(("grp", "src"), "tp"),
        check_vma=False,
    )
```

```python
import functools
import math

import jax
import jax.numpy as jnp
from jax import lax
from jax.experimental import pallas as pl
from jax.experimental.pallas import tpu as pltpu
from jax.sharding import PartitionSpec as P

D = 5120
QUERY_HEADS = 32
KEY_VALUE_HEADS = 4
HEAD_SIZE = 128
QUERY_COLUMNS = 4096
KEY_COLUMNS = 512


norm_epsilon = 1e-06
rope_base = 1000000.0


def unpack_bytes(packed, byte_index):
    return jnp.right_shift(jnp.left_shift(packed, 24 - 8 * byte_index), 24)


def byte_order(block):
    source = lax.broadcasted_iota(jnp.int32, (block, block), 0)
    target = lax.broadcasted_iota(jnp.int32, (block, block), 1)
    return (target == (source % 4) * (block // 4) + source // 4).astype(jnp.bfloat16)


def split_kernel(block, x_ref, order_ref, out_ref):
    lanes = block // 4
    for c in range(x_ref.shape[1] // block):
        moved = jnp.dot(
            x_ref[:, c * block : (c + 1) * block],
            order_ref[...],
            preferred_element_type=jnp.float32,
        ).astype(jnp.bfloat16)
        for j in range(4):
            out_ref[j, :, c * lanes : (c + 1) * lanes] = moved[:, j * lanes : (j + 1) * lanes]


def split_bytes(activations):
    rows, width = activations.shape
    if width % 512:
        return [activations[:, byte_index::4] for byte_index in range(4)]
    split = pl.pallas_call(
        functools.partial(split_kernel, 512),
        out_shape=jax.ShapeDtypeStruct((4, rows, width // 4), jnp.bfloat16),
        cost_estimate=pl.CostEstimate(
            flops=2 * rows * width * 512, bytes_accessed=4 * rows * width, transcendentals=0
        ),
        name="split_bytes",
    )(activations, byte_order(512))
    return [split[byte_index] for byte_index in range(4)]


def byte_product(activations, packed):
    pieces = split_bytes(activations)
    products = [
        jnp.dot(
            pieces[byte_index],
            unpack_bytes(packed, byte_index).astype(jnp.bfloat16),
            preferred_element_type=jnp.float32,
        )
        for byte_index in range(4)
    ]
    return products[0] + products[1] + products[2] + products[3]


def block_of(width):
    return math.gcd(640, width)


def order_kernel(block, x_ref, order_ref, out_ref):
    for c in range(x_ref.shape[1] // block):
        out_ref[:, c * block : (c + 1) * block] = jnp.dot(
            x_ref[:, c * block : (c + 1) * block],
            order_ref[...],
            preferred_element_type=jnp.float32,
        ).astype(jnp.bfloat16)


def order_bytes(activations):
    rows, width = activations.shape
    block = block_of(width)
    if block == width:
        return jnp.dot(activations, byte_order(block), preferred_element_type=jnp.float32).astype(
            jnp.bfloat16
        )
    return pl.pallas_call(
        functools.partial(order_kernel, block),
        out_shape=jax.ShapeDtypeStruct((rows, width), jnp.bfloat16),
        cost_estimate=pl.CostEstimate(
            flops=2 * rows * width * block, bytes_accessed=4 * rows * width, transcendentals=0
        ),
        name="order_bytes",
    )(activations, byte_order(block))


def unpack_ordered(packed):
    rows, columns = packed.shape
    block = block_of(4 * rows) // 4
    blocks = packed.reshape(rows // block, block, columns)
    parts = [unpack_bytes(blocks, j).astype(jnp.bfloat16) for j in range(4)]
    return jnp.stack(parts, axis=1).reshape(4 * rows, columns)


def normalize_rows(values, gain_row):
    return (
        values
        * lax.rsqrt(jnp.mean(values * values, axis=-1, keepdims=True) + norm_epsilon)
        * gain_row
    )


def rotary_embed(values, positions):
    half_dim = values.shape[-1] // 2
    freq_index = jnp.arange(half_dim, dtype=jnp.float32)
    inverse = jnp.exp(freq_index * (-math.log(rope_base) / half_dim))
    angles = positions.astype(jnp.float32)[:, None] * inverse[None, :]
    cosine = jnp.cos(angles)[:, None, :]
    sine_part = jnp.sin(angles)[:, None, :]
    lower_half = values[..., :half_dim]
    upper_half = values[..., half_dim:]
    return jnp.concatenate(
        [
            lower_half * cosine - upper_half * sine_part,
            upper_half * cosine + lower_half * sine_part,
        ],
        axis=-1,
    )


def local_attention(query_key_value_rows, q_gain, k_gain, stored_keys, stored_values, seq_lengths):
    count_of_rows = query_key_value_rows.shape[0]
    cache_length = stored_keys.shape[1]
    query_matrix = (
        query_key_value_rows[:, :QUERY_COLUMNS]
        .astype(jnp.float32)
        .reshape(count_of_rows, QUERY_HEADS, HEAD_SIZE)
    )
    incoming_keys = (
        query_key_value_rows[:, QUERY_COLUMNS : QUERY_COLUMNS + KEY_COLUMNS]
        .astype(jnp.float32)
        .reshape(count_of_rows, KEY_VALUE_HEADS, HEAD_SIZE)
    )
    incoming_values = query_key_value_rows[:, QUERY_COLUMNS + KEY_COLUMNS :].reshape(
        count_of_rows, KEY_VALUE_HEADS, HEAD_SIZE
    )
    query_matrix = rotary_embed(normalize_rows(query_matrix, q_gain), seq_lengths).astype(
        jnp.bfloat16
    )
    incoming_keys = rotary_embed(normalize_rows(incoming_keys, k_gain), seq_lengths).astype(
        jnp.bfloat16
    )
    query_groups = query_matrix.reshape(
        count_of_rows, KEY_VALUE_HEADS, QUERY_HEADS // KEY_VALUE_HEADS, HEAD_SIZE
    )
    key_slices = stored_keys.reshape(count_of_rows, cache_length, KEY_VALUE_HEADS, HEAD_SIZE)
    value_slices = stored_values.reshape(count_of_rows, cache_length, KEY_VALUE_HEADS, HEAD_SIZE)
    logit_scale = 1.0 / math.sqrt(HEAD_SIZE)
    scores = (
        jnp.einsum("bkgd,bpkd->bkgp", query_groups, key_slices, preferred_element_type=jnp.float32)
        * logit_scale
    )
    live_mask = jnp.arange(cache_length, dtype=jnp.int32)[None, :] < seq_lengths[:, None]
    scores = jnp.where(live_mask[:, None, None, :], scores, -jnp.inf)
    self_score = (
        jnp.einsum("nufi,nui->nuf", query_groups, incoming_keys, preferred_element_type=jnp.float32)
        * logit_scale
    )
    row_max = jnp.maximum(jnp.max(scores, axis=-1), self_score)
    soft_weights = jnp.exp(scores - row_max[..., None])
    own_weight = jnp.exp(self_score - row_max)
    denominator = jnp.sum(soft_weights, axis=-1) + own_weight
    own_low = lax.optimization_barrier(own_weight.astype(jnp.bfloat16)).astype(jnp.float32)
    numerator = jnp.einsum(
        "bkgp,bpkd->bkgd",
        soft_weights.astype(jnp.bfloat16),
        value_slices,
        preferred_element_type=jnp.float32,
    )
    numerator = numerator + own_low[..., None] * incoming_values.astype(jnp.float32)[:, :, None, :]
    return (
        (numerator / denominator[..., None])
        .reshape(count_of_rows, QUERY_COLUMNS)
        .astype(jnp.bfloat16)
    )


def summed_share(terms, tp_count):
    rows, columns = terms.shape
    pieces = lax.all_to_all(terms, "tp", split_axis=1, concat_axis=0, tiled=True)
    return jnp.sum(
        pieces.reshape(tp_count, rows, columns // tp_count).astype(jnp.float32), axis=0
    )


def gathered_rows(rows, axis):
    count = lax.axis_size(axis)
    copies = jnp.broadcast_to(rows[None], (count, *rows.shape))
    pieces = lax.all_to_all(copies, axis, split_axis=0, concat_axis=0)
    return pieces.reshape(count * rows.shape[0], rows.shape[1])


def summed_rows(terms, axis):
    count = lax.axis_size(axis)
    rows, columns = terms.shape
    pieces = lax.all_to_all(
        terms.reshape(count, rows // count, columns), axis, split_axis=0, concat_axis=0
    )
    return jnp.sum(pieces.astype(jnp.float32), axis=0)


LANES = 128
MESH = pl.DeviceIdType.MESH


def lane_order(block):
    source = lax.broadcasted_iota(jnp.int32, (block, block), 0)
    target = lax.broadcasted_iota(jnp.int32, (block, block), 1)
    return (target == (source % 4) * (block // 4) + source // 4).astype(jnp.bfloat16)


def unpack_slab(packed):
    rows, columns = packed.shape
    slab = LANES // 4
    parts = []
    for k in range(rows // slab):
        words = packed[k * slab : (k + 1) * slab]
        for j in range(4):
            parts.append(jnp.right_shift(words, 8 * j).astype(jnp.int8).astype(jnp.bfloat16))
    return jnp.concatenate(parts, axis=0)


def stack_lanes(values):
    blocks = values.shape[1] // LANES
    return jnp.concatenate([values[:, k * LANES : (k + 1) * LANES] for k in range(blocks)], axis=0)


def ordered(stacked, order_ref):
    return jnp.dot(stacked, order_ref[...], preferred_element_type=jnp.float32).astype(jnp.bfloat16)


def row_of(ref):
    return ref[...].reshape(1, ref.shape[0])


def attention_phase(here, inputs, mlp_buffers, scratch, sems):
    g, t, s, count_g, count_t, count_s = here
    (
        hidden_ref,
        attn_gain,
        w_qkv,
        qkv_scale,
        q_gain,
        k_gain,
        keys,
        values,
        lengths,
        w_out,
        out_scale,
        mlp_gain,
        weights,
        order_ref,
    ) = inputs
    gate_v, up_v, down_v, x_v, mid_v = mlp_buffers
    (
        qkv_w,
        out_w,
        out_u,
        keys_v,
        values_v,
        normed_v,
        qkv_acc,
        qkv_send,
        qkv_recv,
        q_v,
        own_v,
        score_v,
        own_e_v,
        denom_v,
        attn_v,
        attn_send,
        attn_recv,
        proj_v,
        proj_recv,
        mid_send,
        x_send,
    ) = scratch
    (
        qkv_w_sem,
        out_w_sem,
        cache_sem,
        swap_send_sem,
        swap_recv_sem,
        load_sem,
        qkv_send_sem,
        qkv_recv_sem,
        attn_send_sem,
        attn_recv_sem,
        proj_send_sem,
        proj_recv_sem,
        mid_send_sem,
        mid_recv_sem,
        z_send_sem,
        x_send_sem,
        x_recv_sem,
    ) = sems
    f32, bf16 = jnp.float32, jnp.bfloat16
    rows, model = hidden_ref.shape
    mine = rows // count_t
    qkv_columns = w_qkv.shape[1]
    steps = qkv_w_sem.shape[0]
    step_rows = w_qkv.shape[0] // steps
    out_steps = out_w_sem.shape[0]
    out_width = model // out_steps
    share = model // count_t
    positions = keys_v.shape[1]
    heads = QUERY_HEADS
    per_kv = QUERY_HEADS // KEY_VALUE_HEADS
    heads_t = heads // count_t

    def qkv_load(i):
        part = pl.ds(pl.multiple_of(i * step_rows, step_rows), step_rows)
        return pltpu.make_async_copy(w_qkv.at[part, :], qkv_w.at[part, :], qkv_w_sem.at[i])

    def out_load(i):
        part = pl.ds(pl.multiple_of(i * out_width, LANES), out_width)
        return pltpu.make_async_copy(w_out.at[:, part], out_w.at[:, part], out_w_sem.at[i])

    for i in range(steps):
        qkv_load(i).start()
    cache = [
        pltpu.make_async_copy(keys.at[0], keys_v, cache_sem.at[0]),
        pltpu.make_async_copy(values.at[0], values_v, cache_sem.at[1]),
    ]
    for copy in cache:
        copy.start()
    for i in range(out_steps):
        out_load(i).start()

    barrier = pltpu.get_barrier_semaphore()
    for tt in range(count_t):
        for ss in range(count_s):

            @pl.when((tt != t) | (ss != s))
            def _():
                pl.semaphore_signal(
                    barrier, inc=1, device_id={"tp": tt, "src": ss}, device_id_type=MESH
                )

    pl.semaphore_signal(barrier, inc=1, device_id={"grp": 1 - g}, device_id_type=MESH)

    with jax.named_scope("norm"):
        normed = normalize_rows(hidden_ref[...].astype(f32), row_of(attn_gain)).astype(bf16)
        moved = ordered(stack_lanes(normed), order_ref)
        for k in range(model // LANES):
            normed_v[:, k * LANES : (k + 1) * LANES] = moved[k * rows : (k + 1) * rows]

    swaps = [
        pltpu.make_async_remote_copy(
            src_ref=source,
            dst_ref=target.at[1],
            send_sem=swap_send_sem.at[index],
            recv_sem=swap_recv_sem.at[index],
            device_id={"grp": 1 - g},
            device_id_type=MESH,
        )
        for index, (source, target) in enumerate(zip(weights, (gate_v, up_v, down_v)))
    ]
    loads = [
        pltpu.make_async_copy(source, target.at[0], load_sem.at[index])
        for index, (source, target) in enumerate(zip(weights, (gate_v, up_v, down_v)))
    ]

    qkv_acc[...] = jnp.zeros_like(qkv_acc)

    def qkv_step(i, carry):
        qkv_load(i).wait()
        part = pl.ds(pl.multiple_of(i * step_rows, step_rows), step_rows)
        depth = pl.ds(pl.multiple_of(i * 4 * step_rows, LANES), 4 * step_rows)
        qkv_acc[...] += jnp.dot(
            normed_v[:, depth], unpack_slab(qkv_w[part, :]), preferred_element_type=f32
        )
        return carry

    with jax.named_scope("qkv"):
        lax.fori_loop(0, steps, qkv_step, 0)
        pl.semaphore_wait(barrier, count_t * count_s)
        for copy in swaps + loads:
            copy.start()
        qkv_send[...] = (qkv_acc[...] * row_of(qkv_scale)).astype(bf16)

    def peer_of(shift):
        return lax.rem(t + shift, count_t)

    def rows_of(index):
        return pl.ds(pl.multiple_of(index * mine, mine), mine)

    def qkv_copy(peer, slot):
        return pltpu.make_async_remote_copy(
            src_ref=qkv_send.at[rows_of(peer), :],
            dst_ref=qkv_recv.at[slot],
            send_sem=qkv_send_sem.at[peer],
            recv_sem=qkv_recv_sem.at[slot],
            device_id={"tp": peer},
            device_id_type=MESH,
        )

    for shift in range(1, count_t):
        qkv_copy(peer_of(shift), t).start()
    qkv_recv[t] = qkv_send[rows_of(t), :]

    def unpack_out(i, carry):
        out_load(i).wait()
        part = pl.ds(pl.multiple_of(i * out_width, LANES), out_width)
        out_u[:, part] = unpack_slab(out_w[:, part])
        return carry

    with jax.named_scope("unpack_out"):
        lax.fori_loop(0, out_steps, unpack_out, 0)

    row_index = lax.broadcasted_iota(jnp.int32, (mine, HEAD_SIZE), 0)
    lane = lax.broadcasted_iota(jnp.int32, (mine, HEAD_SIZE), 1)
    place = jnp.zeros((mine, HEAD_SIZE), f32)
    for b in range(mine):
        place = jnp.where(row_index == b, lengths[0, b].astype(f32), place)
    half_dim = HEAD_SIZE // 2
    low = lane < half_dim
    frequency = jnp.where(low, lane, lane - half_dim).astype(f32)
    angle = place * jnp.exp(frequency * (-math.log(rope_base) / half_dim))
    cosine = jnp.cos(angle)
    sine = jnp.sin(angle)
    sine = jnp.where(low, -sine, sine)

    with jax.named_scope("wait_qkv"):
        for shift in range(1, count_t):
            qkv_copy(t, peer_of(shift)).wait_recv()

    per_share = qkv_columns // HEAD_SIZE

    def head_of(h):
        column = (h % per_share) * HEAD_SIZE
        return qkv_recv[h // per_share, :, column : column + HEAD_SIZE]

    def turned(first, count, gain):
        stacked = jnp.concatenate([head_of(first + k) for k in range(count)], axis=0)
        value = normalize_rows(stacked.astype(f32), gain)
        other = pltpu.roll(value, half_dim, 1)
        wide = [jnp.concatenate([table] * count, axis=0) for table in (cosine, sine)]
        return (value * wide[0] + other * wide[1]).astype(bf16).astype(f32)

    logit_scale = 1.0 / math.sqrt(HEAD_SIZE)
    q_row, k_row = row_of(q_gain), row_of(k_gain)
    with jax.named_scope("rope"):
        new_keys = turned(heads, KEY_VALUE_HEADS, k_row)
        for kv in range(KEY_VALUE_HEADS):
            part = slice(kv * per_kv * mine, (kv + 1) * per_kv * mine)
            query = turned(kv * per_kv, per_kv, q_row)
            q_v[part] = query
            new_key = jnp.concatenate([new_keys[kv * mine : (kv + 1) * mine]] * per_kv, axis=0)
            own = jnp.sum(query * new_key, axis=1, keepdims=True) * logit_scale
            own_v[part] = jnp.broadcast_to(own, query.shape)
    for copy in cache:
            copy.wait()

    zeros = jnp.zeros((per_kv, HEAD_SIZE), f32)
    with jax.named_scope("scores"):
        for b in range(mine):
            query = q_v[pl.ds(b, heads, stride=mine), :]
            spread = jnp.concatenate(
                [
                    jnp.concatenate(
                        [
                            query[kv * per_kv : (kv + 1) * per_kv] if kv == place_of else zeros
                            for place_of in range(KEY_VALUE_HEADS)
                        ],
                        axis=1,
                    )
                    for kv in range(KEY_VALUE_HEADS)
                ],
                axis=0,
            ).astype(bf16)
            score_v[b * heads : (b + 1) * heads] = lax.dot_general(
                spread, keys_v[b], (((1,), (1,)), ((), ())), preferred_element_type=f32
            )
    position = lax.broadcasted_iota(jnp.int32, (heads, positions), 1)
    with jax.named_scope("softmax"):
        for b in range(mine):
            strided = pl.ds(b, heads, stride=mine)
            scores = score_v[b * heads : (b + 1) * heads] * logit_scale
            scores = jnp.where(position < lengths[0, b], scores, -jnp.inf)
            own = own_v[strided, :]
            top = jnp.maximum(jnp.max(scores, axis=1, keepdims=True), own)
            weight = jnp.exp(scores - top)
            own_e = jnp.exp(own - top)
            denominator = jnp.sum(weight, axis=1, keepdims=True) + own_e
            score_v[b * heads : (b + 1) * heads] = weight
            own_e_v[strided, :] = own_e
            denom_v[strided, :] = denominator
    with jax.named_scope("mix"):
        for b in range(mine):
            mixed = jnp.dot(
                score_v[b * heads : (b + 1) * heads].astype(bf16),
                values_v[b],
                preferred_element_type=f32,
            )
            attn_v[pl.ds(b, heads, stride=mine), :] = jnp.concatenate(
                [
                    mixed[kv * per_kv : (kv + 1) * per_kv, kv * HEAD_SIZE : (kv + 1) * HEAD_SIZE]
                    for kv in range(KEY_VALUE_HEADS)
                ],
                axis=0,
            )
    with jax.named_scope("finish_attn"):
        finished = []
        for h in range(heads):
            part = slice(h * mine, (h + 1) * mine)
            new_value = head_of(heads + KEY_VALUE_HEADS + h // per_kv).astype(f32)
            own_low = own_e_v[part].astype(bf16).astype(f32)
            finished.append(((attn_v[part] + own_low * new_value) / denom_v[part]).astype(bf16))
        attn_send[...] = ordered(jnp.concatenate(finished, axis=0), order_ref)

    head_rows = heads_t * mine

    def attn_copy(peer, slot):
        return pltpu.make_async_remote_copy(
            src_ref=attn_send.at[pl.ds(pl.multiple_of(peer * head_rows, head_rows), head_rows), :],
            dst_ref=attn_recv.at[slot],
            send_sem=attn_send_sem.at[peer],
            recv_sem=attn_recv_sem.at[slot],
            device_id={"tp": peer},
            device_id_type=MESH,
        )

    for shift in range(1, count_t):
        attn_copy(peer_of(shift), t).start()
    attn_recv[t] = attn_send[pl.ds(pl.multiple_of(t * head_rows, head_rows), head_rows), :]
    with jax.named_scope("wait_attn"):
        for shift in range(1, count_t):
            attn_copy(t, peer_of(shift)).wait_recv()

    def proj_copy(peer, slot, i):
        part = pl.ds(pl.multiple_of(i * out_width, LANES), out_width)
        return pltpu.make_async_remote_copy(
            src_ref=proj_v.at[rows_of(peer), part],
            dst_ref=proj_recv.at[slot, :, part],
            send_sem=proj_send_sem.at[peer],
            recv_sem=proj_recv_sem.at[slot],
            device_id={"tp": peer},
            device_id_type=MESH,
        )

    def proj_whole(peer, slot):
        return pltpu.make_async_remote_copy(
            src_ref=proj_v.at[rows_of(peer), :],
            dst_ref=proj_recv.at[slot],
            send_sem=proj_send_sem.at[peer],
            recv_sem=proj_recv_sem.at[slot],
            device_id={"tp": peer},
            device_id_type=MESH,
        )

    def out_step(i, carry):
        part = pl.ds(pl.multiple_of(i * out_width, LANES), out_width)
        left = jnp.concatenate(
            [
                jnp.concatenate(
                    [attn_recv[tt, h * mine : (h + 1) * mine] for tt in range(count_t)], axis=0
                )
                for h in range(heads_t)
            ],
            axis=1,
        )
        product = jnp.dot(left, out_u[:, part], preferred_element_type=f32)
        proj_v[:, part] = (product * out_scale[part].reshape(1, out_width)).astype(bf16)
        for shift in range(1, count_t):
            proj_copy(peer_of(shift), t, i).start()
        return carry

    with jax.named_scope("proj"):
        lax.fori_loop(0, out_steps, out_step, 0)

    with jax.named_scope("mid"):
        total = hidden_ref[rows_of(t), :].astype(f32) + proj_v[rows_of(t), :].astype(f32)
        for shift in range(1, count_t):
            slot = peer_of(shift)

            proj_whole(t, slot).wait_recv()
            total += proj_recv[slot].astype(f32)
        mid = total.astype(bf16)
        for tt in range(count_t):
            mid_send[tt] = mid[:, tt * share : (tt + 1) * share]
        moved = ordered(
            stack_lanes(normalize_rows(mid.astype(f32), row_of(mlp_gain)).astype(bf16)), order_ref
        )
    block = model // (count_g * count_s) // LANES
    with jax.named_scope("order_x"):
        for number in range(count_g * count_s):
            owner = number % count_s
            first = jnp.where(number // count_s == g, 0, block)
            for k in range(block):
                column = pl.multiple_of((first + k) * LANES, LANES)
                source = number * block + k
                x_send[owner, :, pl.ds(column, LANES)] = moved[source * mine : (source + 1) * mine]

    def x_rows(ss, tt):
        return pl.ds(pl.multiple_of((ss * count_t + tt) * mine, mine), mine)

    def z_copy(peer, ss):
        return pltpu.make_async_remote_copy(
            src_ref=x_send.at[peer],
            dst_ref=x_v.at[x_rows(ss, t), :],
            send_sem=z_send_sem.at[peer],
            recv_sem=x_recv_sem.at[ss, t],
            device_id={"src": peer},
            device_id_type=MESH,
        )

    def x_copy(peer, ss, tt):
        return pltpu.make_async_remote_copy(
            src_ref=x_v.at[x_rows(ss, tt), :],
            dst_ref=x_v.at[x_rows(ss, tt), :],
            send_sem=x_send_sem.at[peer],
            recv_sem=x_recv_sem.at[ss, tt],
            device_id={"tp": peer},
            device_id_type=MESH,
        )

    def own_copy(peer):
        return pltpu.make_async_remote_copy(
            src_ref=x_send.at[s],
            dst_ref=x_v.at[x_rows(s, t), :],
            send_sem=x_send_sem.at[peer],
            recv_sem=x_recv_sem.at[s, t],
            device_id={"tp": peer},
            device_id_type=MESH,
        )

    def x_whole(peer):
        return pltpu.make_async_remote_copy(
            src_ref=x_send,
            dst_ref=x_send,
            send_sem=x_send_sem.at[peer],
            recv_sem=x_recv_sem.at[s, t],
            device_id={"tp": peer},
            device_id_type=MESH,
        )

    def mid_copy(peer, slot):
        return pltpu.make_async_remote_copy(
            src_ref=mid_send.at[peer],
            dst_ref=mid_v.at[rows_of(slot), :],
            send_sem=mid_send_sem.at[peer],
            recv_sem=mid_recv_sem.at[slot],
            device_id={"tp": peer},
            device_id_type=MESH,
        )

    with jax.named_scope("spread_z"):
        def near(distance, action):
            for other in (s + distance, s - distance):

                @pl.when((other >= 0) & (other < count_s))
                def _():
                    action(other)

        for distance in range(count_s - 1, 0, -1):
            near(distance, lambda other: z_copy(other, s).start())
        for shift in range(1, count_t):
            own_copy(peer_of(shift)).start()
        x_v[x_rows(s, t), :] = x_send[s]

        def forward(ss):
            z_copy(s, ss).wait_recv()
            for turn in range(1, count_t):
                x_copy(peer_of(turn), ss, t).start()

        for distance in range(1, count_s):
            near(distance, forward)
    for shift in range(1, count_t):
        mid_copy(peer_of(shift), t).start()
    mid_v[rows_of(t), :] = mid_send[t]
    def x_wait(side):
        groups = count_s // 2
        base = jnp.where(side == 1, 0, groups)
        for k in range(groups):
            for turn in range(1, count_t):
                x_copy(t, base + k, peer_of(turn)).wait_recv()


    def finish():
        for shift in range(1, count_t):
            peer = peer_of(shift)
            qkv_copy(peer, t).wait_send()
            attn_copy(peer, t).wait_send()
            mid_copy(peer, t).wait_send()

            proj_whole(peer, t).wait_send()
            x_whole(peer).wait_send()
        for shift in range(1, count_s):
            z_copy(lax.rem(s + shift, count_s), s).wait_send()
        for copy in swaps:
            copy.wait_send()

    def mid_wait():
        for shift in range(1, count_t):
            mid_copy(t, peer_of(shift)).wait_recv()

    return swaps, loads, mid_wait, x_wait, finish


def mlp_phase(here, lags, scales, mlp_buffers, scratch, sems, attention, out_ref):
    g, t, s, count_g, count_t, count_s = here
    gate_scale, up_scale, down_scale, order_ref = scales
    lag, back_lag, far_lag, second_lag = lags
    gate_v, up_v, down_v, x_v, mid_v = mlp_buffers
    (
        partial,
        sum_recv,
        act,
        total,
        part_send,
        part_recv,
        stage_send,
        stage_recv,
        last_send,
        last_recv,
    ) = scratch
    (
        sum_send_sem,
        sum_recv_sem,
        act_send_sem,
        act_recv_sem,
        part_send_sem,
        part_recv_sem,
        stage_send_sem,
        stage_recv_sem,
        last_send_sem,
        last_recv_sem,
    ) = sems
    swaps, loads, mid_wait, x_wait, finish = attention
    rows = x_v.shape[0]
    half = rows // 2
    hidden = gate_v.shape[2]
    block = down_v.shape[2]
    chunks = hidden // LANES
    group_rows = rows // count_s
    total[...] = jnp.zeros_like(total)

    last = count_s - 1
    far = (last - 1) * lag

    def toward(side):
        return s - 1 + 2 * side

    def sum_copy(side, j):
        return pltpu.make_async_remote_copy(
            src_ref=partial.at[side, j],
            dst_ref=sum_recv.at[side, j],
            send_sem=sum_send_sem.at[side],
            recv_sem=sum_recv_sem.at[side, j],
            device_id={"src": toward(side)},
            device_id_type=MESH,
        )

    def act_copy(side, j):
        return pltpu.make_async_remote_copy(
            src_ref=act.at[side, j],
            dst_ref=act.at[side, j],
            send_sem=act_send_sem.at[side],
            recv_sem=act_recv_sem.at[side, j],
            device_id={"src": toward(1 - side)},
            device_id_type=MESH,
        )

    def whole_copy(array, side, sem):
        return pltpu.make_async_remote_copy(
            src_ref=array.at[side],
            dst_ref=array.at[side],
            send_sem=sem.at[side],
            recv_sem=sum_recv_sem.at[side, 0],
            device_id={"src": toward(side)},
            device_id_type=MESH,
        )

    def depth_of(side):
        if isinstance(side, int):
            return last - s if side == 0 else s
        return jnp.where(side == 0, last - s, s)

    def pass_step(side, j):
        depth = depth_of(side)

        @pl.when(depth > 0)
        def _():
            sum_copy(side, j).wait_recv()
            partial[side, j] = (
                partial[side, j].astype(jnp.float32) + sum_recv[side, j].astype(jnp.float32)
            ).astype(jnp.bfloat16)

        sum_copy(side, j).start()

    def end_step(side, j):
        sum_copy(side, j).wait_recv()
        value = partial[side, j].astype(jnp.float32) + sum_recv[side, j].astype(jnp.float32)
        columns = pl.ds(pl.multiple_of(j * LANES, LANES), LANES)
        gate_value = value[:, :LANES] * gate_scale[columns].reshape(1, LANES)
        up_value = value[:, LANES:] * up_scale[columns].reshape(1, LANES)
        activated = (gate_value / (1.0 + jnp.exp(-gate_value)) * up_value).astype(jnp.bfloat16)
        act[side, j] = jnp.dot(
            activated, order_ref[...], preferred_element_type=jnp.float32
        ).astype(jnp.bfloat16)
        act_copy(side, j).start()

    def act_step(side, j):
        depth = last - depth_of(side)
        act_copy(side, j).wait_recv()

        @pl.when(depth < last)
        def _():
            act_copy(side, j).start()

    near = jnp.where(2 * s < count_s, 1, 0)
    is_end = (s == 0) | (s == last)

    def product_step(side, i):
        columns = pl.ds(pl.multiple_of(i * LANES, LANES), LANES)
        gate_w = [unpack_slab(gate_v[index, :, columns]) for index in range(2)]
        up_w = [unpack_slab(up_v[index, :, columns]) for index in range(2)]
        weights = jnp.concatenate(
            [jnp.concatenate(gate_w, axis=0), jnp.concatenate(up_w, axis=0)], axis=1
        )
        row = pl.ds(pl.multiple_of((1 - side) * half, half), half)
        partial[side, i] = jnp.dot(
            x_v[row, :], weights, preferred_element_type=jnp.float32
        ).astype(jnp.bfloat16)

    def step(i, carry):
        for side, wait in ((near, 0), (1 - near, far_lag)):
            k = i - wait

            @pl.when((k >= 0) & (k < chunks))
            def _():
                @pl.when(k == 0)
                def _():
                    x_wait(side)

                product_step(side, k)

            depth = depth_of(side)
            j = i - depth * lag

            @pl.when((depth < last) & (j >= 0) & (j < chunks))
            def _():
                pass_step(side, j)

        return carry

    def down_step(sides, j):
        slab = LANES // 4
        words = pl.ds(pl.multiple_of(j * slab, slab), slab)
        weights = jnp.concatenate(
            [unpack_slab(down_v[index, words, :]) for index in range(2)], axis=1
        )
        for side in sides:
            total[(1 - side) * half : (2 - side) * half] += jnp.dot(
                act[side, j], weights, preferred_element_type=jnp.float32
            )

    def end_loop(j, carry):
        for side in range(2):

            @pl.when(depth_of(side) == last)
            def _():
                end_step(side, j)
                down_step((side,), j)

        return carry

    near_depth = jnp.minimum(s, last - s)
    far_depth = jnp.maximum(s, last - s)
    second = jnp.where(is_end, last * back_lag + second_lag, chunks + far_depth * back_lag)

    def back_step(i, carry):
        for side in range(2):
            depth = last - depth_of(side)
            j = i - depth * back_lag

            @pl.when((depth > 0) & (j >= 0) & (j < chunks))
            def _():
                act_step(side, j)
                down_step((side,), j)

        @pl.when(jnp.logical_not(is_end) & (i == chunks + near_depth * back_lag))
        def _():
            stage_rows()

        @pl.when(i == second)
        def _():
            pass_rows()

        return carry

    per_share = count_g * count_s // count_t

    groups = count_s // 2
    quarter = group_rows // count_t
    low_half = s < groups
    near_base = jnp.where(low_half, 0, groups)
    cross_base = groups - near_base

    def target_of(index):
        number = jnp.where(index == 0, g, count_g - 1 - g) * count_s + s
        return number // per_share, lax.rem(number, per_share)

    def part_copy(index, k, ss):
        owner, place = target_of(index)
        slot = t * per_share + place
        return owner, slot, pltpu.make_async_remote_copy(
            src_ref=part_send.at[index, k],
            dst_ref=part_recv.at[slot],
            send_sem=part_send_sem.at[index, k],
            recv_sem=part_recv_sem.at[slot],
            device_id={"tp": owner, "src": ss},
            device_id_type=MESH,
        )

    def stage_copy(peer):
        return pltpu.make_async_remote_copy(
            src_ref=stage_send.at[peer],
            dst_ref=stage_recv.at[t],
            send_sem=stage_send_sem.at[peer],
            recv_sem=stage_recv_sem.at[t],
            device_id={"tp": peer},
            device_id_type=MESH,
        )

    def stage_arrival(peer):
        return pltpu.make_async_remote_copy(
            src_ref=stage_send.at[peer],
            dst_ref=stage_recv.at[peer],
            send_sem=stage_send_sem.at[peer],
            recv_sem=stage_recv_sem.at[peer],
            device_id={"tp": peer},
            device_id_type=MESH,
        )

    def last_copy(index, k, place, slot, owner):
        return pltpu.make_async_remote_copy(
            src_ref=last_send.at[index, k],
            dst_ref=last_recv.at[place, slot],
            send_sem=last_send_sem.at[index, k],
            recv_sem=last_recv_sem.at[place, slot],
            device_id={"tp": owner, "src": cross_base + k},
            device_id_type=MESH,
        )

    def quarter_rows(k, tt):
        start = (cross_base + k) * group_rows + tt * quarter
        return pl.ds(pl.multiple_of(start, quarter), quarter)

    def stage_rows():
        for shift in range(1, count_t):
            peer = lax.rem(t + shift, count_t)
            for k in range(groups):
                stage_send[peer, k] = total[quarter_rows(k, peer), :].astype(jnp.bfloat16)
            stage_copy(peer).start()

    def pass_rows():
        for shift in range(1, count_t):
            stage_arrival(lax.rem(t + shift, count_t)).wait_recv()
        for k in range(groups):
            value = total[quarter_rows(k, t), :]
            for turn in range(1, count_t):
                value += stage_recv[lax.rem(t + turn, count_t), k].astype(jnp.float32)
            for index in range(2):
                owner, place = target_of(index)
                last_send[index, k] = value[:, index * block : (index + 1) * block].astype(
                    jnp.bfloat16
                )
                last_copy(index, k, place, t, owner).start()

    def near_rows(k):
        ss = near_base + lax.rem(s - near_base + 1 + k, groups)
        return ss, pl.ds(pl.multiple_of(ss * group_rows, group_rows), group_rows)

    for index in range(2):
        loads[index].wait()
        swaps[index].wait_recv()
    with jax.named_scope("mlp_loop"):
        lax.fori_loop(0, chunks + far, step, 0)
    with jax.named_scope("end_loop"):
        loads[2].wait()
        swaps[2].wait_recv()
        lax.fori_loop(0, chunks, end_loop, 0)

        @pl.when(is_end)
        def _():
            stage_rows()

    with jax.named_scope("back_loop"):
        lax.fori_loop(0, chunks + last * back_lag, back_step, 0)

    def drain():
        with jax.named_scope("drain"):
            finish()
            for side in range(2):
                depth = depth_of(side)

                @pl.when(depth < last)
                def _():
                    whole_copy(partial, side, sum_send_sem).wait_send()

                @pl.when(depth > 0)
                def _():
                    whole_copy(act, side, act_send_sem).wait_send()

    with jax.named_scope("part_send"):
        for k in range(groups):
            ss, row = near_rows(k)
            for index in range(2):
                owner, slot, copy = part_copy(index, k, ss)
                piece = total[row, index * block : (index + 1) * block].astype(jnp.bfloat16)
                mine = (owner == t) & (ss == s)

                @pl.when(mine)
                def _():
                    part_recv[slot] = piece

                @pl.when(jnp.logical_not(mine))
                def _():
                    part_send[index, k] = piece
                    copy.start()

    drain()
    mid_wait()
    with jax.named_scope("part_wait"):
        for place in range(per_share):
            origin = lax.rem(t * per_share + place, count_s)
            crosses = (origin < groups) != low_half
            columns = slice(place * block, (place + 1) * block)
            scale_at = pl.ds(pl.multiple_of((t * per_share + place) * block, LANES), block)

            @pl.when(jnp.logical_not(crosses))
            def _():
                for tt in range(count_t):

                    @pl.when((tt != t) | (origin != s))
                    def _():
                        pltpu.make_async_remote_copy(
                            src_ref=part_send.at[0, 0],
                            dst_ref=part_recv.at[tt * per_share + place],
                            send_sem=part_send_sem.at[0, 0],
                            recv_sem=part_recv_sem.at[tt * per_share + place],
                            device_id={"tp": tt},
                            device_id_type=MESH,
                        ).wait_recv()

                value = part_recv[place].astype(jnp.float32)
                for tt in range(1, count_t):
                    value += part_recv[tt * per_share + place].astype(jnp.float32)
                out_ref[:, columns] = mid_v[:, columns].astype(jnp.float32) + value * down_scale[
                    scale_at
                ].reshape(1, block)

            @pl.when(crosses)
            def _():
                for tt in range(count_t):
                    last_copy(0, 0, place, tt, t).wait_recv()
                    row = slice(tt * quarter, (tt + 1) * quarter)
                    out_ref[row, columns] = mid_v[row, columns].astype(jnp.float32) + last_recv[
                        place, tt
                    ].astype(jnp.float32) * down_scale[scale_at].reshape(1, block)

    for shift in range(1, count_t):
        stage_copy(lax.rem(t + shift, count_t)).wait_send()
    for k in range(groups):
        ss, row = near_rows(k)
        for index in range(2):
            owner, place = target_of(index)
            last_copy(index, k, place, t, owner).wait_send()

            @pl.when((owner != t) | (ss != s))
            def _():
                part_copy(index, k, ss)[2].wait_send()


def layer_kernel(lags, counts, *refs):
    count_in, count_buffers, count_a, count_asem, count_b, count_bsem = counts
    take = iter(refs)

    def some(count):
        return [next(take) for _ in range(count)]

    (
        hidden_ref,
        attn_gain,
        w_qkv,
        qkv_scale,
        q_gain,
        k_gain,
        keys,
        values,
        lengths,
        w_out,
        out_scale,
        mlp_gain,
        w_gate,
        w_up,
        gate_scale,
        up_scale,
        w_down,
        down_scale,
    ) = some(count_in)
    out_ref = next(take)
    order_ref = next(take)
    order_ref[...] = lane_order(LANES)
    mlp_buffers = some(count_buffers)
    scratch_a, sems_a = some(count_a), some(count_asem)
    scratch_b, sems_b = some(count_b), some(count_bsem)
    here = tuple(lax.axis_index(name) for name in ("grp", "tp", "src")) + tuple(
        lax.axis_size(name) for name in ("grp", "tp", "src")
    )
    attention = attention_phase(
        here,
        (
            hidden_ref,
            attn_gain,
            w_qkv,
            qkv_scale,
            q_gain,
            k_gain,
            keys,
            values,
            lengths,
            w_out,
            out_scale,
            mlp_gain,
            (w_gate, w_up, w_down),
            order_ref,
        ),
        mlp_buffers,
        scratch_a,
        sems_a,
    )
    mlp_phase(
        here,
        lags,
        (gate_scale, up_scale, down_scale, order_ref),
        mlp_buffers,
        scratch_b,
        sems_b,
        attention,
        out_ref,
    )


def layer(args, lags):
    (
        hidden_in,
        attn_gain,
        w_qkv,
        qkv_scale,
        q_gain,
        k_gain,
        key_cache,
        value_cache,
        lengths,
        w_out,
        out_scale,
        mlp_gain,
        w_gate,
        w_up,
        gate_scale,
        up_scale,
        w_down,
        down_scale,
    ) = args
    count_g, count_t, count_s = (lax.axis_size(name) for name in ("grp", "tp", "src"))
    group_rows, model = hidden_in.shape
    rows = group_rows * count_s
    half = rows // 2
    mine = group_rows // count_t
    packed_rows, hidden = w_gate.shape
    packed_hidden, block = w_down.shape
    depth = 2 * block
    chunks = hidden // LANES
    share = model // count_t
    slots = count_g * count_s
    steps = 10 if w_qkv.shape[0] % 320 == 0 else w_qkv.shape[0] // 32
    out_steps = 5 if model % (5 * LANES) == 0 else model // LANES
    qkv_columns = w_qkv.shape[1]
    head_rows = QUERY_HEADS * mine
    bf16, f32, i32 = jnp.bfloat16, jnp.float32, jnp.int32
    dma = pltpu.SemaphoreType.DMA
    vmem = pl.BlockSpec(memory_space=pltpu.VMEM)
    smem = pl.BlockSpec(memory_space=pltpu.SMEM)
    hbm = pl.BlockSpec(memory_space=pl.ANY)
    buffers = [
        pltpu.VMEM((2, packed_rows, hidden), i32),
        pltpu.VMEM((2, packed_rows, hidden), i32),
        pltpu.VMEM((2, packed_hidden, block), i32),
        pltpu.VMEM((rows, depth), bf16),
        pltpu.VMEM((group_rows, share), bf16),
    ]
    scratch_a = [
        pltpu.VMEM(w_qkv.shape, i32),
        pltpu.VMEM(w_out.shape, i32),
        pltpu.VMEM((4 * w_out.shape[0], model), bf16),
        pltpu.VMEM(key_cache.shape[1:], bf16),
        pltpu.VMEM(value_cache.shape[1:], bf16),
        pltpu.VMEM((group_rows, model), bf16),
        pltpu.VMEM((group_rows, qkv_columns), f32),
        pltpu.VMEM((group_rows, qkv_columns), bf16),
        pltpu.VMEM((count_t, mine, qkv_columns), bf16),
        pltpu.VMEM((head_rows, HEAD_SIZE), f32),
        pltpu.VMEM((head_rows, HEAD_SIZE), f32),
        pltpu.VMEM((head_rows, key_cache.shape[2]), f32),
        pltpu.VMEM((head_rows, HEAD_SIZE), f32),
        pltpu.VMEM((head_rows, HEAD_SIZE), f32),
        pltpu.VMEM((head_rows, HEAD_SIZE), f32),
        pltpu.VMEM((head_rows, HEAD_SIZE), bf16),
        pltpu.VMEM((count_t, head_rows // count_t, HEAD_SIZE), bf16),
        pltpu.VMEM((group_rows, model), bf16),
        pltpu.VMEM((count_t, mine, model), bf16),
        pltpu.VMEM((count_t, mine, share), bf16),
        pltpu.VMEM((count_s, mine, depth), bf16),
    ]
    sems_a = [
        dma((steps,)),
        dma((out_steps,)),
        dma((2,)),
        dma((3,)),
        dma((3,)),
        dma((3,)),
        dma((count_t,)),
        dma((count_t,)),
        dma((count_t,)),
        dma((count_t,)),
        dma((count_t,)),
        dma((count_t,)),
        dma((count_t,)),
        dma((count_t,)),
        dma((count_s,)),
        dma((count_t,)),
        dma((count_s, count_t)),
    ]
    scratch_b = [
        pltpu.VMEM((2, chunks, half, 2 * LANES), bf16),
        pltpu.VMEM((2, chunks, half, 2 * LANES), bf16),
        pltpu.VMEM((2, chunks, half, LANES), bf16),
        pltpu.VMEM((rows, depth), f32),
        pltpu.VMEM((2, count_s // 2, group_rows, block), bf16),
        pltpu.VMEM((slots, group_rows, block), bf16),
        pltpu.VMEM((count_t, count_s // 2, mine, depth), bf16),
        pltpu.VMEM((count_t, count_s // 2, mine, depth), bf16),
        pltpu.VMEM((2, count_s // 2, mine, block), bf16),
        pltpu.VMEM((slots // count_t, count_t, mine, block), bf16),
    ]
    sems_b = [
        dma((2,)),
        dma((2, chunks)),
        dma((2,)),
        dma((2, chunks)),
        dma((2, count_s // 2)),
        dma((slots,)),
        dma((count_t,)),
        dma((count_t,)),
        dma((2, count_s // 2)),
        dma((slots // count_t, count_t)),
    ]
    specs = [vmem] * len(args)
    for place in (2, 6, 7, 9, 12, 13, 16):
        specs[place] = hbm
    specs[8] = smem
    counts = (
        len(specs),
        len(buffers),
        len(scratch_a),
        len(sems_a),
        len(scratch_b),
        len(sems_b),
    )
    return pl.pallas_call(
        functools.partial(layer_kernel, lags, counts),
        out_shape=pltpu.VMEM((group_rows, share), f32),
        in_specs=specs,
        out_specs=vmem,
        scratch_shapes=[pltpu.VMEM((LANES, LANES), bf16)] + buffers + scratch_a + sems_a + scratch_b + sems_b,
        compiler_params=pltpu.CompilerParams(
            collective_id=1, has_side_effects=True, vmem_limit_bytes=63 * 1024 * 1024
        ),
        name="layer",
    )(*args).astype(bf16)


def fast_layer(args):
    hidden_in, w_qkv, w_out, w_gate, w_down = (args[k] for k in (0, 2, 9, 12, 16))
    grp, tp, src = (lax.axis_size(name) for name in ("grp", "tp", "src"))
    rows, model = hidden_in.shape
    return (
        grp == 2
        and src % 2 == 0
        and tp > 1
        and (grp * src) % tp == 0
        and rows % (16 * tp) == 0
        and QUERY_HEADS % tp == 0
        and model % (LANES * tp) == 0
        and w_qkv.shape[0] % 32 == 0
        and w_qkv.shape[1] % HEAD_SIZE == 0
        and w_out.shape[0] % 32 == 0
        and w_gate.shape[0] % 32 == 0
        and w_gate.shape[1] % LANES == 0
        and w_down.shape[1] % LANES == 0
        and args[6].shape[2] == LANES
        and HEAD_SIZE == LANES
    )


def local(
    hidden_in,
    attn_gain,
    w_qkv,
    qkv_scale,
    q_gain,
    k_gain,
    key_cache,
    value_cache,
    lengths,
    w_out,
    out_scale,
    mlp_gain,
    w_gate,
    w_up,
    gate_scale,
    up_scale,
    w_down,
    down_scale,
):
    args = (
        hidden_in,
        attn_gain,
        w_qkv,
        qkv_scale,
        q_gain,
        k_gain,
        key_cache,
        value_cache,
        lengths,
        w_out,
        out_scale,
        mlp_gain,
        w_gate,
        w_up,
        gate_scale,
        up_scale,
        w_down,
        down_scale,
    )
    if fast_layer(args):
        return layer(args, (4, 8, 4, 14))
    tp_count = lax.axis_size("tp")
    tp_index = lax.axis_index("tp")
    share_cols = D // tp_count
    residual = hidden_in.astype(jnp.float32)
    normed = normalize_rows(residual, attn_gain).astype(jnp.bfloat16)
    qkv_part = (byte_product(normed, w_qkv) * qkv_scale).astype(jnp.bfloat16)
    query_key_value_rows = lax.all_to_all(qkv_part, "tp", split_axis=0, concat_axis=1, tiled=True)
    heads_out = local_attention(
        query_key_value_rows, q_gain, k_gain, key_cache[0], value_cache[0], lengths[0]
    )
    head_rows = lax.all_to_all(heads_out, "tp", split_axis=1, concat_axis=0, tiled=True)
    partial_value = (byte_product(head_rows, w_out) * out_scale).astype(jnp.bfloat16)
    residual_share = lax.dynamic_slice_in_dim(hidden_in, tp_index * share_cols, share_cols, 1)
    mid_share = (
        residual_share.astype(jnp.float32) + summed_share(partial_value, tp_count)
    ).astype(jnp.bfloat16)
    mid_full = lax.all_gather(mid_share, "tp", axis=1, tiled=True)
    normed_mlp = normalize_rows(mid_full.astype(jnp.float32), mlp_gain).astype(jnp.bfloat16)
    mlp_columns = order_bytes(
        lax.all_to_all(normed_mlp, ("grp", "src"), split_axis=1, concat_axis=0, tiled=True)
    )
    gate_terms = jnp.dot(mlp_columns, unpack_ordered(w_gate), preferred_element_type=jnp.float32)
    up_terms = jnp.dot(mlp_columns, unpack_ordered(w_up), preferred_element_type=jnp.float32)
    both_terms = jnp.concatenate(
        [gate_terms.astype(jnp.bfloat16), up_terms.astype(jnp.bfloat16)], axis=1
    )
    both = summed_rows(summed_rows(both_terms, "grp").astype(jnp.bfloat16), "src")
    hidden = gate_scale.shape[0]
    gate_value = both[:, :hidden] * gate_scale
    up_value = both[:, hidden:] * up_scale
    activated = order_bytes((jax.nn.silu(gate_value) * up_value).astype(jnp.bfloat16))
    all_activated = gathered_rows(gathered_rows(activated, "src"), "grp")
    down_columns = jnp.dot(
        all_activated, unpack_ordered(w_down), preferred_element_type=jnp.float32
    ).astype(jnp.bfloat16)
    down_rows = lax.all_to_all(
        down_columns, ("grp", "src"), split_axis=0, concat_axis=1, tiled=True
    )
    down_share = lax.dynamic_slice_in_dim(down_scale, tp_index * share_cols, share_cols, 0)
    mlp_share = summed_share(down_rows, tp_count) * down_share
    return (mid_share.astype(jnp.float32) + mlp_share).astype(jnp.bfloat16)


def solution(mesh):
    return jax.shard_map(
        local,
        mesh=mesh,
        in_specs=(
            P(("grp", "src"), None),
            P(),
            P(None, "tp"),
            P("tp"),
            P(),
            P(),
            P(("grp", "src"), "tp", None, None),
            P(("grp", "src"), "tp", None, None),
            P(("grp", "src"), "tp"),
            P("tp", None),
            P(),
            P(),
            P(("grp", "src"), "tp"),
            P(("grp", "src"), "tp"),
            P("tp"),
            P("tp"),
            P("tp", ("grp", "src")),
            P(),
        ),
        out_specs=P(("grp", "src"), "tp"),
        check_vma=False,
    )
```

```python
import functools
import math

import jax
import jax.numpy as jnp
from jax import lax
from jax.experimental import pallas as pl
from jax.experimental.pallas import tpu as pltpu
from jax.sharding import PartitionSpec as P

D = 5120
QUERY_HEADS = 32
KEY_VALUE_HEADS = 4
HEAD_SIZE = 128
QUERY_COLUMNS = 4096
KEY_COLUMNS = 512


norm_epsilon = 1e-06
rope_base = 1000000.0


def unpack_bytes(packed, byte_index):
    return jnp.right_shift(jnp.left_shift(packed, 24 - 8 * byte_index), 24)


def byte_order(block):
    source = lax.broadcasted_iota(jnp.int32, (block, block), 0)
    target = lax.broadcasted_iota(jnp.int32, (block, block), 1)
    return (target == (source % 4) * (block // 4) + source // 4).astype(jnp.bfloat16)


def split_kernel(block, x_ref, order_ref, out_ref):
    lanes = block // 4
    for c in range(x_ref.shape[1] // block):
        moved = jnp.dot(
            x_ref[:, c * block : (c + 1) * block],
            order_ref[...],
            preferred_element_type=jnp.float32,
        ).astype(jnp.bfloat16)
        for j in range(4):
            out_ref[j, :, c * lanes : (c + 1) * lanes] = moved[:, j * lanes : (j + 1) * lanes]


def split_bytes(activations):
    rows, width = activations.shape
    if width % 512:
        return [activations[:, byte_index::4] for byte_index in range(4)]
    split = pl.pallas_call(
        functools.partial(split_kernel, 512),
        out_shape=jax.ShapeDtypeStruct((4, rows, width // 4), jnp.bfloat16),
        cost_estimate=pl.CostEstimate(
            flops=2 * rows * width * 512, bytes_accessed=4 * rows * width, transcendentals=0
        ),
        name="split_bytes",
    )(activations, byte_order(512))
    return [split[byte_index] for byte_index in range(4)]


def byte_product(activations, packed):
    pieces = split_bytes(activations)
    products = [
        jnp.dot(
            pieces[byte_index],
            unpack_bytes(packed, byte_index).astype(jnp.bfloat16),
            preferred_element_type=jnp.float32,
        )
        for byte_index in range(4)
    ]
    return products[0] + products[1] + products[2] + products[3]


def block_of(width):
    return math.gcd(640, width)


def order_kernel(block, x_ref, order_ref, out_ref):
    for c in range(x_ref.shape[1] // block):
        out_ref[:, c * block : (c + 1) * block] = jnp.dot(
            x_ref[:, c * block : (c + 1) * block],
            order_ref[...],
            preferred_element_type=jnp.float32,
        ).astype(jnp.bfloat16)


def order_bytes(activations):
    rows, width = activations.shape
    block = block_of(width)
    if block == width:
        return jnp.dot(activations, byte_order(block), preferred_element_type=jnp.float32).astype(
            jnp.bfloat16
        )
    return pl.pallas_call(
        functools.partial(order_kernel, block),
        out_shape=jax.ShapeDtypeStruct((rows, width), jnp.bfloat16),
        cost_estimate=pl.CostEstimate(
            flops=2 * rows * width * block, bytes_accessed=4 * rows * width, transcendentals=0
        ),
        name="order_bytes",
    )(activations, byte_order(block))


def unpack_ordered(packed):
    rows, columns = packed.shape
    block = block_of(4 * rows) // 4
    blocks = packed.reshape(rows // block, block, columns)
    parts = [unpack_bytes(blocks, j).astype(jnp.bfloat16) for j in range(4)]
    return jnp.stack(parts, axis=1).reshape(4 * rows, columns)


def normalize_rows(values, gain_row):
    return (
        values
        * lax.rsqrt(jnp.mean(values * values, axis=-1, keepdims=True) + norm_epsilon)
        * gain_row
    )


def rotary_embed(values, positions):
    half_dim = values.shape[-1] // 2
    freq_index = jnp.arange(half_dim, dtype=jnp.float32)
    inverse = jnp.exp(freq_index * (-math.log(rope_base) / half_dim))
    angles = positions.astype(jnp.float32)[:, None] * inverse[None, :]
    cosine = jnp.cos(angles)[:, None, :]
    sine_part = jnp.sin(angles)[:, None, :]
    lower_half = values[..., :half_dim]
    upper_half = values[..., half_dim:]
    return jnp.concatenate(
        [
            lower_half * cosine - upper_half * sine_part,
            upper_half * cosine + lower_half * sine_part,
        ],
        axis=-1,
    )


def local_attention(query_key_value_rows, q_gain, k_gain, stored_keys, stored_values, seq_lengths):
    count_of_rows = query_key_value_rows.shape[0]
    cache_length = stored_keys.shape[1]
    query_matrix = (
        query_key_value_rows[:, :QUERY_COLUMNS]
        .astype(jnp.float32)
        .reshape(count_of_rows, QUERY_HEADS, HEAD_SIZE)
    )
    incoming_keys = (
        query_key_value_rows[:, QUERY_COLUMNS : QUERY_COLUMNS + KEY_COLUMNS]
        .astype(jnp.float32)
        .reshape(count_of_rows, KEY_VALUE_HEADS, HEAD_SIZE)
    )
    incoming_values = query_key_value_rows[:, QUERY_COLUMNS + KEY_COLUMNS :].reshape(
        count_of_rows, KEY_VALUE_HEADS, HEAD_SIZE
    )
    query_matrix = rotary_embed(normalize_rows(query_matrix, q_gain), seq_lengths).astype(
        jnp.bfloat16
    )
    incoming_keys = rotary_embed(normalize_rows(incoming_keys, k_gain), seq_lengths).astype(
        jnp.bfloat16
    )
    query_groups = query_matrix.reshape(
        count_of_rows, KEY_VALUE_HEADS, QUERY_HEADS // KEY_VALUE_HEADS, HEAD_SIZE
    )
    key_slices = stored_keys.reshape(count_of_rows, cache_length, KEY_VALUE_HEADS, HEAD_SIZE)
    value_slices = stored_values.reshape(count_of_rows, cache_length, KEY_VALUE_HEADS, HEAD_SIZE)
    logit_scale = 1.0 / math.sqrt(HEAD_SIZE)
    scores = (
        jnp.einsum("bkgd,bpkd->bkgp", query_groups, key_slices, preferred_element_type=jnp.float32)
        * logit_scale
    )
    live_mask = jnp.arange(cache_length, dtype=jnp.int32)[None, :] < seq_lengths[:, None]
    scores = jnp.where(live_mask[:, None, None, :], scores, -jnp.inf)
    self_score = (
        jnp.einsum("nufi,nui->nuf", query_groups, incoming_keys, preferred_element_type=jnp.float32)
        * logit_scale
    )
    row_max = jnp.maximum(jnp.max(scores, axis=-1), self_score)
    soft_weights = jnp.exp(scores - row_max[..., None])
    own_weight = jnp.exp(self_score - row_max)
    denominator = jnp.sum(soft_weights, axis=-1) + own_weight
    own_low = lax.optimization_barrier(own_weight.astype(jnp.bfloat16)).astype(jnp.float32)
    numerator = jnp.einsum(
        "bkgp,bpkd->bkgd",
        soft_weights.astype(jnp.bfloat16),
        value_slices,
        preferred_element_type=jnp.float32,
    )
    numerator = numerator + own_low[..., None] * incoming_values.astype(jnp.float32)[:, :, None, :]
    return (
        (numerator / denominator[..., None])
        .reshape(count_of_rows, QUERY_COLUMNS)
        .astype(jnp.bfloat16)
    )


def summed_share(terms, tp_count):
    rows, columns = terms.shape
    pieces = lax.all_to_all(terms, "tp", split_axis=1, concat_axis=0, tiled=True)
    return jnp.sum(
        pieces.reshape(tp_count, rows, columns // tp_count).astype(jnp.float32), axis=0
    )


def gathered_rows(rows, axis):
    count = lax.axis_size(axis)
    copies = jnp.broadcast_to(rows[None], (count, *rows.shape))
    pieces = lax.all_to_all(copies, axis, split_axis=0, concat_axis=0)
    return pieces.reshape(count * rows.shape[0], rows.shape[1])


def summed_rows(terms, axis):
    count = lax.axis_size(axis)
    rows, columns = terms.shape
    pieces = lax.all_to_all(
        terms.reshape(count, rows // count, columns), axis, split_axis=0, concat_axis=0
    )
    return jnp.sum(pieces.astype(jnp.float32), axis=0)


LANES = 128
MESH = pl.DeviceIdType.MESH


def lane_order(block):
    source = lax.broadcasted_iota(jnp.int32, (block, block), 0)
    target = lax.broadcasted_iota(jnp.int32, (block, block), 1)
    return (target == (source % 4) * (block // 4) + source // 4).astype(jnp.bfloat16)


def unpack_slab(packed):
    rows, columns = packed.shape
    slab = LANES // 4
    parts = []
    for k in range(rows // slab):
        words = packed[k * slab : (k + 1) * slab]
        for j in range(4):
            parts.append(jnp.right_shift(words, 8 * j).astype(jnp.int8).astype(jnp.bfloat16))
    return jnp.concatenate(parts, axis=0)


def stack_lanes(values):
    blocks = values.shape[1] // LANES
    return jnp.concatenate([values[:, k * LANES : (k + 1) * LANES] for k in range(blocks)], axis=0)


def ordered(stacked, order_ref):
    return jnp.dot(stacked, order_ref[...], preferred_element_type=jnp.float32).astype(jnp.bfloat16)


def row_of(ref):
    return ref[...].reshape(1, ref.shape[0])


def attention_phase(here, inputs, mlp_buffers, scratch, sems):
    g, t, s, count_g, count_t, count_s = here
    (
        hidden_ref,
        attn_gain,
        w_qkv,
        qkv_scale,
        q_gain,
        k_gain,
        keys,
        values,
        lengths,
        w_out,
        out_scale,
        mlp_gain,
        weights,
        order_ref,
    ) = inputs
    gate_v, up_v, down_v, x_v, mid_v = mlp_buffers
    (
        qkv_w,
        out_w,
        out_u,
        keys_v,
        values_v,
        normed_v,
        qkv_acc,
        qkv_send,
        qkv_recv,
        q_v,
        own_v,
        score_v,
        own_e_v,
        denom_v,
        attn_v,
        attn_send,
        attn_recv,
        proj_v,
        proj_recv,
        mid_send,
        x_send,
    ) = scratch
    (
        qkv_w_sem,
        out_w_sem,
        cache_sem,
        swap_send_sem,
        swap_recv_sem,
        load_sem,
        qkv_send_sem,
        qkv_recv_sem,
        attn_send_sem,
        attn_recv_sem,
        proj_send_sem,
        proj_recv_sem,
        mid_send_sem,
        mid_recv_sem,
        z_send_sem,
        x_send_sem,
        x_recv_sem,
    ) = sems
    f32, bf16 = jnp.float32, jnp.bfloat16
    rows, model = hidden_ref.shape
    mine = rows // count_t
    qkv_columns = w_qkv.shape[1]
    steps = qkv_w_sem.shape[0]
    step_rows = w_qkv.shape[0] // steps
    out_steps = out_w_sem.shape[0]
    out_width = model // out_steps
    share = model // count_t
    positions = keys_v.shape[1]
    heads = QUERY_HEADS
    per_kv = QUERY_HEADS // KEY_VALUE_HEADS
    heads_t = heads // count_t

    def qkv_load(i):
        part = pl.ds(pl.multiple_of(i * step_rows, step_rows), step_rows)
        return pltpu.make_async_copy(w_qkv.at[part, :], qkv_w.at[part, :], qkv_w_sem.at[i])

    def out_load(i):
        part = pl.ds(pl.multiple_of(i * out_width, LANES), out_width)
        return pltpu.make_async_copy(w_out.at[:, part], out_w.at[:, part], out_w_sem.at[i])

    for i in range(steps):
        qkv_load(i).start()
    cache = [
        pltpu.make_async_copy(keys.at[0], keys_v, cache_sem.at[0]),
        pltpu.make_async_copy(values.at[0], values_v, cache_sem.at[1]),
    ]
    for copy in cache:
        copy.start()
    for i in range(out_steps):
        out_load(i).start()

    barrier = pltpu.get_barrier_semaphore()
    for tt in range(count_t):
        for ss in range(count_s):

            @pl.when((tt != t) | (ss != s))
            def _():
                pl.semaphore_signal(
                    barrier, inc=1, device_id={"tp": tt, "src": ss}, device_id_type=MESH
                )

    pl.semaphore_signal(barrier, inc=1, device_id={"grp": 1 - g}, device_id_type=MESH)

    with jax.named_scope("norm"):
        normed = normalize_rows(hidden_ref[...].astype(f32), row_of(attn_gain)).astype(bf16)
        moved = ordered(stack_lanes(normed), order_ref)
        for k in range(model // LANES):
            normed_v[:, k * LANES : (k + 1) * LANES] = moved[k * rows : (k + 1) * rows]

    swaps = [
        pltpu.make_async_remote_copy(
            src_ref=source,
            dst_ref=target.at[1],
            send_sem=swap_send_sem.at[index],
            recv_sem=swap_recv_sem.at[index],
            device_id={"grp": 1 - g},
            device_id_type=MESH,
        )
        for index, (source, target) in enumerate(zip(weights, (gate_v, up_v, down_v)))
    ]
    loads = [
        pltpu.make_async_copy(source, target.at[0], load_sem.at[index])
        for index, (source, target) in enumerate(zip(weights, (gate_v, up_v, down_v)))
    ]

    qkv_acc[...] = jnp.zeros_like(qkv_acc)

    def qkv_step(i, carry):
        qkv_load(i).wait()
        part = pl.ds(pl.multiple_of(i * step_rows, step_rows), step_rows)
        depth = pl.ds(pl.multiple_of(i * 4 * step_rows, LANES), 4 * step_rows)
        qkv_acc[...] += jnp.dot(
            normed_v[:, depth], unpack_slab(qkv_w[part, :]), preferred_element_type=f32
        )
        return carry

    with jax.named_scope("qkv"):
        lax.fori_loop(0, steps, qkv_step, 0)
        pl.semaphore_wait(barrier, count_t * count_s)
        for copy in swaps + loads:
            copy.start()
        qkv_send[...] = (qkv_acc[...] * row_of(qkv_scale)).astype(bf16)

    def peer_of(shift):
        return lax.rem(t + shift, count_t)

    def rows_of(index):
        return pl.ds(pl.multiple_of(index * mine, mine), mine)

    def qkv_copy(peer, slot):
        return pltpu.make_async_remote_copy(
            src_ref=qkv_send.at[rows_of(peer), :],
            dst_ref=qkv_recv.at[slot],
            send_sem=qkv_send_sem.at[peer],
            recv_sem=qkv_recv_sem.at[slot],
            device_id={"tp": peer},
            device_id_type=MESH,
        )

    for shift in range(1, count_t):
        qkv_copy(peer_of(shift), t).start()
    qkv_recv[t] = qkv_send[rows_of(t), :]

    def unpack_out(i, carry):
        out_load(i).wait()
        part = pl.ds(pl.multiple_of(i * out_width, LANES), out_width)
        out_u[:, part] = unpack_slab(out_w[:, part])
        return carry

    with jax.named_scope("unpack_out"):
        lax.fori_loop(0, out_steps, unpack_out, 0)

    row_index = lax.broadcasted_iota(jnp.int32, (mine, HEAD_SIZE), 0)
    lane = lax.broadcasted_iota(jnp.int32, (mine, HEAD_SIZE), 1)
    place = jnp.zeros((mine, HEAD_SIZE), f32)
    for b in range(mine):
        place = jnp.where(row_index == b, lengths[0, b].astype(f32), place)
    half_dim = HEAD_SIZE // 2
    low = lane < half_dim
    frequency = jnp.where(low, lane, lane - half_dim).astype(f32)
    angle = place * jnp.exp(frequency * (-math.log(rope_base) / half_dim))
    cosine = jnp.cos(angle)
    sine = jnp.sin(angle)
    sine = jnp.where(low, -sine, sine)

    with jax.named_scope("wait_qkv"):
        for shift in range(1, count_t):
            qkv_copy(t, peer_of(shift)).wait_recv()

    per_share = qkv_columns // HEAD_SIZE

    def head_of(h):
        column = (h % per_share) * HEAD_SIZE
        return qkv_recv[h // per_share, :, column : column + HEAD_SIZE]

    def turned(first, count, gain):
        stacked = jnp.concatenate([head_of(first + k) for k in range(count)], axis=0)
        value = normalize_rows(stacked.astype(f32), gain)
        other = pltpu.roll(value, half_dim, 1)
        wide = [jnp.concatenate([table] * count, axis=0) for table in (cosine, sine)]
        return (value * wide[0] + other * wide[1]).astype(bf16).astype(f32)

    logit_scale = 1.0 / math.sqrt(HEAD_SIZE)
    q_row, k_row = row_of(q_gain), row_of(k_gain)
    with jax.named_scope("rope"):
        new_keys = turned(heads, KEY_VALUE_HEADS, k_row)
        for kv in range(KEY_VALUE_HEADS):
            part = slice(kv * per_kv * mine, (kv + 1) * per_kv * mine)
            query = turned(kv * per_kv, per_kv, q_row)
            q_v[part] = query
            new_key = jnp.concatenate([new_keys[kv * mine : (kv + 1) * mine]] * per_kv, axis=0)
            own = jnp.sum(query * new_key, axis=1, keepdims=True) * logit_scale
            own_v[part] = jnp.broadcast_to(own, query.shape)
    for copy in cache:
            copy.wait()

    zeros = jnp.zeros((per_kv, HEAD_SIZE), f32)
    with jax.named_scope("scores"):
        for b in range(mine):
            query = q_v[pl.ds(b, heads, stride=mine), :]
            spread = jnp.concatenate(
                [
                    jnp.concatenate(
                        [
                            query[kv * per_kv : (kv + 1) * per_kv] if kv == place_of else zeros
                            for place_of in range(KEY_VALUE_HEADS)
                        ],
                        axis=1,
                    )
                    for kv in range(KEY_VALUE_HEADS)
                ],
                axis=0,
            ).astype(bf16)
            score_v[b * heads : (b + 1) * heads] = lax.dot_general(
                spread, keys_v[b], (((1,), (1,)), ((), ())), preferred_element_type=f32
            )
    position = lax.broadcasted_iota(jnp.int32, (heads, positions), 1)
    with jax.named_scope("softmax"):
        for b in range(mine):
            strided = pl.ds(b, heads, stride=mine)
            scores = score_v[b * heads : (b + 1) * heads] * logit_scale
            scores = jnp.where(position < lengths[0, b], scores, -jnp.inf)
            own = own_v[strided, :]
            top = jnp.maximum(jnp.max(scores, axis=1, keepdims=True), own)
            weight = jnp.exp(scores - top)
            own_e = jnp.exp(own - top)
            denominator = jnp.sum(weight, axis=1, keepdims=True) + own_e
            score_v[b * heads : (b + 1) * heads] = weight
            own_e_v[strided, :] = own_e
            denom_v[strided, :] = denominator
    with jax.named_scope("mix"):
        for b in range(mine):
            mixed = jnp.dot(
                score_v[b * heads : (b + 1) * heads].astype(bf16),
                values_v[b],
                preferred_element_type=f32,
            )
            attn_v[pl.ds(b, heads, stride=mine), :] = jnp.concatenate(
                [
                    mixed[kv * per_kv : (kv + 1) * per_kv, kv * HEAD_SIZE : (kv + 1) * HEAD_SIZE]
                    for kv in range(KEY_VALUE_HEADS)
                ],
                axis=0,
            )
    with jax.named_scope("finish_attn"):
        finished = []
        for h in range(heads):
            part = slice(h * mine, (h + 1) * mine)
            new_value = head_of(heads + KEY_VALUE_HEADS + h // per_kv).astype(f32)
            own_low = own_e_v[part].astype(bf16).astype(f32)
            finished.append(((attn_v[part] + own_low * new_value) / denom_v[part]).astype(bf16))
        attn_send[...] = ordered(jnp.concatenate(finished, axis=0), order_ref)

    head_rows = heads_t * mine

    def attn_copy(peer, slot):
        return pltpu.make_async_remote_copy(
            src_ref=attn_send.at[pl.ds(pl.multiple_of(peer * head_rows, head_rows), head_rows), :],
            dst_ref=attn_recv.at[slot],
            send_sem=attn_send_sem.at[peer],
            recv_sem=attn_recv_sem.at[slot],
            device_id={"tp": peer},
            device_id_type=MESH,
        )

    for shift in range(1, count_t):
        attn_copy(peer_of(shift), t).start()
    attn_recv[t] = attn_send[pl.ds(pl.multiple_of(t * head_rows, head_rows), head_rows), :]
    with jax.named_scope("wait_attn"):
        for shift in range(1, count_t):
            attn_copy(t, peer_of(shift)).wait_recv()

    def proj_copy(peer, slot, i):
        part = pl.ds(pl.multiple_of(i * out_width, LANES), out_width)
        return pltpu.make_async_remote_copy(
            src_ref=proj_v.at[rows_of(peer), part],
            dst_ref=proj_recv.at[slot, :, part],
            send_sem=proj_send_sem.at[peer],
            recv_sem=proj_recv_sem.at[slot],
            device_id={"tp": peer},
            device_id_type=MESH,
        )

    def proj_whole(peer, slot):
        return pltpu.make_async_remote_copy(
            src_ref=proj_v.at[rows_of(peer), :],
            dst_ref=proj_recv.at[slot],
            send_sem=proj_send_sem.at[peer],
            recv_sem=proj_recv_sem.at[slot],
            device_id={"tp": peer},
            device_id_type=MESH,
        )

    def out_step(i, carry):
        part = pl.ds(pl.multiple_of(i * out_width, LANES), out_width)
        left = jnp.concatenate(
            [
                jnp.concatenate(
                    [attn_recv[tt, h * mine : (h + 1) * mine] for tt in range(count_t)], axis=0
                )
                for h in range(heads_t)
            ],
            axis=1,
        )
        product = jnp.dot(left, out_u[:, part], preferred_element_type=f32)
        proj_v[:, part] = (product * out_scale[part].reshape(1, out_width)).astype(bf16)
        for shift in range(1, count_t):
            proj_copy(peer_of(shift), t, i).start()
        return carry

    with jax.named_scope("proj"):
        lax.fori_loop(0, out_steps, out_step, 0)

    with jax.named_scope("mid"):
        total = hidden_ref[rows_of(t), :].astype(f32) + proj_v[rows_of(t), :].astype(f32)
        for shift in range(1, count_t):
            slot = peer_of(shift)

            proj_whole(t, slot).wait_recv()
            total += proj_recv[slot].astype(f32)
        mid = total.astype(bf16)
        for tt in range(count_t):
            mid_send[tt] = mid[:, tt * share : (tt + 1) * share]
        moved = ordered(
            stack_lanes(normalize_rows(mid.astype(f32), row_of(mlp_gain)).astype(bf16)), order_ref
        )
    block = model // (count_g * count_s) // LANES
    with jax.named_scope("order_x"):
        for number in range(count_g * count_s):
            owner = number % count_s
            first = jnp.where(number // count_s == g, 0, block)
            for k in range(block):
                column = pl.multiple_of((first + k) * LANES, LANES)
                source = number * block + k
                x_send[owner, :, pl.ds(column, LANES)] = moved[source * mine : (source + 1) * mine]

    def x_rows(ss, tt):
        return pl.ds(pl.multiple_of((ss * count_t + tt) * mine, mine), mine)

    def z_copy(peer, ss):
        return pltpu.make_async_remote_copy(
            src_ref=x_send.at[peer],
            dst_ref=x_v.at[x_rows(ss, t), :],
            send_sem=z_send_sem.at[peer],
            recv_sem=x_recv_sem.at[ss, t],
            device_id={"src": peer},
            device_id_type=MESH,
        )

    def x_copy(peer, ss, tt):
        return pltpu.make_async_remote_copy(
            src_ref=x_v.at[x_rows(ss, tt), :],
            dst_ref=x_v.at[x_rows(ss, tt), :],
            send_sem=x_send_sem.at[peer],
            recv_sem=x_recv_sem.at[ss, tt],
            device_id={"tp": peer},
            device_id_type=MESH,
        )

    def own_copy(peer):
        return pltpu.make_async_remote_copy(
            src_ref=x_send.at[s],
            dst_ref=x_v.at[x_rows(s, t), :],
            send_sem=x_send_sem.at[peer],
            recv_sem=x_recv_sem.at[s, t],
            device_id={"tp": peer},
            device_id_type=MESH,
        )

    def x_whole(peer):
        return pltpu.make_async_remote_copy(
            src_ref=x_send,
            dst_ref=x_send,
            send_sem=x_send_sem.at[peer],
            recv_sem=x_recv_sem.at[s, t],
            device_id={"tp": peer},
            device_id_type=MESH,
        )

    def mid_copy(peer, slot):
        return pltpu.make_async_remote_copy(
            src_ref=mid_send.at[peer],
            dst_ref=mid_v.at[rows_of(slot), :],
            send_sem=mid_send_sem.at[peer],
            recv_sem=mid_recv_sem.at[slot],
            device_id={"tp": peer},
            device_id_type=MESH,
        )

    with jax.named_scope("spread_z"):
        def near(distance, action):
            for other in (s + distance, s - distance):

                @pl.when((other >= 0) & (other < count_s))
                def _():
                    action(other)

        for distance in range(count_s - 1, 0, -1):
            near(distance, lambda other: z_copy(other, s).start())
        for shift in range(1, count_t):
            own_copy(peer_of(shift)).start()
        x_v[x_rows(s, t), :] = x_send[s]

        def forward(ss):
            z_copy(s, ss).wait_recv()
            for turn in range(1, count_t):
                x_copy(peer_of(turn), ss, t).start()

        for distance in range(1, count_s):
            near(distance, forward)
    for shift in range(1, count_t):
        mid_copy(peer_of(shift), t).start()
    mid_v[rows_of(t), :] = mid_send[t]
    def x_wait(side):
        groups = count_s // 2
        base = jnp.where(side == 1, 0, groups)
        for k in range(groups):
            for turn in range(1, count_t):
                x_copy(t, base + k, peer_of(turn)).wait_recv()


    def finish():
        for shift in range(1, count_t):
            peer = peer_of(shift)
            qkv_copy(peer, t).wait_send()
            attn_copy(peer, t).wait_send()
            mid_copy(peer, t).wait_send()

            proj_whole(peer, t).wait_send()
            x_whole(peer).wait_send()
        for shift in range(1, count_s):
            z_copy(lax.rem(s + shift, count_s), s).wait_send()
        for copy in swaps:
            copy.wait_send()

    def mid_wait():
        for shift in range(1, count_t):
            mid_copy(t, peer_of(shift)).wait_recv()

    return swaps, loads, mid_wait, x_wait, finish


def mlp_phase(here, lags, scales, mlp_buffers, scratch, sems, attention, out_ref):
    g, t, s, count_g, count_t, count_s = here
    gate_scale, up_scale, down_scale, order_ref = scales
    lag, back_lag, far_lag, second_lag = lags
    gate_v, up_v, down_v, x_v, mid_v = mlp_buffers
    (
        partial,
        sum_recv,
        act,
        total,
        part_send,
        part_recv,
        stage_send,
        stage_recv,
        last_send,
        last_recv,
    ) = scratch
    (
        sum_send_sem,
        sum_recv_sem,
        act_send_sem,
        part_send_sem,
        part_recv_sem,
        stage_send_sem,
        stage_recv_sem,
        last_send_sem,
        last_recv_sem,
    ) = sems
    swaps, loads, mid_wait, x_wait, finish = attention
    rows = x_v.shape[0]
    half = rows // 2
    hidden = gate_v.shape[2]
    block = down_v.shape[2]
    chunks = hidden // LANES
    group_rows = rows // count_s
    total[...] = jnp.zeros_like(total)

    last = count_s - 1
    far = (last - 1) * lag

    def toward(side):
        return s - 1 + 2 * side

    def sum_copy(side, j):
        return pltpu.make_async_remote_copy(
            src_ref=partial.at[side, j],
            dst_ref=sum_recv.at[side, j],
            send_sem=sum_send_sem.at[side],
            recv_sem=sum_recv_sem.at[side, j],
            device_id={"src": toward(side)},
            device_id_type=MESH,
        )

    def act_copy(side, j):
        return pltpu.make_async_remote_copy(
            src_ref=act.at[side, j],
            dst_ref=act.at[side, j],
            send_sem=act_send_sem.at[side],
            recv_sem=sum_recv_sem.at[side, j],
            device_id={"src": toward(1 - side)},
            device_id_type=MESH,
        )

    def whole_copy(array, side, sem):
        return pltpu.make_async_remote_copy(
            src_ref=array.at[side],
            dst_ref=array.at[side],
            send_sem=sem.at[side],
            recv_sem=sum_recv_sem.at[side, 0],
            device_id={"src": toward(side)},
            device_id_type=MESH,
        )

    def depth_of(side):
        if isinstance(side, int):
            return last - s if side == 0 else s
        return jnp.where(side == 0, last - s, s)

    def pass_step(side, j):
        depth = depth_of(side)

        @pl.when(depth > 0)
        def _():
            sum_copy(side, j).wait_recv()
            partial[side, j] = (
                partial[side, j].astype(jnp.float32) + sum_recv[side, j].astype(jnp.float32)
            ).astype(jnp.bfloat16)

        sum_copy(side, j).start()

    def end_step(side, j):
        sum_copy(side, j).wait_recv()
        value = partial[side, j].astype(jnp.float32) + sum_recv[side, j].astype(jnp.float32)
        columns = pl.ds(pl.multiple_of(j * LANES, LANES), LANES)
        gate_value = value[:, :LANES] * gate_scale[columns].reshape(1, LANES)
        up_value = value[:, LANES:] * up_scale[columns].reshape(1, LANES)
        activated = (gate_value / (1.0 + jnp.exp(-gate_value)) * up_value).astype(jnp.bfloat16)
        act[side, j] = jnp.dot(
            activated, order_ref[...], preferred_element_type=jnp.float32
        ).astype(jnp.bfloat16)
        act_copy(side, j).start()

    def act_step(side, j):
        depth = last - depth_of(side)
        act_copy(side, j).wait_recv()

        @pl.when(depth < last)
        def _():
            act_copy(side, j).start()

    near = jnp.where(2 * s < count_s, 1, 0)
    is_end = (s == 0) | (s == last)

    def product_step(side, i):
        columns = pl.ds(pl.multiple_of(i * LANES, LANES), LANES)
        gate_w = [unpack_slab(gate_v[index, :, columns]) for index in range(2)]
        up_w = [unpack_slab(up_v[index, :, columns]) for index in range(2)]
        weights = jnp.concatenate(
            [jnp.concatenate(gate_w, axis=0), jnp.concatenate(up_w, axis=0)], axis=1
        )
        row = pl.ds(pl.multiple_of((1 - side) * half, half), half)
        partial[side, i] = jnp.dot(
            x_v[row, :], weights, preferred_element_type=jnp.float32
        ).astype(jnp.bfloat16)

    def step(i, carry):
        for side, wait in ((near, 0), (1 - near, far_lag)):
            k = i - wait

            @pl.when((k >= 0) & (k < chunks))
            def _():
                @pl.when(k == 0)
                def _():
                    x_wait(side)

                product_step(side, k)

            depth = depth_of(side)
            j = i - depth * lag

            @pl.when((depth < last) & (j >= 0) & (j < chunks))
            def _():
                pass_step(side, j)

        return carry

    def down_step(sides, j):
        slab = LANES // 4
        words = pl.ds(pl.multiple_of(j * slab, slab), slab)
        weights = jnp.concatenate(
            [unpack_slab(down_v[index, words, :]) for index in range(2)], axis=1
        )
        for side in sides:
            total[(1 - side) * half : (2 - side) * half] += jnp.dot(
                act[side, j], weights, preferred_element_type=jnp.float32
            )

    def end_loop(j, carry):
        for side in range(2):

            @pl.when(depth_of(side) == last)
            def _():
                end_step(side, j)
                down_step((side,), j)

        return carry

    near_depth = jnp.minimum(s, last - s)
    far_depth = jnp.maximum(s, last - s)
    second = jnp.where(is_end, last * back_lag + second_lag, chunks + far_depth * back_lag)

    def back_step(i, carry):
        for side in range(2):
            depth = last - depth_of(side)
            j = i - depth * back_lag

            @pl.when((depth > 0) & (j >= 0) & (j < chunks))
            def _():
                act_step(side, j)
                down_step((side,), j)

        @pl.when(jnp.logical_not(is_end) & (i == chunks + near_depth * back_lag))
        def _():
            stage_rows()

        @pl.when(i == second)
        def _():
            pass_rows()

        return carry

    per_share = count_g * count_s // count_t

    groups = count_s // 2
    quarter = group_rows // count_t
    low_half = s < groups
    near_base = jnp.where(low_half, 0, groups)
    cross_base = groups - near_base

    def target_of(index):
        number = jnp.where(index == 0, g, count_g - 1 - g) * count_s + s
        return number // per_share, lax.rem(number, per_share)

    def part_copy(index, k, ss):
        owner, place = target_of(index)
        slot = t * per_share + place
        return owner, slot, pltpu.make_async_remote_copy(
            src_ref=part_send.at[index, k],
            dst_ref=part_recv.at[slot],
            send_sem=part_send_sem.at[index, k],
            recv_sem=part_recv_sem.at[slot],
            device_id={"tp": owner, "src": ss},
            device_id_type=MESH,
        )

    def stage_copy(peer):
        return pltpu.make_async_remote_copy(
            src_ref=stage_send.at[peer],
            dst_ref=stage_recv.at[t],
            send_sem=stage_send_sem.at[peer],
            recv_sem=stage_recv_sem.at[t],
            device_id={"tp": peer},
            device_id_type=MESH,
        )

    def stage_arrival(peer):
        return pltpu.make_async_remote_copy(
            src_ref=stage_send.at[peer],
            dst_ref=stage_recv.at[peer],
            send_sem=stage_send_sem.at[peer],
            recv_sem=stage_recv_sem.at[peer],
            device_id={"tp": peer},
            device_id_type=MESH,
        )

    def last_copy(index, k, place, slot, owner):
        return pltpu.make_async_remote_copy(
            src_ref=last_send.at[index, k],
            dst_ref=last_recv.at[place, slot],
            send_sem=last_send_sem.at[index, k],
            recv_sem=last_recv_sem.at[place, slot],
            device_id={"tp": owner, "src": cross_base + k},
            device_id_type=MESH,
        )

    def quarter_rows(k, tt):
        start = (cross_base + k) * group_rows + tt * quarter
        return pl.ds(pl.multiple_of(start, quarter), quarter)

    def stage_rows():
        for shift in range(1, count_t):
            peer = lax.rem(t + shift, count_t)
            for k in range(groups):
                stage_send[peer, k] = total[quarter_rows(k, peer), :].astype(jnp.bfloat16)
            stage_copy(peer).start()

    def pass_rows():
        for shift in range(1, count_t):
            stage_arrival(lax.rem(t + shift, count_t)).wait_recv()
        for k in range(groups):
            value = total[quarter_rows(k, t), :]
            for turn in range(1, count_t):
                value += stage_recv[lax.rem(t + turn, count_t), k].astype(jnp.float32)
            for index in range(2):
                owner, place = target_of(index)
                last_send[index, k] = value[:, index * block : (index + 1) * block].astype(
                    jnp.bfloat16
                )
                last_copy(index, k, place, t, owner).start()

    def near_rows(k):
        ss = near_base + lax.rem(s - near_base + 1 + k, groups)
        return ss, pl.ds(pl.multiple_of(ss * group_rows, group_rows), group_rows)

    for index in range(2):
        loads[index].wait()
        swaps[index].wait_recv()
    with jax.named_scope("mlp_loop"):
        lax.fori_loop(0, chunks + far, step, 0)
    with jax.named_scope("end_loop"):
        loads[2].wait()
        swaps[2].wait_recv()
        lax.fori_loop(0, chunks, end_loop, 0)

        @pl.when(is_end)
        def _():
            stage_rows()

    with jax.named_scope("back_loop"):
        lax.fori_loop(0, chunks + last * back_lag, back_step, 0)

    def drain():
        with jax.named_scope("drain"):
            finish()
            for side in range(2):
                depth = depth_of(side)

                @pl.when(depth < last)
                def _():
                    whole_copy(partial, side, sum_send_sem).wait_send()

                @pl.when(depth > 0)
                def _():
                    whole_copy(act, side, act_send_sem).wait_send()

    with jax.named_scope("part_send"):
        for k in range(groups):
            ss, row = near_rows(k)
            for index in range(2):
                owner, slot, copy = part_copy(index, k, ss)
                piece = total[row, index * block : (index + 1) * block].astype(jnp.bfloat16)
                mine = (owner == t) & (ss == s)

                @pl.when(mine)
                def _():
                    part_recv[slot] = piece

                @pl.when(jnp.logical_not(mine))
                def _():
                    part_send[index, k] = piece
                    copy.start()

    drain()
    mid_wait()
    with jax.named_scope("part_wait"):
        for place in range(per_share):
            origin = lax.rem(t * per_share + place, count_s)
            crosses = (origin < groups) != low_half
            columns = slice(place * block, (place + 1) * block)
            scale_at = pl.ds(pl.multiple_of((t * per_share + place) * block, LANES), block)

            @pl.when(jnp.logical_not(crosses))
            def _():
                for tt in range(count_t):

                    @pl.when((tt != t) | (origin != s))
                    def _():
                        pltpu.make_async_remote_copy(
                            src_ref=part_send.at[0, 0],
                            dst_ref=part_recv.at[tt * per_share + place],
                            send_sem=part_send_sem.at[0, 0],
                            recv_sem=part_recv_sem.at[tt * per_share + place],
                            device_id={"tp": tt},
                            device_id_type=MESH,
                        ).wait_recv()

                value = part_recv[place].astype(jnp.float32)
                for tt in range(1, count_t):
                    value += part_recv[tt * per_share + place].astype(jnp.float32)
                out_ref[:, columns] = mid_v[:, columns].astype(jnp.float32) + value * down_scale[
                    scale_at
                ].reshape(1, block)

            @pl.when(crosses)
            def _():
                for tt in range(count_t):
                    last_copy(0, 0, place, tt, t).wait_recv()
                    row = slice(tt * quarter, (tt + 1) * quarter)
                    out_ref[row, columns] = mid_v[row, columns].astype(jnp.float32) + last_recv[
                        place, tt
                    ].astype(jnp.float32) * down_scale[scale_at].reshape(1, block)

    for shift in range(1, count_t):
        stage_copy(lax.rem(t + shift, count_t)).wait_send()
    for k in range(groups):
        ss, row = near_rows(k)
        for index in range(2):
            owner, place = target_of(index)
            last_copy(index, k, place, t, owner).wait_send()

            @pl.when((owner != t) | (ss != s))
            def _():
                part_copy(index, k, ss)[2].wait_send()


def layer_kernel(lags, counts, *refs):
    count_in, count_buffers, count_a, count_asem, count_b, count_bsem = counts
    take = iter(refs)

    def some(count):
        return [next(take) for _ in range(count)]

    (
        hidden_ref,
        attn_gain,
        w_qkv,
        qkv_scale,
        q_gain,
        k_gain,
        keys,
        values,
        lengths,
        w_out,
        out_scale,
        mlp_gain,
        w_gate,
        w_up,
        gate_scale,
        up_scale,
        w_down,
        down_scale,
    ) = some(count_in)
    out_ref = next(take)
    order_ref = next(take)
    order_ref[...] = lane_order(LANES)
    mlp_buffers = some(count_buffers)
    scratch_a, sems_a = some(count_a), some(count_asem)
    scratch_b, sems_b = some(count_b), some(count_bsem)
    here = tuple(lax.axis_index(name) for name in ("grp", "tp", "src")) + tuple(
        lax.axis_size(name) for name in ("grp", "tp", "src")
    )
    attention = attention_phase(
        here,
        (
            hidden_ref,
            attn_gain,
            w_qkv,
            qkv_scale,
            q_gain,
            k_gain,
            keys,
            values,
            lengths,
            w_out,
            out_scale,
            mlp_gain,
            (w_gate, w_up, w_down),
            order_ref,
        ),
        mlp_buffers,
        scratch_a,
        sems_a,
    )
    mlp_phase(
        here,
        lags,
        (gate_scale, up_scale, down_scale, order_ref),
        mlp_buffers,
        scratch_b,
        sems_b,
        attention,
        out_ref,
    )


def layer(args, lags):
    (
        hidden_in,
        attn_gain,
        w_qkv,
        qkv_scale,
        q_gain,
        k_gain,
        key_cache,
        value_cache,
        lengths,
        w_out,
        out_scale,
        mlp_gain,
        w_gate,
        w_up,
        gate_scale,
        up_scale,
        w_down,
        down_scale,
    ) = args
    count_g, count_t, count_s = (lax.axis_size(name) for name in ("grp", "tp", "src"))
    group_rows, model = hidden_in.shape
    rows = group_rows * count_s
    half = rows // 2
    mine = group_rows // count_t
    packed_rows, hidden = w_gate.shape
    packed_hidden, block = w_down.shape
    depth = 2 * block
    chunks = hidden // LANES
    share = model // count_t
    slots = count_g * count_s
    steps = 10 if w_qkv.shape[0] % 320 == 0 else w_qkv.shape[0] // 32
    out_steps = 8 if model % (8 * LANES) == 0 else model // LANES
    qkv_columns = w_qkv.shape[1]
    head_rows = QUERY_HEADS * mine
    bf16, f32, i32 = jnp.bfloat16, jnp.float32, jnp.int32
    dma = pltpu.SemaphoreType.DMA
    vmem = pl.BlockSpec(memory_space=pltpu.VMEM)
    smem = pl.BlockSpec(memory_space=pltpu.SMEM)
    hbm = pl.BlockSpec(memory_space=pl.ANY)
    buffers = [
        pltpu.VMEM((2, packed_rows, hidden), i32),
        pltpu.VMEM((2, packed_rows, hidden), i32),
        pltpu.VMEM((2, packed_hidden, block), i32),
        pltpu.VMEM((rows, depth), bf16),
        pltpu.VMEM((group_rows, share), bf16),
    ]
    scratch_a = [
        pltpu.VMEM(w_qkv.shape, i32),
        pltpu.VMEM(w_out.shape, i32),
        pltpu.VMEM((4 * w_out.shape[0], model), bf16),
        pltpu.VMEM(key_cache.shape[1:], bf16),
        pltpu.VMEM(value_cache.shape[1:], bf16),
        pltpu.VMEM((group_rows, model), bf16),
        pltpu.VMEM((group_rows, qkv_columns), f32),
        pltpu.VMEM((group_rows, qkv_columns), bf16),
        pltpu.VMEM((count_t, mine, qkv_columns), bf16),
        pltpu.VMEM((head_rows, HEAD_SIZE), f32),
        pltpu.VMEM((head_rows, HEAD_SIZE), f32),
        pltpu.VMEM((head_rows, key_cache.shape[2]), f32),
        pltpu.VMEM((head_rows, HEAD_SIZE), f32),
        pltpu.VMEM((head_rows, HEAD_SIZE), f32),
        pltpu.VMEM((head_rows, HEAD_SIZE), f32),
        pltpu.VMEM((head_rows, HEAD_SIZE), bf16),
        pltpu.VMEM((count_t, head_rows // count_t, HEAD_SIZE), bf16),
        pltpu.VMEM((group_rows, model), bf16),
        pltpu.VMEM((count_t, mine, model), bf16),
        pltpu.VMEM((count_t, mine, share), bf16),
        pltpu.VMEM((count_s, mine, depth), bf16),
    ]
    sems_a = [
        dma((steps,)),
        dma((out_steps,)),
        dma((2,)),
        dma((3,)),
        dma((3,)),
        dma((3,)),
        dma((count_t,)),
        dma((count_t,)),
        dma((count_t,)),
        dma((count_t,)),
        dma((count_t,)),
        dma((count_t,)),
        dma((count_t,)),
        dma((count_t,)),
        dma((count_s,)),
        dma((count_t,)),
        dma((count_s, count_t)),
    ]
    scratch_b = [
        pltpu.VMEM((2, chunks, half, 2 * LANES), bf16),
        pltpu.VMEM((2, chunks, half, 2 * LANES), bf16),
        pltpu.VMEM((2, chunks, half, LANES), bf16),
        pltpu.VMEM((rows, depth), f32),
        pltpu.VMEM((2, count_s // 2, group_rows, block), bf16),
        pltpu.VMEM((slots, group_rows, block), bf16),
        pltpu.VMEM((count_t, count_s // 2, mine, depth), bf16),
        pltpu.VMEM((count_t, count_s // 2, mine, depth), bf16),
        pltpu.VMEM((2, count_s // 2, mine, block), bf16),
        pltpu.VMEM((slots // count_t, count_t, mine, block), bf16),
    ]
    sems_b = [
        dma((2,)),
        dma((2, chunks)),
        dma((2,)),
        dma((2, count_s // 2)),
        dma((slots,)),
        dma((count_t,)),
        dma((count_t,)),
        dma((2, count_s // 2)),
        dma((slots // count_t, count_t)),
    ]
    specs = [vmem] * len(args)
    for place in (2, 6, 7, 9, 12, 13, 16):
        specs[place] = hbm
    specs[8] = smem
    counts = (
        len(specs),
        len(buffers),
        len(scratch_a),
        len(sems_a),
        len(scratch_b),
        len(sems_b),
    )
    return pl.pallas_call(
        functools.partial(layer_kernel, lags, counts),
        out_shape=pltpu.VMEM((group_rows, share), f32),
        in_specs=specs,
        out_specs=vmem,
        scratch_shapes=[pltpu.VMEM((LANES, LANES), bf16)] + buffers + scratch_a + sems_a + scratch_b + sems_b,
        compiler_params=pltpu.CompilerParams(
            collective_id=1, has_side_effects=True, vmem_limit_bytes=63 * 1024 * 1024
        ),
        name="layer",
    )(*args).astype(bf16)


def fast_layer(args):
    hidden_in, w_qkv, w_out, w_gate, w_down = (args[k] for k in (0, 2, 9, 12, 16))
    grp, tp, src = (lax.axis_size(name) for name in ("grp", "tp", "src"))
    rows, model = hidden_in.shape
    return (
        grp == 2
        and src % 2 == 0
        and tp > 1
        and (grp * src) % tp == 0
        and rows % (16 * tp) == 0
        and QUERY_HEADS % tp == 0
        and model % (LANES * tp) == 0
        and w_qkv.shape[0] % 32 == 0
        and w_qkv.shape[1] % HEAD_SIZE == 0
        and w_out.shape[0] % 32 == 0
        and w_gate.shape[0] % 32 == 0
        and w_gate.shape[1] % LANES == 0
        and w_down.shape[1] % LANES == 0
        and args[6].shape[2] == LANES
        and HEAD_SIZE == LANES
    )


def local(
    hidden_in,
    attn_gain,
    w_qkv,
    qkv_scale,
    q_gain,
    k_gain,
    key_cache,
    value_cache,
    lengths,
    w_out,
    out_scale,
    mlp_gain,
    w_gate,
    w_up,
    gate_scale,
    up_scale,
    w_down,
    down_scale,
):
    args = (
        hidden_in,
        attn_gain,
        w_qkv,
        qkv_scale,
        q_gain,
        k_gain,
        key_cache,
        value_cache,
        lengths,
        w_out,
        out_scale,
        mlp_gain,
        w_gate,
        w_up,
        gate_scale,
        up_scale,
        w_down,
        down_scale,
    )
    if fast_layer(args):
        return layer(args, (4, 8, 4, 14))
    tp_count = lax.axis_size("tp")
    tp_index = lax.axis_index("tp")
    share_cols = D // tp_count
    residual = hidden_in.astype(jnp.float32)
    normed = normalize_rows(residual, attn_gain).astype(jnp.bfloat16)
    qkv_part = (byte_product(normed, w_qkv) * qkv_scale).astype(jnp.bfloat16)
    query_key_value_rows = lax.all_to_all(qkv_part, "tp", split_axis=0, concat_axis=1, tiled=True)
    heads_out = local_attention(
        query_key_value_rows, q_gain, k_gain, key_cache[0], value_cache[0], lengths[0]
    )
    head_rows = lax.all_to_all(heads_out, "tp", split_axis=1, concat_axis=0, tiled=True)
    partial_value = (byte_product(head_rows, w_out) * out_scale).astype(jnp.bfloat16)
    residual_share = lax.dynamic_slice_in_dim(hidden_in, tp_index * share_cols, share_cols, 1)
    mid_share = (
        residual_share.astype(jnp.float32) + summed_share(partial_value, tp_count)
    ).astype(jnp.bfloat16)
    mid_full = lax.all_gather(mid_share, "tp", axis=1, tiled=True)
    normed_mlp = normalize_rows(mid_full.astype(jnp.float32), mlp_gain).astype(jnp.bfloat16)
    mlp_columns = order_bytes(
        lax.all_to_all(normed_mlp, ("grp", "src"), split_axis=1, concat_axis=0, tiled=True)
    )
    gate_terms = jnp.dot(mlp_columns, unpack_ordered(w_gate), preferred_element_type=jnp.float32)
    up_terms = jnp.dot(mlp_columns, unpack_ordered(w_up), preferred_element_type=jnp.float32)
    both_terms = jnp.concatenate(
        [gate_terms.astype(jnp.bfloat16), up_terms.astype(jnp.bfloat16)], axis=1
    )
    both = summed_rows(summed_rows(both_terms, "grp").astype(jnp.bfloat16), "src")
    hidden = gate_scale.shape[0]
    gate_value = both[:, :hidden] * gate_scale
    up_value = both[:, hidden:] * up_scale
    activated = order_bytes((jax.nn.silu(gate_value) * up_value).astype(jnp.bfloat16))
    all_activated = gathered_rows(gathered_rows(activated, "src"), "grp")
    down_columns = jnp.dot(
        all_activated, unpack_ordered(w_down), preferred_element_type=jnp.float32
    ).astype(jnp.bfloat16)
    down_rows = lax.all_to_all(
        down_columns, ("grp", "src"), split_axis=0, concat_axis=1, tiled=True
    )
    down_share = lax.dynamic_slice_in_dim(down_scale, tp_index * share_cols, share_cols, 0)
    mlp_share = summed_share(down_rows, tp_count) * down_share
    return (mid_share.astype(jnp.float32) + mlp_share).astype(jnp.bfloat16)


def solution(mesh):
    return jax.shard_map(
        local,
        mesh=mesh,
        in_specs=(
            P(("grp", "src"), None),
            P(),
            P(None, "tp"),
            P("tp"),
            P(),
            P(),
            P(("grp", "src"), "tp", None, None),
            P(("grp", "src"), "tp", None, None),
            P(("grp", "src"), "tp"),
            P("tp", None),
            P(),
            P(),
            P(("grp", "src"), "tp"),
            P(("grp", "src"), "tp"),
            P("tp"),
            P("tp"),
            P("tp", ("grp", "src")),
            P(),
        ),
        out_specs=P(("grp", "src"), "tp"),
        check_vma=False,
    )
```
